32 devices in a mesh: seq: 8 (over z, x), head: 4 (over y, core).
Axes of the slice: x: 2, y: 2, z: 4, core: 2. Of those that a mesh axis runs over, the one named last changes fastest.
Arguments:
- queries: bfloat16 [8192, 2048], P('seq', 'head'), may hold values from -64 to 64
- keys: bfloat16 [8192, 2048], P('seq', 'head'), may hold values from -16 to 16
- values: bfloat16 [8192, 2048], P('seq', 'head'), may hold values from -6 to 6
- span_bounds: int32 [16, 2], replicated, may hold values from 0 to 8192, as said below
- mem_decay: float32 [8, 16], P(None, 'head'), may hold values from 0.01 to 1
- mem_gate: float32 [16], P('head'), may hold values from -2 to 2
- out_weight: bfloat16 [2048, 4096], P('head'), may hold values from -0.125 to 0.125
Outputs:
- mixed: bfloat16 [8192, 4096], P('seq', 'head')
The draws below stay inside these ranges and needn't reach their ends.
Inputs may be any that keep to these rules, and one draw needn't show every extreme that they name: `span_bounds`: slot k lies in segment k // 2, inside the k % 2-th of 2 equal parts of it; start <= end, an empty slot has start == end; some slot covers a whole part.
All inputs are finite; a program needn't handle non-finite values.
Results may differ from the reference program's by a relative error of at most 0.0052.
The reference program's roundings to bfloat16 on the way (of `weights` and `attended`) count: a program that leaves them out, or rounds other values in their place, can miss the bound.
Values may be sent and summed in bfloat16 or wider, within the bound.
No kernel may reach another device: no remote copies, remote signals or barrier semaphores. Data moves between devices by JAX's collectives and lax.ppermute only.
A program may use at most 128 MiB of HBM per device.

```python
import math
import jax
import jax.numpy as jnp
from jax import lax

D = 4096
HEAD_DIM = 128
SEG = 1024
BAND = 512
SPAN_DEV = 2
HEAD_TOTAL = 16
TOKENS = 8192
SPANS = 16
N_SEQ = 8


def query_key_pair(key):
    random_subkeys = jax.random.split(jax.random.fold_in(key, 7), 2)
    query_draw = jnp.clip(jax.random.normal(random_subkeys[0], (TOKENS, HEAD_TOTAL * HEAD_DIM), jnp.float32), -6.0, 6.0)
    key_draw = jnp.clip(jax.random.normal(random_subkeys[1], (TOKENS, HEAD_TOTAL * HEAD_DIM), jnp.float32), -6.0, 6.0)
    return (query_draw, key_draw)


def draw_queries(key, part):
    return query_key_pair(key)[0].astype(jnp.bfloat16)


def draw_keys(key, part):
    return query_key_pair(key)[1].astype(jnp.bfloat16)


def draw_span_bounds(key, part):
    random_subkeys = jax.random.split(key, 5)
    region = SEG // SPAN_DEV
    heaviness = jax.random.randint(random_subkeys[0], (N_SEQ, 1), 0, 4)
    offset = jax.random.randint(random_subkeys[1], (N_SEQ, SPAN_DEV), 0, region // 4 + 1)
    length_raw = jax.random.randint(random_subkeys[2], (N_SEQ, SPAN_DEV), region // 4, region + 1)
    length = jnp.minimum(length_raw, region - offset)
    live = (jax.random.randint(random_subkeys[3], (N_SEQ, SPAN_DEV), 0, 4) < heaviness).astype(jnp.int32)
    chosen_slot = jax.random.randint(random_subkeys[4], (), 0, N_SEQ * SPAN_DEV)
    flat_index = jnp.arange(N_SEQ * SPAN_DEV).reshape(N_SEQ, SPAN_DEV)
    forced = flat_index == chosen_slot
    offset = jnp.where(forced, 0, offset)
    length = jnp.where(forced, region, length)
    live = jnp.where(forced, 1, live)
    seg_start = (jnp.arange(N_SEQ) * SEG)[:, None]
    part_start = (jnp.arange(SPAN_DEV) * region)[None, :]
    starts = seg_start + part_start + offset
    ends = starts + length * live
    return jnp.stack([starts.reshape(-1), ends.reshape(-1)], axis=1).astype(jnp.int32)


def draw_mem_decay(key, part):
    random_subkeys = jax.random.split(key, 6)
    slow_heads = jax.random.uniform(random_subkeys[0], (HEAD_TOTAL,), jnp.float32) < 0.5
    total_loss = jnp.where(slow_heads, jax.random.uniform(random_subkeys[1], (HEAD_TOTAL,), jnp.float32, 0.3, 2.0), jax.random.uniform(random_subkeys[2], (HEAD_TOTAL,), jnp.float32, 20.0, 60.0))
    iteration_loss = total_loss[None, :] / N_SEQ * jax.random.uniform(random_subkeys[3], (N_SEQ, HEAD_TOTAL), jnp.float32, 0.5, 1.5)
    surge_events = jax.random.uniform(random_subkeys[4], (N_SEQ, HEAD_TOTAL), jnp.float32) < 3.0 / N_SEQ
    surge_loss_value = jnp.where(surge_events, -jnp.log(jax.random.uniform(random_subkeys[5], (N_SEQ, HEAD_TOTAL), jnp.float32, 0.5, 0.8)), 0.0)
    return jnp.maximum(jnp.exp(-iteration_loss - surge_loss_value), 0.01)


def levels(own_key, dims, shards, low, top_value):
    level = 1.0
    for axis_at, parts in shards:
        draws = jax.random.uniform(jax.random.fold_in(jax.random.fold_in(own_key, 6), axis_at), (parts,), jnp.float32, low / len(shards), top_value / len(shards))
        level = level * jnp.repeat(jnp.exp(draws), dims[axis_at] // parts).reshape((-1,) + (1,) * (len(dims) - 1 - axis_at))
    return level


def centred(rng, dims, deviation, bound, shards=(), dtype=jnp.bfloat16):
    result = deviation * jax.random.normal(rng, dims, jnp.float32)
    if shards:
        result = result * levels(rng, dims, shards, -0.22, 0.18)
    return jnp.clip(result, -bound, bound).astype(dtype)


def setup_inputs(seed: int = 0) -> dict:
    arg_keys = jax.random.split(jax.random.key(seed), 8)
    return {
        "queries": draw_queries(jax.random.fold_in(arg_keys[7], 71), 0),
        "keys": draw_keys(jax.random.fold_in(arg_keys[7], 71), 0),
        "values": centred(arg_keys[2], (TOKENS, HEAD_TOTAL * HEAD_DIM), 1.0, 6.0, ((0, 8), (1, 4))),
        "span_bounds": draw_span_bounds(jax.random.fold_in(arg_keys[7], 71), 0),
        "mem_decay": draw_mem_decay(jax.random.fold_in(arg_keys[7], 71), 0),
        "mem_gate": jnp.clip(jax.random.uniform(arg_keys[5], (HEAD_TOTAL,), jnp.float32, -2.0, 2.0) * levels(arg_keys[5], (HEAD_TOTAL,), ((0, 4),), -0.4, 0.0), -2.0, 2.0),
        "out_weight": centred(arg_keys[6], (HEAD_TOTAL * HEAD_DIM, D), (HEAD_TOTAL * HEAD_DIM) ** -0.5, 0.125, ((0, 4),)),
    }


HIGHEST_PRECISION = lax.Precision.HIGHEST

def feature_map(values_in):
    return jnp.where(values_in > 0, values_in + 1.0, jnp.exp(jnp.minimum(values_in, 0.0)))

def local_attention(queries_3d, band_keys, band_values, query_labels, key_labels, shard_index, band_width):
    seg_rows, head_count, head_width = queries_3d.shape
    block_rows = min(seg_rows, 512)
    key_count = band_keys.shape[0]
    key_pos = jnp.arange(key_count).astype(jnp.int32) - band_width
    key_valid = (key_pos >= 0) | (shard_index > 0)
    score_scale = 1.0 / math.sqrt(head_width)
    keys_wide = band_keys.astype(jnp.float32)
    values_wide = band_values.astype(jnp.float32)

    def attend_block(block_index):
        row_start = (block_index * block_rows).astype(jnp.int32)
        query_block = lax.dynamic_slice_in_dim(queries_3d, row_start, block_rows, 0).astype(jnp.float32)
        label_block = lax.dynamic_slice_in_dim(query_labels, row_start, block_rows, 0)
        query_pos = row_start + jnp.arange(block_rows).astype(jnp.int32)
        scores = jnp.einsum('qhd,khd->hqk', query_block, keys_wide) * score_scale
        nearby = (key_pos[None, :] <= query_pos[:, None]) & (key_pos[None, :] > query_pos[:, None] - band_width) & key_valid[None, :]
        same_span = (label_block[:, None] > 0) & (label_block[:, None] == key_labels[None, :])
        visible = nearby | same_span
        scores = jnp.where(visible[None], scores, -1e+30)
        top_score = lax.optimization_barrier(jnp.max(scores, axis=-1, keepdims=True))
        weights = jnp.exp(scores - top_score)
        totals = lax.optimization_barrier(jnp.sum(weights, axis=-1))
        rounded = lax.optimization_barrier(weights.astype(jnp.bfloat16)).astype(jnp.float32)
        mixed_out = jnp.einsum('hqk,khd->qhd', rounded, values_wide)
        return mixed_out / jnp.transpose(totals)[:, :, None]
    blocks = lax.map(attend_block, jnp.arange(seg_rows // block_rows).astype(jnp.int32))
    return blocks.reshape(seg_rows, head_count, head_width)

def reference(queries, keys, values, span_bounds, mem_decay, mem_gate, out_weight):
    positions = jnp.arange(TOKENS).astype(jnp.int32)
    inside = (positions[:, None] >= span_bounds[None, :, 0]) & (positions[:, None] < span_bounds[None, :, 1])
    slot_ids = (jnp.arange(SPANS).astype(jnp.int32) + 1)[None, :]
    labels = lax.optimization_barrier(jnp.sum(inside.astype(jnp.int32) * slot_ids, axis=1)).astype(jnp.int32)
    query_seg = queries.reshape(N_SEQ, SEG, HEAD_TOTAL, HEAD_DIM)
    key_seg = keys.reshape(N_SEQ, SEG, HEAD_TOTAL, HEAD_DIM)
    value_seg = values.reshape(N_SEQ, SEG, HEAD_TOTAL, HEAD_DIM)
    label_segment = labels.reshape(N_SEQ, SEG)

    def memory_step(carry, inputs):
        memory, feat_total = carry
        shard_q, shard_k, shard_v, decay = inputs
        query_feats = feature_map(shard_q.astype(jnp.float32))
        key_feats = feature_map(shard_k.astype(jnp.float32))
        value_rows = shard_v.astype(jnp.float32)
        numer = jnp.einsum('thd,hde->the', query_feats, memory, precision=HIGHEST_PRECISION)
        denom = jnp.einsum('thd,hd->th', query_feats, feat_total, precision=HIGHEST_PRECISION) + 1.0
        readout = numer / denom[:, :, None]
        state = jnp.einsum('thd,the->hde', key_feats, value_rows, precision=HIGHEST_PRECISION)
        memory = decay[:, None, None] * memory + state
        feat_total = decay[:, None] * feat_total + lax.optimization_barrier(jnp.sum(key_feats, axis=0))
        return ((memory, feat_total), readout)
    start_memory = jnp.zeros((HEAD_TOTAL, HEAD_DIM, HEAD_DIM), jnp.float32)
    start_total = jnp.zeros((HEAD_TOTAL, HEAD_DIM), jnp.float32)
    unused, readouts = lax.scan(memory_step, (start_memory, start_total), (query_seg, key_seg, value_seg, mem_decay))

    def shard_attention(shard_index):
        earlier = jnp.maximum(shard_index - 1, 0)
        band_keys = jnp.concatenate([key_seg[earlier][SEG - BAND:], key_seg[shard_index]], axis=0)
        band_values = jnp.concatenate([value_seg[earlier][SEG - BAND:], value_seg[shard_index]], axis=0)
        query_labels = label_segment[shard_index]
        key_labels = jnp.concatenate([jnp.zeros((BAND,), jnp.int32), query_labels])
        return local_attention(query_seg[shard_index], band_keys, band_values, query_labels, key_labels, shard_index, BAND)
    local = lax.map(shard_attention, jnp.arange(N_SEQ).astype(jnp.int32))
    gate = jax.nn.sigmoid(mem_gate)[None, None, :, None]
    attended = (gate * readouts + (1.0 - gate) * local).astype(jnp.bfloat16).reshape(TOKENS, HEAD_TOTAL * HEAD_DIM)
    return jnp.dot(attended, out_weight, preferred_element_type=jnp.float32).astype(jnp.bfloat16)
```

```python
import functools
import math

import jax
import jax.numpy as jnp
from jax import lax
from jax.experimental import pallas as pl
from jax.experimental.pallas import tpu as pltpu
from jax.sharding import PartitionSpec as P

BAND = 512
SPAN_DEV = 2
PAD = 8
MASKED = -1e30


SMEM = pl.BlockSpec(memory_space=pltpu.SMEM)


def phi(x):
    return jnp.where(x > 0, x + 1.0, jnp.exp(jnp.minimum(x, 0.0)))


def split(x):
    high = x.astype(jnp.bfloat16)
    return high, (x - high.astype(jnp.float32)).astype(jnp.bfloat16)


def params(limit_mib, semantics=None):
    return pltpu.CompilerParams(vmem_limit_bytes=limit_mib << 20, dimension_semantics=semantics)


def cost(flops, moved):
    return pl.CostEstimate(flops=int(flops), bytes_accessed=int(moved), transcendentals=0)


def state_kernel(keys_ref, values_ref, state_ref):
    feats = phi(keys_ref[...].astype(jnp.float32))
    high, low = split(feats)
    vals = values_ref[...]
    dims = (((0,), (0,)), ((), ()))
    state = lax.dot_general(high, vals, dims, preferred_element_type=jnp.float32)
    state += lax.dot_general(low, vals, dims, preferred_element_type=jnp.float32)
    width = state.shape[0]
    state_ref[0, :width, :] = state
    total = jnp.sum(feats, axis=0, keepdims=True)
    state_ref[0, width:, :] = jnp.broadcast_to(total, (PAD, total.shape[1]))


def make_state(keys, values, heads, width):
    rows = keys.shape[0]
    col = pl.BlockSpec((rows, width), lambda h: (0, h))
    return pl.pallas_call(
        state_kernel,
        grid=(heads,),
        in_specs=[col, col],
        out_specs=pl.BlockSpec((1, width + PAD, width), lambda h: (h, 0, 0)),
        out_shape=jax.ShapeDtypeStruct((heads, width + PAD, width), jnp.float32),
        compiler_params=params(16),
        cost_estimate=cost(3e9, 2 * keys.size * 2),
        name="state",
    )(keys, values)


def fold_kernel(distance, me_ref, decay_ref, memory_ref, got_ref, state_ref, out_ref, send_ref):
    me = me_ref[0]
    for head in range(state_ref.shape[0]):
        factor = 1.0
        for back in range(1, distance):
            factor = factor * decay_ref[jnp.maximum(me - back, 0), head]
        memory = memory_ref[head] + factor * got_ref[head]
        out_ref[head] = memory
        send_ref[head] = state_ref[head] + decay_ref[me, head] * memory


def fold_first_kernel(me_ref, decay_ref, got_ref, state_ref, send_ref):
    me = me_ref[0]
    for head in range(state_ref.shape[0]):
        send_ref[head] = state_ref[head] + decay_ref[me, head] * got_ref[head]


def prefix(state, decay, me, size):
    shape = jax.ShapeDtypeStruct(state.shape, state.dtype)
    memory, send = None, state
    distance = 1
    while distance < size:
        route = [(i, i + distance) for i in range(size - distance)]
        got = lax.ppermute(send, "seq", route)
        last = 2 * distance >= size
        full = pl.BlockSpec(memory_space=pltpu.VMEM)
        if memory is None:
            memory = got
            if not last:
                send = pl.pallas_call(
                    fold_first_kernel,
                    in_specs=[SMEM, SMEM, full, full],
                    out_specs=full,
                    out_shape=shape,
                    compiler_params=params(8),
                    cost_estimate=cost(1e8, 3 * state.size * 4),
                    name="fold_first",
                )(me, decay, got, state)
        else:
            memory, send = pl.pallas_call(
                functools.partial(fold_kernel, distance),
                in_specs=[SMEM, SMEM, full, full, full],
                out_specs=[full, full],
                out_shape=[shape, shape],
                compiler_params=params(8),
                cost_estimate=cost(1e8, 5 * state.size * 4),
                name="fold",
            )(me, decay, memory, got, state)
        distance *= 2
    return memory


def local_kernel(half, block, me_ref, spans_ref, q_ref, kp_ref, vp_ref, k_ref, v_ref, out_ref):
    me = me_ref[0]
    rows, width = q_ref.shape
    factor = math.log2(math.e) / math.sqrt(width)
    origin = (me * SPAN_DEV + half) * rows
    first = spans_ref[me * SPAN_DEV + half, 0] - origin
    end = spans_ref[me * SPAN_DEV + half, 1] - origin
    shift = 0 if half else jnp.where(me > 0, 0, rows + 1)
    for start in range(0, rows, block):
        query = q_ref[start : start + block, :]
        dims = (((1,), (1,)), ((), ()))
        before = lax.dot_general(query, kp_ref[start:, :], dims, preferred_element_type=jnp.float32)
        own = lax.dot_general(query, k_ref[...], dims, preferred_element_type=jnp.float32)
        row = start + lax.broadcasted_iota(jnp.int32, (block, 1), 0)
        limit = jnp.where((row >= first) & (row < end), end - 1, row)
        col = lax.broadcasted_iota(jnp.int32, before.shape, 1) + start
        before = jnp.where(col > row + shift, before, MASKED)
        col = lax.broadcasted_iota(jnp.int32, own.shape, 1)
        own = jnp.where(col <= limit, own, MASKED)
        top = jnp.maximum(
            jnp.max(before, axis=1, keepdims=True), jnp.max(own, axis=1, keepdims=True)
        )
        before = jnp.exp2((before - top) * factor)
        own = jnp.exp2((own - top) * factor)
        total = jnp.sum(before, axis=1, keepdims=True) + jnp.sum(own, axis=1, keepdims=True)
        mixed = jnp.dot(
            before.astype(jnp.bfloat16), vp_ref[start:, :], preferred_element_type=jnp.float32
        )
        mixed += jnp.dot(own.astype(jnp.bfloat16), v_ref[...], preferred_element_type=jnp.float32)
        out_ref[start : start + block, :] = mixed / total


def local_half(half, queries, keys, values, prev_keys, prev_values, spans, me, heads, width):
    rows = queries.shape[0] // SPAN_DEV
    here = pl.BlockSpec((rows, width), lambda h: (half, h))
    before = pl.BlockSpec((rows, width), lambda h: (0, h))
    return pl.pallas_call(
        functools.partial(local_kernel, half, min(256, rows)),
        grid=(heads,),
        in_specs=[SMEM, SMEM, here, before, before, here, here],
        out_specs=before,
        out_shape=jax.ShapeDtypeStruct((rows, heads * width), jnp.float32),
        compiler_params=params(32),
        cost_estimate=cost(1.5e10, 6 * rows * heads * width * 2),
        name="local",
    )(me, spans, queries, prev_keys, prev_values, keys, values)


def readout_kernel(gate_ref, q_ref, local_ref, memory_ref, out_ref):
    heads = memory_ref.shape[0]
    width = memory_ref.shape[2]
    for head in range(heads):
        cols = slice(head * width, (head + 1) * width)
        feats = phi(q_ref[:, cols].astype(jnp.float32))
        q_high, q_low = split(feats)
        memory = memory_ref[head, :width, :]
        m_high, m_low = split(memory)
        left = jnp.concatenate([q_high, q_low], axis=1)
        right = jnp.concatenate(
            [
                jnp.concatenate([m_high, m_low], axis=1),
                jnp.concatenate([m_high, jnp.zeros_like(m_low)], axis=1),
            ],
            axis=0,
        )
        both = jnp.dot(left, right, preferred_element_type=jnp.float32)
        numer = both[:, :width] + both[:, width:]
        norm = memory_ref[head, width : width + 1, :]
        denom = jnp.sum(feats * norm, axis=1, keepdims=True) + 1.0
        gate = 1.0 / (1.0 + jnp.exp(jnp.full((1, width), -gate_ref[head], jnp.float32)))
        out = gate * (numer / denom) + (1.0 - gate) * local_ref[:, cols]
        out_ref[:, cols] = out.astype(jnp.bfloat16)


def readout(chunk_index, chunk, queries, local, local_index, memory, gate):
    cols = queries.shape[1]
    whole = pl.BlockSpec(memory.shape, lambda i: (0, 0, 0))
    return pl.pallas_call(
        readout_kernel,
        grid=(1,),
        in_specs=[
            SMEM,
            pl.BlockSpec((chunk, cols), lambda i: (chunk_index, 0)),
            pl.BlockSpec((chunk, cols), lambda i: (local_index, 0)),
            whole,
        ],
        out_specs=pl.BlockSpec((chunk, cols), lambda i: (0, 0)),
        out_shape=jax.ShapeDtypeStruct((chunk, cols), jnp.bfloat16),
        compiler_params=params(16),
        cost_estimate=cost(2e9, chunk * cols * 8),
        name="readout",
    )(gate, queries, local, memory)


def project_kernel(parts, *refs):
    xs, ws, out_ref = refs[1 : 1 + parts], refs[1 + parts : 1 + 2 * parts], refs[-1]
    acc = jnp.dot(xs[0][...], ws[0][...], preferred_element_type=jnp.float32)
    for x_ref, w_ref in zip(xs[1:], ws[1:]):
        acc += jnp.dot(x_ref[...], w_ref[...], preferred_element_type=jnp.float32)
    out_ref[...] = acc.astype(out_ref.dtype)


def project(chunk_index, total_rows, xs, ws, head_index, out):
    parts = len(xs)
    chunk, depth = xs[0].shape
    columns = ws[1].shape[1]
    tile = min(256, columns)
    tiles = columns // tile
    x_spec = pl.BlockSpec((chunk, depth), lambda n, h: (0, 0))
    own = pl.BlockSpec((depth, tile), lambda n, h: (0, h[0] * tiles + n))
    other = pl.BlockSpec((depth, tile), lambda n, h: (0, n))
    in_specs = [x_spec] * parts + [own] + [other] * (parts - 1)
    operands = [head_index, *xs, *ws]
    aliases = {}
    if out is not None:
        in_specs.append(pl.BlockSpec(memory_space=pl.ANY))
        aliases = {len(operands): 0}
        operands.append(out)
    return pl.pallas_call(
        functools.partial(project_kernel, parts),
        grid_spec=pltpu.PrefetchScalarGridSpec(
            num_scalar_prefetch=1,
            grid=(tiles,),
            in_specs=in_specs,
            out_specs=pl.BlockSpec((chunk, tile), lambda n, h: (chunk_index, n)),
        ),
        out_shape=jax.ShapeDtypeStruct((total_rows, columns), jnp.bfloat16),
        input_output_aliases=aliases,
        compiler_params=params(24),
        cost_estimate=cost(2 * chunk * depth * parts * columns, parts * depth * columns * 2),
        name="project",
    )(*operands)


def swap(x, axis, mask):
    size = lax.axis_size(axis)
    return lax.ppermute(x, axis, [(i, i ^ mask) for i in range(size)])


def body(queries, keys, values, span_bounds, mem_decay, mem_gate, out_weight):
    seg_rows = queries.shape[0]
    heads = mem_gate.shape[0]
    width = queries.shape[1] // heads
    seq_size, head_size = lax.axis_size("seq"), lax.axis_size("head")
    assert head_size & (head_size - 1) == 0 and seg_rows == BAND * SPAN_DEV
    seq_index, head_index = lax.axis_index("seq"), lax.axis_index("head")
    me = seq_index.astype(jnp.int32).reshape(1)
    head_at = head_index.astype(jnp.int32).reshape(1)
    columns = out_weight.shape[1] // head_size

    weights = {0: out_weight}
    for mask in sorted(range(1, head_size), reverse=True):
        block = lax.dynamic_slice_in_dim(out_weight, (head_index ^ mask) * columns, columns, 1)
        weights[mask] = swap(block, "head", mask)

    halo = jnp.stack([keys[seg_rows - BAND :], values[seg_rows - BAND :]])
    halo = lax.ppermute(halo, "seq", [(i, i + 1) for i in range(seq_size - 1)])

    state = make_state(keys, values, heads, width)
    memory = prefix(state, mem_decay, me, seq_size)

    locals_ = {}
    locals_[1] = local_half(1, queries, keys, values, keys, values, span_bounds, me, heads, width)
    locals_[0] = local_half(
        0, queries, keys, values, halo[0], halo[1], span_bounds, me, heads, width
    )

    chunk = 256
    per_half = BAND // chunk
    out = None
    for half in (1, 0):
        for part in range(per_half):
            index = half * per_half + part
            own = readout(index, chunk, queries, locals_[half], part, memory, mem_gate)
            xs = {0: own}
            mask = head_size // 2
            while mask:
                xs.update({at ^ mask: swap(x, "head", mask) for at, x in list(xs.items())})
                mask //= 2
            order = range(head_size)
            out = project(
                index,
                seg_rows,
                [xs[i] for i in order],
                [weights[i] for i in order],
                head_at,
                out,
            )
    return out


def solution(mesh):
    return jax.shard_map(
        body,
        mesh=mesh,
        in_specs=(
            P("seq", "head"),
            P("seq", "head"),
            P("seq", "head"),
            P(),
            P(None, "head"),
            P("head"),
            P("head", None),
        ),
        out_specs=P("seq", "head"),
        check_vma=False,
    )
```

```python
import functools
import math

import jax
import jax.numpy as jnp
from jax import lax
from jax.experimental import pallas as pl
from jax.experimental.pallas import tpu as pltpu
from jax.sharding import PartitionSpec as P

BAND = 512
SPAN_DEV = 2
PAD = 8
SEND_PAD = 16
MASKED = -1e30
BLOCK = 256


SMEM = pl.BlockSpec(memory_space=pltpu.SMEM)
VMEM = pl.BlockSpec(memory_space=pltpu.VMEM)
HBM = pl.BlockSpec(memory_space=pltpu.HBM)
F32, BF16 = jnp.float32, jnp.bfloat16


def phi(x):
    return jnp.where(x > 0, x + 1.0, jnp.exp(jnp.minimum(x, 0.0)))


def split(x):
    high = x.astype(BF16)
    return high, (x - high.astype(F32)).astype(BF16)


def params(limit_mib):
    return pltpu.CompilerParams(vmem_limit_bytes=limit_mib << 20)


def cost(flops, moved):
    return pl.CostEstimate(flops=int(flops), bytes_accessed=int(moved), transcendentals=0)


def pack(ref, head, memory, total):
    width = memory.shape[0]
    ref[head, :width, :] = memory.astype(BF16)
    high, low = split(total)
    row = lax.broadcasted_iota(jnp.int32, (SEND_PAD, total.shape[1]), 0)
    both = jnp.where(row == 0, high.astype(F32), jnp.where(row == 1, low.astype(F32), 0.0))
    ref[head, width:, :] = both.astype(BF16)


def unpack(ref, head):
    width = ref.shape[2]
    memory = ref[head, :width, :].astype(F32)
    total = jnp.sum(ref[head, width:, :].astype(F32), axis=0, keepdims=True)
    return memory, total


def store(ref, head, memory, total):
    width = memory.shape[0]
    ref[head, :width, :] = memory
    ref[head, width:, :] = jnp.broadcast_to(total, (PAD, total.shape[1]))


def load(ref, head):
    width = ref.shape[2]
    return ref[head, :width, :], ref[head, width : width + 1, :]


def state_kernel(k_hbm, v_hbm, state_ref, send_ref, *refs):
    *tails, k_buf, v_buf, sems = refs
    heads, width = state_ref.shape[0], state_ref.shape[2]
    rows = k_buf.shape[0]
    steps = rows // BLOCK
    copies = []
    for step in range(steps):
        at = pl.ds(step * BLOCK, BLOCK)
        pair = [
            pltpu.make_async_copy(src.at[at], buf.at[at], sems.at[which, step])
            for which, (src, buf) in enumerate(((k_hbm, k_buf), (v_hbm, v_buf)))
        ]
        for copy in pair:
            copy.start()
        copies.append(pair)
    for step in range(steps):
        for copy in copies[step]:
            copy.wait()
        at = slice(step * BLOCK, (step + 1) * BLOCK)
        for head in range(heads):
            cols = slice(head * width, (head + 1) * width)
            feats = phi(k_buf[at, cols].astype(F32))
            high, low = split(feats)
            vals = v_buf[at, cols]
            dims = (((0,), (0,)), ((), ()))
            memory = lax.dot_general(high, vals, dims, preferred_element_type=F32)
            memory += lax.dot_general(low, vals, dims, preferred_element_type=F32)
            total = jnp.sum(feats, axis=0, keepdims=True)
            if step:
                had, had_total = load(state_ref, head)
                memory, total = memory + had, total + had_total
            store(state_ref, head, memory, total)
            if step == steps - 1:
                pack(send_ref, head, memory, total)
    half = BAND // 2
    tails[0][...] = k_buf[rows - BAND : rows - half, :]
    tails[1][...] = k_buf[rows - half :, :]
    tails[2][...] = v_buf[rows - BAND :, :]


def make_state(keys, values, heads, width):
    rows, cols = keys.shape
    steps = rows // BLOCK
    half = jax.ShapeDtypeStruct((BAND // 2, cols), BF16)
    return pl.pallas_call(
        state_kernel,
        in_specs=[HBM, HBM],
        out_specs=[VMEM] * 5,
        out_shape=[
            jax.ShapeDtypeStruct((heads, width + PAD, width), F32),
            jax.ShapeDtypeStruct((heads, width + SEND_PAD, width), BF16),
            half,
            half,
            jax.ShapeDtypeStruct((BAND, cols), BF16),
        ],
        scratch_shapes=[
            pltpu.VMEM((rows, cols), BF16),
            pltpu.VMEM((rows, cols), BF16),
            pltpu.SemaphoreType.DMA((2, steps)),
        ],
        compiler_params=params(24),
        cost_estimate=cost(1e10, 4 * keys.size * 2),
        name="state",
    )(keys, values)


def fold(distance, me, decay_ref, head, memory, group, got):
    upper = (me & distance) != 0
    base = me & ~(distance - 1)
    above = base | distance
    through, before = 1.0, 1.0
    for step in range(distance):
        through = through * decay_ref[above + step, head]
        if step < distance - 1:
            factor = decay_ref[base + step, head]
            before = before * jnp.where(base + step < me, factor, 1.0)
    before = jnp.where(upper, before, 0.0)
    low, high = jnp.where(upper, 1.0, through), jnp.where(upper, through, 1.0)
    both = [low * mine + high * theirs for mine, theirs in zip(group, got)]
    if memory is None:
        memory = [before * theirs for theirs in got]
    else:
        memory = [mine + before * theirs for mine, theirs in zip(memory, got)]
    return memory, both


def fold_kernel(distance, me_ref, decay_ref, *refs):
    *inner, got_ref, group_ref, memory_ref, total_ref, send_ref = refs
    me = me_ref[0]
    for head in range(group_ref.shape[0]):
        memory = load(inner[0], head) if inner else None
        memory, both = fold(
            distance, me, decay_ref, head, memory, load(group_ref, head), unpack(got_ref, head)
        )
        store(memory_ref, head, *memory)
        store(total_ref, head, *both)
        pack(send_ref, head, *both)


def local_kernel(half, me_ref, spans_ref, q_hbm, k_hbm, v_hbm, *refs):
    *halo, out_ref, q_buf, k_buf, v_buf, kp_buf, vp_buf, sems = refs
    me = me_ref[0]
    heads, rows, width = q_buf.shape
    here, before = pl.ds(half * rows, rows), pl.ds((half - 1) * rows, rows)

    def copies(head):
        cols = pl.ds(head * width, width)
        table = [(q_hbm, here, q_buf), (k_hbm, here, k_buf), (v_hbm, here, v_buf)]
        if half:
            table += [(k_hbm, before, kp_buf), (v_hbm, before, vp_buf)]
        return [
            pltpu.make_async_copy(src.at[at, cols], buf.at[head], sems.at[which, head])
            for which, (src, at, buf) in enumerate(table)
        ]

    for head in range(heads):
        for copy in copies(head):
            copy.start()
    if not half:
        for head in range(heads):
            cols = slice(head * width, (head + 1) * width)
            kp_buf[head, : rows // 2, :] = halo[0][:, cols]
            kp_buf[head, rows // 2 :, :] = halo[1][:, cols]
            vp_buf[head] = halo[2][:, cols]

    factor = math.log2(math.e) / math.sqrt(width)
    origin = (me * SPAN_DEV + half) * rows
    first = spans_ref[me * SPAN_DEV + half, 0] - origin
    end = spans_ref[me * SPAN_DEV + half, 1] - origin
    shift = 0 if half else jnp.where(me > 0, 0, rows + 1)
    for head in range(heads):
        for copy in copies(head):
            copy.wait()
        for start in range(0, rows, BLOCK):
            query = q_buf[head, start : start + BLOCK, :]
            dims = (((1,), (1,)), ((), ()))
            prev = lax.dot_general(query, kp_buf[head, start:, :], dims, preferred_element_type=F32)
            own = lax.dot_general(query, k_buf[head], dims, preferred_element_type=F32)
            row = start + lax.broadcasted_iota(jnp.int32, (BLOCK, 1), 0)
            limit = jnp.where((row >= first) & (row < end), end - 1, row)
            col = lax.broadcasted_iota(jnp.int32, prev.shape, 1) + start
            prev = jnp.where(col > row + shift, prev, MASKED)
            col = lax.broadcasted_iota(jnp.int32, own.shape, 1)
            own = jnp.where(col <= limit, own, MASKED)
            top = jnp.maximum(
                jnp.max(prev, axis=1, keepdims=True), jnp.max(own, axis=1, keepdims=True)
            )
            prev = jnp.exp2((prev - top) * factor)
            own = jnp.exp2((own - top) * factor)
            total = jnp.sum(prev, axis=1, keepdims=True) + jnp.sum(own, axis=1, keepdims=True)
            mixed = jnp.dot(prev.astype(BF16), vp_buf[head, start:, :], preferred_element_type=F32)
            mixed += jnp.dot(own.astype(BF16), v_buf[head], preferred_element_type=F32)
            out_ref[start : start + BLOCK, head * width : (head + 1) * width] = mixed / total


def local_half(half, queries, keys, values, halo, spans, me, heads, width):
    rows = queries.shape[0] // SPAN_DEV
    buf = pltpu.VMEM((heads, rows, width), BF16)
    halo = list(halo)
    return pl.pallas_call(
        functools.partial(local_kernel, half),
        in_specs=[SMEM, SMEM, HBM, HBM, HBM] + [VMEM] * len(halo),
        out_specs=VMEM,
        out_shape=jax.ShapeDtypeStruct((rows, heads * width), F32),
        scratch_shapes=[buf] * 5 + [pltpu.SemaphoreType.DMA((5, heads))],
        compiler_params=params(32),
        cost_estimate=cost(1.5e10, 6 * rows * heads * width * 2),
    )(me, spans, queries, keys, values, *halo)


def readout_kernel(distance, me_ref, decay_ref, gate_ref, q_ref, local_ref, *refs):
    *inner, got_ref, group_ref, out_ref = refs
    me = me_ref[0]
    heads, width = group_ref.shape[0], group_ref.shape[2]
    for head in range(heads):
        memory = load(inner[0], head) if inner else None
        (memory, norm), unused = fold(
            distance, me, decay_ref, head, memory, load(group_ref, head), unpack(got_ref, head)
        )
        cols = slice(head * width, (head + 1) * width)
        feats = phi(q_ref[:, cols].astype(F32))
        q_high, q_low = split(feats)
        m_high, m_low = split(memory)
        left = jnp.concatenate([q_high, q_low], axis=1)
        right = jnp.concatenate(
            [
                jnp.concatenate([m_high, m_low], axis=1),
                jnp.concatenate([m_high, jnp.zeros_like(m_low)], axis=1),
            ],
            axis=0,
        )
        both = jnp.dot(left, right, preferred_element_type=F32)
        numer = both[:, :width] + both[:, width:]
        denom = jnp.sum(feats * norm, axis=1, keepdims=True) + 1.0
        gate = 1.0 / (1.0 + jnp.exp(jnp.full((1, width), -gate_ref[head], F32)))
        out = gate * (numer / denom) + (1.0 - gate) * local_ref[:, cols]
        out_ref[:, cols] = out.astype(BF16)


def readout(distance, start, rows, queries, local, memory, me, decay, gate):
    cols = queries.shape[1]
    chunk = lambda at: pl.BlockSpec((rows, cols), lambda i: (at // rows, 0))
    whole = [pl.BlockSpec(m.shape, lambda i: (0, 0, 0)) for m in memory]
    return pl.pallas_call(
        functools.partial(readout_kernel, distance),
        grid=(1,),
        in_specs=[SMEM, SMEM, SMEM, chunk(start), chunk(start % BAND), *whole],
        out_specs=chunk(0),
        out_shape=jax.ShapeDtypeStruct((rows, cols), BF16),
        compiler_params=params(16),
        cost_estimate=cost(2e9, rows * cols * 8),
    )(me, decay, gate, queries, local, *memory)


def project_kernel(shared, odd_ref, *refs):
    xs, ws, out_ref = refs[: len(shared)], list(refs[len(shared) :]), refs[-1]
    columns = out_ref.shape[1]
    odd = odd_ref[0]
    lefts, rights = [], []
    for x_ref, is_shared in zip(xs, shared):
        if is_shared:
            unit = x_ref.shape[1] // 4
            most = x_ref[:, pl.ds(pl.multiple_of(odd * unit, unit), 3 * unit)]
            rest = x_ref[:, pl.ds(pl.multiple_of((1 - odd) * 3 * unit, unit), unit)]
            lefts.append(jnp.concatenate([most, rest], axis=1))
            rights.append((ws.pop(0), ws.pop(0)))
        else:
            lefts.append(x_ref[...])
            rights.append((ws.pop(0),))
    tile = 256
    for start in range(0, columns, tile):
        at = slice(start, start + tile)
        acc = None
        for left, right in zip(lefts, rights):
            block = [w_ref[:, at] for w_ref in right]
            block = jnp.concatenate(block, axis=0) if len(block) > 1 else block[0]
            term = jnp.dot(left, block, preferred_element_type=F32)
            acc = term if acc is None else acc + term
        out_ref[:, at] = acc.astype(out_ref.dtype)


def project(start, total_rows, xs, weights, odd, out):
    rows = xs[0].shape[0]
    flat = [w for ws in weights for w in ws]
    columns = flat[0].shape[1]
    whole = lambda a: pl.BlockSpec(a.shape, lambda i: (0, 0))
    operands = [odd, *xs, *flat]
    in_specs = [SMEM] + [whole(a) for a in operands[1:]]
    aliases = {}
    if out is not None:
        in_specs.append(pl.BlockSpec(memory_space=pl.ANY))
        aliases = {len(operands): 0}
        operands.append(out)
    depth = sum(w.shape[0] for w in flat)
    return pl.pallas_call(
        functools.partial(project_kernel, [len(ws) > 1 for ws in weights]),
        grid=(1,),
        in_specs=in_specs,
        out_specs=pl.BlockSpec((rows, columns), lambda i: (start // rows, 0)),
        out_shape=jax.ShapeDtypeStruct((total_rows, columns), BF16),
        input_output_aliases=aliases,
        compiler_params=params(24),
        cost_estimate=cost(2 * rows * depth * columns, depth * columns * 2),
    )(*operands)


def swap(x, axis, mask):
    size = lax.axis_size(axis)
    return lax.ppermute(x, axis, [(i, i ^ mask) for i in range(size)])


CHUNKS = ((512, 512), (0, 256), (256, 256))


def body(queries, keys, values, span_bounds, mem_decay, mem_gate, out_weight):
    seg_rows = queries.shape[0]
    heads = mem_gate.shape[0]
    width = queries.shape[1] // heads
    seq_size, head_size = lax.axis_size("seq"), lax.axis_size("head")
    assert head_size & (head_size - 1) == 0 and seg_rows == BAND * SPAN_DEV
    assert seq_size & (seq_size - 1) == 0 and seq_size > 1
    seq_index, head_index = lax.axis_index("seq"), lax.axis_index("head")
    me = seq_index.astype(jnp.int32).reshape(1)
    odd = me & 1
    depth = out_weight.shape[0]
    unit = depth // 4
    columns = out_weight.shape[1] // head_size

    weights = {}
    last = out_weight
    for mask in sorted(range(1, head_size), reverse=True):
        shared = mask > 1
        row, rows = (odd[0] * unit, 3 * unit) if shared else (0, depth)
        source, _ = lax.optimization_barrier((out_weight, last))
        block = lax.dynamic_slice(source, (row, (head_index ^ mask) * columns), (rows, columns))
        last = block[:8, :128]
        weights[mask] = (swap(block, "head", mask),)
    for mask in weights:
        if mask > 1:
            most = weights[mask][0]
            part = lax.dynamic_slice_in_dim(most, odd[0] * 2 * unit, unit, 0)
            weights[mask] = (most, swap(part, "seq", 1))
    weights[0] = (lax.dynamic_slice_in_dim(out_weight, head_index * columns, columns, 1),)

    state, send, *tails = make_state(keys, values, heads, width)
    halo = []
    for tail in tails:
        halo.append(lax.ppermute(tail, "seq", [(i, i + 1) for i in range(seq_size - 1)]))

    inner, group, distance = [], state, 1
    while True:
        got = swap(send, "seq", distance)
        if 2 * distance >= seq_size:
            break
        shape = jax.ShapeDtypeStruct(state.shape, F32)
        operands = [me, mem_decay, *inner, got, group]
        memory, group, send = pl.pallas_call(
            functools.partial(fold_kernel, distance),
            in_specs=[SMEM, SMEM] + [VMEM] * (len(operands) - 2),
            out_specs=[VMEM] * 3,
            out_shape=[shape, shape, jax.ShapeDtypeStruct(send.shape, BF16)],
            compiler_params=params(16),
            cost_estimate=cost(1e9, 5 * state.size * 4),
        )(*operands)
        inner, distance = [memory], 2 * distance
    memory = [*inner, got, group]

    locals_ = {}
    for half in (1, 0):
        locals_[half] = local_half(
            half, queries, keys, values, () if half else halo,
            span_bounds, me, heads, width,
        )

    out = None
    for start, rows in CHUNKS:
        own = readout(
            distance, start, rows, queries,
            locals_[start // BAND], memory, me, mem_decay, mem_gate,
        )
        xs = {0: own}
        mask = head_size // 2
        while mask:
            for at, x in list(xs.items()):
                xs[at ^ mask] = swap(x, "head", mask)
            mask //= 2
        order = range(head_size)
        out = project(
            start, seg_rows,
            [xs[i] for i in order], [weights[i] for i in order], odd, out,
        )
    return out


def solution(mesh):
    return jax.shard_map(
        body,
        mesh=mesh,
        in_specs=(
            P("seq", "head"),
            P("seq", "head"),
            P("seq", "head"),
            P(),
            P(None, "head"),
            P("head"),
            P("head", None),
        ),
        out_specs=P("seq", "head"),
        check_vma=False,
    )
```

```python
import functools
import math

import jax
import jax.numpy as jnp
from jax import lax
from jax.experimental import pallas as pl
from jax.experimental.pallas import tpu as pltpu
from jax.sharding import PartitionSpec as P

BAND = 512
SPAN_DEV = 2
PAD = 8
SEND_PAD = 16
MASKED = -1e30
BLOCK = 256
TILE = 256


SMEM = pl.BlockSpec(memory_space=pltpu.SMEM)
VMEM = pl.BlockSpec(memory_space=pltpu.VMEM)
HBM = pl.BlockSpec(memory_space=pltpu.HBM)
F32, BF16 = jnp.float32, jnp.bfloat16


def phi(x):
    return jnp.where(x > 0, x + 1.0, jnp.exp(jnp.minimum(x, 0.0)))


def split(x):
    high = x.astype(BF16)
    return high, (x - high.astype(F32)).astype(BF16)


def params(limit_mib):
    return pltpu.CompilerParams(vmem_limit_bytes=limit_mib << 20)


def in_hbm(x):
    return pltpu.with_memory_space_constraint(x, pltpu.HBM)


def in_vmem(x):
    return pltpu.with_memory_space_constraint(x, pltpu.VMEM)


def cost(flops, moved):
    return pl.CostEstimate(flops=int(flops), bytes_accessed=int(moved), transcendentals=0)


def pack(ref, head, memory, total):
    width = memory.shape[0]
    ref[head, :width, :] = memory.astype(BF16)
    high, low = split(total)
    row = lax.broadcasted_iota(jnp.int32, (SEND_PAD, total.shape[1]), 0)
    both = jnp.where(row == 0, high.astype(F32), jnp.where(row == 1, low.astype(F32), 0.0))
    ref[head, width:, :] = both.astype(BF16)


def unpack(ref, head):
    width = ref.shape[2]
    memory = ref[head, :width, :].astype(F32)
    total = jnp.sum(ref[head, width:, :].astype(F32), axis=0, keepdims=True)
    return memory, total


def store(ref, head, memory, total):
    width = memory.shape[0]
    ref[head, :width, :] = memory
    ref[head, width:, :] = jnp.broadcast_to(total, (PAD, total.shape[1]))


def load(ref, head):
    width = ref.shape[2]
    return ref[head, :width, :], ref[head, width : width + 1, :]


def slice_copies(slices, at_ref, w_hbm, blocks, sems):
    odd, head_index = at_ref[0], at_ref[1]
    copies = []
    for number, (mask, rows) in enumerate(slices):
        columns = blocks[number].shape[1]
        unit = w_hbm.shape[0] // 4
        row = pl.multiple_of(odd * unit, unit) if rows < w_hbm.shape[0] else 0
        col = pl.multiple_of((head_index ^ mask) * columns, columns)
        source = w_hbm.at[pl.ds(row, rows), pl.ds(col, columns)]
        copies.append(pltpu.make_async_copy(source, blocks[number], sems.at[number]))
    return copies


def slice_kernel(slices, at_ref, w_hbm, *refs):
    *blocks, sems = refs
    copies = slice_copies(slices, at_ref, w_hbm, blocks, sems)
    for copy in copies:
        copy.start()
    for copy in copies:
        copy.wait()


def make_slices(out_weight, slices, at, columns):
    return pl.pallas_call(
        functools.partial(slice_kernel, slices),
        in_specs=[SMEM, HBM],
        out_specs=[VMEM] * len(slices),
        out_shape=[pltpu.VMEM((rows, columns), BF16) for _, rows in slices],
        scratch_shapes=[pltpu.SemaphoreType.DMA((len(slices),))],
        compiler_params=params(8),
        cost_estimate=cost(1e9, 2 * columns * sum(rows for _, rows in slices) * 2),
        name="slices",
    )(at, in_hbm(out_weight))


def part_kernel(odd_ref, most_ref, part_ref):
    unit = part_ref.shape[0]
    part_ref[...] = most_ref[pl.ds(pl.multiple_of(odd_ref[0] * 2 * unit, unit), unit), :]


def make_part(most, odd, unit):
    return pl.pallas_call(
        part_kernel,
        in_specs=[SMEM, VMEM],
        out_specs=VMEM,
        out_shape=pltpu.VMEM((unit, most.shape[1]), BF16),
        compiler_params=params(4),
        cost_estimate=cost(1e8, 4 * unit * most.shape[1]),
        name="part",
    )(odd, in_vmem(most))


def state_kernel(slices, at_ref, k_hbm, v_hbm, w_hbm, state_ref, send_ref, *refs):
    *outs, k_buf, v_buf, sems, w_sems = refs
    tails, blocks = outs[:3], outs[3:]
    heads, width = state_ref.shape[0], state_ref.shape[2]
    rows = k_buf.shape[0]
    steps = rows // BLOCK
    copies = []
    for step in range(steps):
        at = pl.ds(step * BLOCK, BLOCK)
        pair = [
            pltpu.make_async_copy(src.at[at], buf.at[at], sems.at[which, step])
            for which, (src, buf) in enumerate(((k_hbm, k_buf), (v_hbm, v_buf)))
        ]
        for copy in pair:
            copy.start()
        copies.append(pair)
    moves = slice_copies(slices, at_ref, w_hbm, blocks, w_sems)
    for copy in moves:
        copy.start()
    for step in range(steps):
        for copy in copies[step]:
            copy.wait()
        at = slice(step * BLOCK, (step + 1) * BLOCK)
        for head in range(heads):
            cols = slice(head * width, (head + 1) * width)
            feats = phi(k_buf[at, cols].astype(F32))
            high, low = split(feats)
            vals = v_buf[at, cols]
            dims = (((0,), (0,)), ((), ()))
            memory = lax.dot_general(high, vals, dims, preferred_element_type=F32)
            memory += lax.dot_general(low, vals, dims, preferred_element_type=F32)
            total = jnp.sum(feats, axis=0, keepdims=True)
            if step:
                had, had_total = load(state_ref, head)
                memory, total = memory + had, total + had_total
            store(state_ref, head, memory, total)
            if step == steps - 1:
                pack(send_ref, head, memory, total)
    half = BAND // 2
    tails[0][...] = k_buf[rows - BAND : rows - half, :]
    tails[1][...] = k_buf[rows - half :, :]
    tails[2][...] = v_buf[rows - BAND :, :]
    for copy in moves:
        copy.wait()


def make_state(keys, values, out_weight, slices, at, heads, width, columns):
    rows, cols = keys.shape
    steps = rows // BLOCK
    half = pltpu.VMEM((BAND // 2, cols), BF16)
    return pl.pallas_call(
        functools.partial(state_kernel, slices),
        in_specs=[SMEM, HBM, HBM, HBM],
        out_specs=[VMEM] * (5 + len(slices)),
        out_shape=[
            pltpu.VMEM((heads, width + PAD, width), F32),
            pltpu.VMEM((heads, width + SEND_PAD, width), BF16),
            half,
            half,
            pltpu.VMEM((BAND, cols), BF16),
            *(pltpu.VMEM((rows_, columns), BF16) for _, rows_ in slices),
        ],
        scratch_shapes=[
            pltpu.VMEM((rows, cols), BF16),
            pltpu.VMEM((rows, cols), BF16),
            pltpu.SemaphoreType.DMA((2, steps)),
            pltpu.SemaphoreType.DMA((len(slices),)),
        ],
        compiler_params=params(24),
        cost_estimate=cost(1e10, 4 * keys.size * 2),
        name="state",
    )(at, in_hbm(keys), in_hbm(values), in_hbm(out_weight))


def fold(distance, me, decay_ref, head, memory, group, got):
    upper = (me & distance) != 0
    base = me & ~(distance - 1)
    above = base | distance
    through, before = 1.0, 1.0
    for step in range(distance):
        through = through * decay_ref[head, above + step]
        if step < distance - 1:
            factor = decay_ref[head, base + step]
            before = before * jnp.where(base + step < me, factor, 1.0)
    before = jnp.where(upper, before, 0.0)
    low, high = jnp.where(upper, 1.0, through), jnp.where(upper, through, 1.0)
    both = [low * mine + high * theirs for mine, theirs in zip(group, got)]
    if memory is None:
        memory = [before * theirs for theirs in got]
    else:
        memory = [mine + before * theirs for mine, theirs in zip(memory, got)]
    return memory, both


def fold_kernel(distance, me_ref, decay_ref, *refs):
    *inner, got_ref, group_ref, memory_ref, total_ref, send_ref = refs
    me = me_ref[0]
    for head in range(group_ref.shape[0]):
        memory = load(inner[0], head) if inner else None
        memory, both = fold(
            distance, me, decay_ref, head, memory, load(group_ref, head), unpack(got_ref, head)
        )
        store(memory_ref, head, *memory)
        store(total_ref, head, *both)
        pack(send_ref, head, *both)


def local_kernel(half, me_ref, spans_ref, q_hbm, k_hbm, v_hbm, *refs):
    *halo, out_ref, q_buf, k_buf, v_buf, kp_buf, vp_buf, sems = refs
    me = me_ref[0]
    heads, rows, width = q_buf.shape
    here, before = pl.ds(half * rows, rows), pl.ds((half - 1) * rows, rows)

    def copies(head):
        cols = pl.ds(head * width, width)
        table = [(q_hbm, here, q_buf), (k_hbm, here, k_buf), (v_hbm, here, v_buf)]
        if half:
            table += [(k_hbm, before, kp_buf), (v_hbm, before, vp_buf)]
        return [
            pltpu.make_async_copy(src.at[at, cols], buf.at[head], sems.at[which, head])
            for which, (src, at, buf) in enumerate(table)
        ]

    for head in range(heads):
        for copy in copies(head):
            copy.start()
    if not half:
        for head in range(heads):
            cols = slice(head * width, (head + 1) * width)
            kp_buf[head, : rows // 2, :] = halo[0][:, cols]
            kp_buf[head, rows // 2 :, :] = halo[1][:, cols]
            vp_buf[head] = halo[2][:, cols]

    factor = math.log2(math.e) / math.sqrt(width)
    origin = (me * SPAN_DEV + half) * rows
    first = spans_ref[0, me * SPAN_DEV + half] - origin
    end = spans_ref[1, me * SPAN_DEV + half] - origin
    shift = 0 if half else jnp.where(me > 0, 0, rows + 1)
    for head in range(heads):
        for copy in copies(head):
            copy.wait()
        for start in range(0, rows, BLOCK):
            query = q_buf[head, start : start + BLOCK, :]
            dims = (((1,), (1,)), ((), ()))
            prev = lax.dot_general(query, kp_buf[head, start:, :], dims, preferred_element_type=F32)
            own = lax.dot_general(query, k_buf[head], dims, preferred_element_type=F32)
            row = start + lax.broadcasted_iota(jnp.int32, (BLOCK, 1), 0)
            limit = jnp.where((row >= first) & (row < end), end - 1, row)
            col = lax.broadcasted_iota(jnp.int32, prev.shape, 1) + start
            prev = jnp.where(col > row + shift, prev, MASKED)
            col = lax.broadcasted_iota(jnp.int32, own.shape, 1)
            own = jnp.where(col <= limit, own, MASKED)
            top = jnp.maximum(
                jnp.max(prev, axis=1, keepdims=True), jnp.max(own, axis=1, keepdims=True)
            )
            prev = jnp.exp2((prev - top) * factor)
            own = jnp.exp2((own - top) * factor)
            total = jnp.sum(prev, axis=1, keepdims=True) + jnp.sum(own, axis=1, keepdims=True)
            mixed = jnp.dot(prev.astype(BF16), vp_buf[head, start:, :], preferred_element_type=F32)
            mixed += jnp.dot(own.astype(BF16), v_buf[head], preferred_element_type=F32)
            out_ref[start : start + BLOCK, head * width : (head + 1) * width] = mixed / total


def local_half(half, queries, keys, values, halo, spans, me, heads, width):
    rows = queries.shape[0] // SPAN_DEV
    buf = pltpu.VMEM((heads, rows, width), BF16)
    halo = list(halo)
    return pl.pallas_call(
        functools.partial(local_kernel, half),
        in_specs=[SMEM, SMEM, HBM, HBM, HBM] + [VMEM] * len(halo),
        out_specs=VMEM,
        out_shape=pltpu.VMEM((rows, heads * width), F32),
        scratch_shapes=[buf] * 5 + [pltpu.SemaphoreType.DMA((5, heads))],
        compiler_params=params(32),
        cost_estimate=cost(1.5e10, 6 * rows * heads * width * 2),
    )(me, spans, in_hbm(queries), in_hbm(keys), in_hbm(values), *halo)


def readout_kernel(distance, start, me_ref, decay_ref, gate_ref, q_hbm, local_ref, *refs):
    *inner, got_ref, group_ref, out_ref, q_ref, sem = refs
    me = me_ref[0]
    rows = out_ref.shape[0]
    fetch = pltpu.make_async_copy(q_hbm.at[pl.ds(start, rows)], q_ref, sem)
    fetch.start()
    local_rows = slice(start % BAND, start % BAND + rows)
    fetch.wait()
    heads, width = group_ref.shape[0], group_ref.shape[2]
    for head in range(heads):
        memory = load(inner[0], head) if inner else None
        (memory, norm), unused = fold(
            distance, me, decay_ref, head, memory, load(group_ref, head), unpack(got_ref, head)
        )
        cols = slice(head * width, (head + 1) * width)
        feats = phi(q_ref[:, cols].astype(F32))
        q_high, q_low = split(feats)
        m_high, m_low = split(memory)
        left = jnp.concatenate([q_high, q_low], axis=1)
        right = jnp.concatenate(
            [
                jnp.concatenate([m_high, m_low], axis=1),
                jnp.concatenate([m_high, jnp.zeros_like(m_low)], axis=1),
            ],
            axis=0,
        )
        both = jnp.dot(left, right, preferred_element_type=F32)
        numer = both[:, :width] + both[:, width:]
        denom = jnp.sum(feats * norm, axis=1, keepdims=True) + 1.0
        gate = 1.0 / (1.0 + jnp.exp(jnp.full((1, width), -gate_ref[head], F32)))
        out = gate * (numer / denom) + (1.0 - gate) * local_ref[local_rows, cols]
        out_ref[:, cols] = out.astype(BF16)


def readout(distance, start, rows, queries, local, memory, me, decay, gate):
    cols = queries.shape[1]
    return pl.pallas_call(
        functools.partial(readout_kernel, distance, start),
        in_specs=[SMEM, SMEM, SMEM, HBM, VMEM] + [VMEM] * len(memory),
        out_specs=VMEM,
        out_shape=pltpu.VMEM((rows, cols), BF16),
        scratch_shapes=[pltpu.VMEM((rows, cols), BF16), pltpu.SemaphoreType.DMA],
        compiler_params=params(16),
        cost_estimate=cost(2e9, rows * cols * 8),
    )(me, decay, gate, in_hbm(queries), local, *memory)


def project_kernel(shared, first_row, odd_ref, *refs):
    *refs, out_hbm, out_ref, sems = refs
    xs, ws = refs[: len(shared)], list(refs[len(shared) :])
    rows, columns = out_ref.shape
    odd = odd_ref[0]
    lefts, rights = [], []
    for x_ref, is_shared in zip(xs, shared):
        if is_shared:
            unit = x_ref.shape[1] // 4
            most = x_ref[:, pl.ds(pl.multiple_of(odd * unit, unit), 3 * unit)]
            rest = x_ref[:, pl.ds(pl.multiple_of((1 - odd) * 3 * unit, unit), unit)]
            lefts.append(jnp.concatenate([most, rest], axis=1))
            rights.append((ws.pop(0), ws.pop(0)))
        else:
            lefts.append(x_ref[...])
            rights.append((ws.pop(0),))
    copies = []
    for number, start in enumerate(range(0, columns, TILE)):
        at = slice(start, start + TILE)
        acc = None
        for left, right in zip(lefts, rights):
            block = [w_ref[:, at] for w_ref in right]
            block = jnp.concatenate(block, axis=0) if len(block) > 1 else block[0]
            term = jnp.dot(left, block, preferred_element_type=F32)
            acc = term if acc is None else acc + term
        out_ref[:, at] = acc.astype(out_ref.dtype)
        target = out_hbm.at[pl.ds(first_row, rows), pl.ds(start, TILE)]
        copy = pltpu.make_async_copy(out_ref.at[:, pl.ds(start, TILE)], target, sems.at[number])
        copy.start()
        copies.append(copy)
    for copy in copies:
        copy.wait()


def project(start, total_rows, xs, weights, odd, out):
    rows = xs[0].shape[0]
    flat = [w for ws in weights for w in ws]
    columns = flat[0].shape[1]
    operands = [odd, *map(in_vmem, xs), *map(in_vmem, flat)]
    in_specs = [SMEM] + [VMEM] * (len(operands) - 1)
    aliases = {}
    if out is not None:
        in_specs.append(HBM)
        aliases = {len(operands): 0}
        operands.append(out)
    depth = sum(w.shape[0] for w in flat)
    return pl.pallas_call(
        functools.partial(project_kernel, [len(ws) > 1 for ws in weights], start),
        in_specs=in_specs,
        out_specs=HBM,
        out_shape=pltpu.HBM((total_rows, columns), BF16),
        scratch_shapes=[
            pltpu.VMEM((rows, columns), BF16),
            pltpu.SemaphoreType.DMA((columns // TILE,)),
        ],
        input_output_aliases=aliases,
        compiler_params=params(24),
        cost_estimate=cost(2 * rows * depth * columns, depth * columns * 2),
    )(*operands)


def swap(x, axis, mask):
    size = lax.axis_size(axis)
    return lax.ppermute(x, axis, [(i, i ^ mask) for i in range(size)])


CHUNKS = ((512, 512), (0, 256), (256, 256))


def body(queries, keys, values, span_bounds, mem_decay, mem_gate, out_weight):
    mem_decay, span_bounds = mem_decay.T, span_bounds.T
    seg_rows = queries.shape[0]
    heads = mem_gate.shape[0]
    width = queries.shape[1] // heads
    seq_size, head_size = lax.axis_size("seq"), lax.axis_size("head")
    assert head_size & (head_size - 1) == 0 and seg_rows == BAND * SPAN_DEV
    assert seq_size & (seq_size - 1) == 0 and seq_size > 1
    seq_index, head_index = lax.axis_index("seq"), lax.axis_index("head")
    me = seq_index.astype(jnp.int32).reshape(1)
    odd = me & 1
    depth = out_weight.shape[0]
    unit = depth // 4
    columns = out_weight.shape[1] // head_size

    masks = sorted(range(1, head_size), reverse=True)
    slices = [(mask, depth if mask == 1 else 3 * unit) for mask in masks] + [(0, depth)]
    at = jnp.concatenate([odd, head_index.astype(jnp.int32).reshape(1)])
    first = make_slices(out_weight, slices[:1], at, columns)
    state, send, *more = make_state(keys, values, out_weight, slices[1:], at, heads, width, columns)
    tails, blocks = more[:3], [*first, *more[3:]]
    weights = {}
    for mask, block in zip([*masks, 0], blocks):
        weights[mask] = (swap(block, "head", mask) if mask else block,)
        if mask > 1:
            most = weights[mask][0]
            part = make_part(most, odd, unit)
            weights[mask] = (most, swap(part, "seq", 1))

    halo = []
    for tail in tails:
        halo.append(lax.ppermute(tail, "seq", [(i, i + 1) for i in range(seq_size - 1)]))

    inner, group, distance = [], state, 1
    while True:
        got = swap(send, "seq", distance)
        if 2 * distance >= seq_size:
            break
        shape = pltpu.VMEM(state.shape, F32)
        operands = [me, mem_decay, *inner, got, group]
        memory, group, send = pl.pallas_call(
            functools.partial(fold_kernel, distance),
            in_specs=[SMEM, SMEM] + [VMEM] * (len(operands) - 2),
            out_specs=[VMEM] * 3,
            out_shape=[shape, shape, pltpu.VMEM(send.shape, BF16)],
            compiler_params=params(16),
            cost_estimate=cost(1e9, 5 * state.size * 4),
        )(*operands)
        inner, distance = [memory], 2 * distance
    memory = [*inner, got, group]

    locals_ = {}
    for half in (1, 0):
        locals_[half] = local_half(
            half, queries, keys, values, () if half else halo,
            span_bounds, me, heads, width,
        )

    out = None
    for start, rows in CHUNKS:
        own = readout(
            distance, start, rows, queries,
            locals_[start // BAND], memory, me, mem_decay, mem_gate,
        )
        xs = {0: own}
        mask = head_size // 2
        while mask:
            for at, x in list(xs.items()):
                xs[at ^ mask] = swap(x, "head", mask)
            mask //= 2
        order = range(head_size)
        out = project(
            start, seg_rows,
            [xs[i] for i in order], [weights[i] for i in order], odd, out,
        )
    return out


def solution(mesh):
    return jax.shard_map(
        body,
        mesh=mesh,
        in_specs=(
            P("seq", "head"),
            P("seq", "head"),
            P("seq", "head"),
            P(),
            P(None, "head"),
            P("head"),
            P("head", None),
        ),
        out_specs=P("seq", "head"),
        check_vma=False,
    )
```

```python
import functools
import math

import jax
import jax.numpy as jnp
from jax import lax
from jax.experimental import pallas as pl
from jax.experimental.pallas import tpu as pltpu
from jax.sharding import PartitionSpec as P

BAND = 512
SPAN_DEV = 2
PAD = 8
SEND_PAD = 16
MASKED = -1e30
BLOCK = 256
TILE = 256
HALO = (128, 256)


SMEM = pl.BlockSpec(memory_space=pltpu.SMEM)
VMEM = pl.BlockSpec(memory_space=pltpu.VMEM)
HBM = pl.BlockSpec(memory_space=pltpu.HBM)
F32, BF16 = jnp.float32, jnp.bfloat16


def phi(x):
    return jnp.where(x > 0, x + 1.0, jnp.exp(jnp.minimum(x, 0.0)))


def split(x):
    high = x.astype(BF16)
    return high, (x - high.astype(F32)).astype(BF16)


def params(limit_mib):
    return pltpu.CompilerParams(vmem_limit_bytes=limit_mib << 20)


def in_hbm(x):
    return pltpu.with_memory_space_constraint(x, pltpu.HBM)


def in_vmem(x):
    return pltpu.with_memory_space_constraint(x, pltpu.VMEM)


def cost(flops, moved):
    return pl.CostEstimate(flops=int(flops), bytes_accessed=int(moved), transcendentals=0)


def pack(ref, head, memory, total):
    width = memory.shape[0]
    ref[head, :width, :] = memory.astype(BF16)
    high, low = split(total)
    row = lax.broadcasted_iota(jnp.int32, (SEND_PAD, total.shape[1]), 0)
    both = jnp.where(row == 0, high.astype(F32), jnp.where(row == 1, low.astype(F32), 0.0))
    ref[head, width:, :] = both.astype(BF16)


def unpack(ref, head):
    width = ref.shape[2]
    memory = ref[head, :width, :].astype(F32)
    total = jnp.sum(ref[head, width:, :].astype(F32), axis=0, keepdims=True)
    return memory, total


def store(ref, head, memory, total):
    width = memory.shape[0]
    ref[head, :width, :] = memory
    ref[head, width:, :] = jnp.broadcast_to(total, (PAD, total.shape[1]))


def load(ref, head):
    width = ref.shape[2]
    return ref[head, :width, :], ref[head, width : width + 1, :]


def slice_copies(slices, at_ref, w_hbm, blocks, sems):
    odd, head_index = at_ref[0], at_ref[1]
    copies = []
    for number, (mask, rows) in enumerate(slices):
        columns = blocks[number].shape[1]
        unit = w_hbm.shape[0] // 4
        row = pl.multiple_of(odd * unit, unit) if rows < w_hbm.shape[0] else 0
        col = pl.multiple_of((head_index ^ mask) * columns, columns)
        source = w_hbm.at[pl.ds(row, rows), pl.ds(col, columns)]
        copies.append(pltpu.make_async_copy(source, blocks[number], sems.at[number]))
    return copies


def slice_kernel(slices, at_ref, w_hbm, *refs):
    *blocks, sems = refs
    copies = slice_copies(slices, at_ref, w_hbm, blocks, sems)
    for copy in copies:
        copy.start()
    for copy in copies:
        copy.wait()


def make_slices(out_weight, slices, at, columns):
    return pl.pallas_call(
        functools.partial(slice_kernel, slices),
        in_specs=[SMEM, HBM],
        out_specs=[VMEM] * len(slices),
        out_shape=[pltpu.VMEM((rows, columns), BF16) for _, rows in slices],
        scratch_shapes=[pltpu.SemaphoreType.DMA((len(slices),))],
        compiler_params=params(8),
        cost_estimate=cost(1e9, 2 * columns * sum(rows for _, rows in slices) * 2),
        name="slices",
    )(at, in_hbm(out_weight))


def part_kernel(odd_ref, most_ref, part_ref):
    unit = part_ref.shape[0]
    part_ref[...] = most_ref[pl.ds(pl.multiple_of(odd_ref[0] * 2 * unit, unit), unit), :]


def make_part(most, odd, unit):
    return pl.pallas_call(
        part_kernel,
        in_specs=[SMEM, VMEM],
        out_specs=VMEM,
        out_shape=pltpu.VMEM((unit, most.shape[1]), BF16),
        compiler_params=params(4),
        cost_estimate=cost(1e8, 4 * unit * most.shape[1]),
        name="part",
    )(odd, in_vmem(most))


def state_kernel(slices, at_ref, q_hbm, k_hbm, v_hbm, w_hbm, state_ref, send_ref, *refs):
    *outs, sems, w_sems = refs
    (q_buf, k_buf, v_buf), tails, blocks = outs[:3], outs[3:6], outs[6:]
    heads, width = state_ref.shape[0], state_ref.shape[2]
    rows = k_buf.shape[0]
    steps = rows // BLOCK
    copies = []
    for step in range(steps):
        at = pl.ds(step * BLOCK, BLOCK)
        pair = [
            pltpu.make_async_copy(src.at[at], buf.at[at], sems.at[which, step])
            for which, (src, buf) in enumerate(((k_hbm, k_buf), (v_hbm, v_buf)))
        ]
        for copy in pair:
            copy.start()
        copies.append(pair)
    moves = slice_copies(slices, at_ref, w_hbm, blocks, w_sems)
    moves.append(pltpu.make_async_copy(q_hbm, q_buf, w_sems.at[len(slices)]))
    for copy in moves:
        copy.start()
    for step in range(steps):
        for copy in copies[step]:
            copy.wait()
        at = slice(step * BLOCK, (step + 1) * BLOCK)
        for head in range(heads):
            cols = slice(head * width, (head + 1) * width)
            feats = phi(k_buf[at, cols].astype(F32))
            high, low = split(feats)
            vals = v_buf[at, cols]
            dims = (((0,), (0,)), ((), ()))
            memory = lax.dot_general(high, vals, dims, preferred_element_type=F32)
            memory += lax.dot_general(low, vals, dims, preferred_element_type=F32)
            total = jnp.sum(feats, axis=0, keepdims=True)
            if step:
                had, had_total = load(state_ref, head)
                memory, total = memory + had, total + had_total
            store(state_ref, head, memory, total)
            if step == steps - 1:
                pack(send_ref, head, memory, total)
    near, far = rows - BAND + HALO[0], rows - BAND + HALO[0] + HALO[1]
    tails[0][...] = k_buf[rows - BAND : near, :]
    tails[1][...] = k_buf[near:far, :]
    tails[2][: rows - far, :] = k_buf[far:, :]
    tails[2][rows - far :, :] = v_buf[rows - BAND :, :]
    for copy in moves:
        copy.wait()


def make_state(queries, keys, values, out_weight, slices, at, heads, width, columns):
    rows, cols = keys.shape
    steps = rows // BLOCK
    tails = (*HALO, 2 * BAND - sum(HALO))
    return pl.pallas_call(
        functools.partial(state_kernel, slices),
        in_specs=[SMEM, HBM, HBM, HBM, HBM],
        out_specs=[VMEM] * (8 + len(slices)),
        out_shape=[
            pltpu.VMEM((heads, width + PAD, width), F32),
            pltpu.VMEM((heads, width + SEND_PAD, width), BF16),
            *[pltpu.VMEM((rows, cols), BF16)] * 3,
            *(pltpu.VMEM((tail, cols), BF16) for tail in tails),
            *(pltpu.VMEM((rows_, columns), BF16) for _, rows_ in slices),
        ],
        scratch_shapes=[
            pltpu.SemaphoreType.DMA((2, steps)),
            pltpu.SemaphoreType.DMA((len(slices) + 1,)),
        ],
        compiler_params=params(24),
        cost_estimate=cost(1e10, 4 * keys.size * 2),
        name="state",
    )(at, in_hbm(queries), in_hbm(keys), in_hbm(values), in_hbm(out_weight))


def fold(distance, me, decay_ref, head, memory, group, got):
    upper = (me & distance) != 0
    base = me & ~(distance - 1)
    above = base | distance
    through, before = 1.0, 1.0
    for step in range(distance):
        through = through * decay_ref[head, above + step]
        if step < distance - 1:
            factor = decay_ref[head, base + step]
            before = before * jnp.where(base + step < me, factor, 1.0)
    before = jnp.where(upper, before, 0.0)
    low, high = jnp.where(upper, 1.0, through), jnp.where(upper, through, 1.0)
    both = [low * mine + high * theirs for mine, theirs in zip(group, got)]
    if memory is None:
        memory = [before * theirs for theirs in got]
    else:
        memory = [mine + before * theirs for mine, theirs in zip(memory, got)]
    return memory, both


def fold_kernel(distance, me_ref, decay_ref, *refs):
    *inner, got_ref, group_ref, memory_ref, total_ref, send_ref = refs
    me = me_ref[0]
    for head in range(group_ref.shape[0]):
        memory = load(inner[0], head) if inner else None
        memory, both = fold(
            distance, me, decay_ref, head, memory, load(group_ref, head), unpack(got_ref, head)
        )
        store(memory_ref, head, *memory)
        store(total_ref, head, *both)
        pack(send_ref, head, *both)


def local_block(half, start, me_ref, spans_ref, query, keys_before, values_before, keys, values):
    me = me_ref[0]
    rows, width = keys.shape
    factor = math.log2(math.e) / math.sqrt(width)
    origin = (me * SPAN_DEV + half) * rows
    first = spans_ref[0, me * SPAN_DEV + half] - origin
    end = spans_ref[1, me * SPAN_DEV + half] - origin
    shift = 0 if half else jnp.where(me > 0, 0, rows + 1)
    dims = (((1,), (1,)), ((), ()))
    prev = lax.dot_general(query, keys_before, dims, preferred_element_type=F32)
    own = lax.dot_general(query, keys, dims, preferred_element_type=F32)
    row = start + lax.broadcasted_iota(jnp.int32, (query.shape[0], 1), 0)
    limit = jnp.where((row >= first) & (row < end), end - 1, row)
    col = lax.broadcasted_iota(jnp.int32, prev.shape, 1) + start
    prev = jnp.where(col > row + shift, prev, MASKED)
    col = lax.broadcasted_iota(jnp.int32, own.shape, 1)
    own = jnp.where(col <= limit, own, MASKED)
    top = jnp.maximum(jnp.max(prev, axis=1, keepdims=True), jnp.max(own, axis=1, keepdims=True))
    prev = jnp.exp2((prev - top) * factor)
    own = jnp.exp2((own - top) * factor)
    total = jnp.sum(prev, axis=1, keepdims=True) + jnp.sum(own, axis=1, keepdims=True)
    mixed = jnp.dot(prev.astype(BF16), values_before, preferred_element_type=F32)
    mixed += jnp.dot(own.astype(BF16), values, preferred_element_type=F32)
    return mixed / total


def read_block(query, memory, norm, gate, local):
    width = query.shape[1]
    feats = phi(query.astype(F32))
    left = jnp.concatenate(split(feats), axis=1)
    both = jnp.dot(left, memory, preferred_element_type=F32)
    numer = both[:, :width] + both[:, width:]
    denom = jnp.sum(feats * norm, axis=1, keepdims=True) + 1.0
    gate = 1.0 / (1.0 + jnp.exp(jnp.full((1, width), -gate, F32)))
    return (gate * (numer / denom) + (1.0 - gate) * local).astype(BF16)


def local_kernel(width, me_ref, spans_ref, q_ref, k_ref, v_ref, out_ref):
    rows, cols = out_ref.shape
    for head in range(cols // width):
        at = slice(head * width, (head + 1) * width)
        for start in range(0, rows, BLOCK):
            out_ref[start : start + BLOCK, at] = local_block(
                1, start, me_ref, spans_ref, q_ref[rows + start : rows + start + BLOCK, at],
                k_ref[start:rows, at], v_ref[start:rows, at], k_ref[rows:, at], v_ref[rows:, at],
            )


def make_local(queries, keys, values, spans, me, width):
    rows, cols = queries.shape[0] // SPAN_DEV, queries.shape[1]
    return pl.pallas_call(
        functools.partial(local_kernel, width),
        in_specs=[SMEM, SMEM, VMEM, VMEM, VMEM],
        out_specs=VMEM,
        out_shape=pltpu.VMEM((rows, cols), F32),
        compiler_params=params(24),
        cost_estimate=cost(1.5e10, 6 * rows * cols * 2),
        name="local",
    )(me, spans, *map(in_vmem, (queries, keys, values)))


def readout_kernel(distance, me_ref, decay_ref, gate_ref, q_ref, local_ref, *refs):
    *inner, got_ref, group_ref, out_ref, memory_ref, norm_ref = refs
    me = me_ref[0]
    heads, width = group_ref.shape[0], group_ref.shape[2]
    rows = out_ref.shape[0]
    for head in range(heads):
        had = load(inner[0], head) if inner else None
        (memory, norm), unused = fold(
            distance, me, decay_ref, head, had, load(group_ref, head), unpack(got_ref, head)
        )
        high, low = split(memory)
        memory_ref[head, :width, :width] = high
        memory_ref[head, :width, width:] = low
        memory_ref[head, width:, :width] = high
        memory_ref[head, width:, width:] = jnp.zeros_like(low)
        norm_ref[head] = jnp.broadcast_to(norm, (PAD, width))
        at = slice(head * width, (head + 1) * width)
        out_ref[:, at] = read_block(
            q_ref[-rows:, at], memory_ref[head], norm, gate_ref[head], local_ref[:, at]
        )


def make_readout(distance, queries, local, memory, me, decay, gate):
    rows, cols = local.shape
    heads, _, width = memory[-1].shape
    return pl.pallas_call(
        functools.partial(readout_kernel, distance),
        in_specs=[SMEM, SMEM, SMEM] + [VMEM] * (2 + len(memory)),
        out_specs=[VMEM] * 3,
        out_shape=[
            pltpu.VMEM((rows, cols), BF16),
            pltpu.VMEM((heads, 2 * width, 2 * width), BF16),
            pltpu.VMEM((heads, PAD, width), F32),
        ],
        compiler_params=params(16),
        cost_estimate=cost(2e9, rows * cols * 8),
        name="readout",
    )(me, decay, gate, *map(in_vmem, (queries, local)), *memory)


def attend_kernel(start, me_ref, spans_ref, gate_ref, q_ref, k_ref, v_ref, *refs):
    *halo, memory_ref, norm_ref, out_ref, before_ref = refs
    heads, width = norm_ref.shape[0], norm_ref.shape[2]
    rows = before_ref.shape[0]
    near, far = HALO[0], sum(HALO)
    before_ref[:near, :] = halo[0][...]
    before_ref[near:far, :] = halo[1][...]
    before_ref[far:, :] = halo[2][: rows - far, :]
    for head in range(heads):
        at = slice(head * width, (head + 1) * width)
        query = q_ref[start : start + BLOCK, at]
        local = local_block(
            0, start, me_ref, spans_ref, query, before_ref[start:, at],
            halo[2][rows - far + start :, at], k_ref[:rows, at], v_ref[:rows, at],
        )
        out_ref[:, at] = read_block(
            query, memory_ref[head], norm_ref[head, :1, :], gate_ref[head], local
        )


def make_attend(start, queries, keys, values, halo, memory, norm, spans, me, gate):
    rows, cols = queries.shape[0] // SPAN_DEV, queries.shape[1]
    operands = [*map(in_vmem, (queries, keys, values, *halo)), memory, norm]
    return pl.pallas_call(
        functools.partial(attend_kernel, start),
        in_specs=[SMEM] * 3 + [VMEM] * len(operands),
        out_specs=VMEM,
        out_shape=pltpu.VMEM((BLOCK, cols), BF16),
        scratch_shapes=[pltpu.VMEM((rows, cols), BF16)],
        compiler_params=params(24),
        cost_estimate=cost(8e9, 6 * rows * cols * 2),
    )(me, spans, gate, *operands)


def project_kernel(shared, first_row, odd_ref, *refs):
    *refs, out_hbm, out_ref, sems = refs
    xs, ws = refs[: len(shared)], list(refs[len(shared) :])
    rows, columns = out_ref.shape
    odd = odd_ref[0]
    lefts, rights = [], []
    for x_ref, is_shared in zip(xs, shared):
        if is_shared:
            unit = x_ref.shape[1] // 4
            most = x_ref[:, pl.ds(pl.multiple_of(odd * unit, unit), 3 * unit)]
            rest = x_ref[:, pl.ds(pl.multiple_of((1 - odd) * 3 * unit, unit), unit)]
            lefts.append(jnp.concatenate([most, rest], axis=1))
            rights.append((ws.pop(0), ws.pop(0)))
        else:
            lefts.append(x_ref[...])
            rights.append((ws.pop(0),))
    copies = []
    for number, start in enumerate(range(0, columns, TILE)):
        at = slice(start, start + TILE)
        acc = None
        for left, right in zip(lefts, rights):
            block = [w_ref[:, at] for w_ref in right]
            block = jnp.concatenate(block, axis=0) if len(block) > 1 else block[0]
            term = jnp.dot(left, block, preferred_element_type=F32)
            acc = term if acc is None else acc + term
        out_ref[:, at] = acc.astype(out_ref.dtype)
        target = out_hbm.at[pl.ds(first_row, rows), pl.ds(start, TILE)]
        copy = pltpu.make_async_copy(out_ref.at[:, pl.ds(start, TILE)], target, sems.at[number])
        copy.start()
        copies.append(copy)
    for copy in copies:
        copy.wait()


def project(start, total_rows, xs, weights, odd, out):
    rows = xs[0].shape[0]
    flat = [w for ws in weights for w in ws]
    columns = flat[0].shape[1]
    operands = [odd, *map(in_vmem, xs), *map(in_vmem, flat)]
    in_specs = [SMEM] + [VMEM] * (len(operands) - 1)
    aliases = {}
    if out is not None:
        in_specs.append(HBM)
        aliases = {len(operands): 0}
        operands.append(out)
    depth = sum(w.shape[0] for w in flat)
    return pl.pallas_call(
        functools.partial(project_kernel, [len(ws) > 1 for ws in weights], start),
        in_specs=in_specs,
        out_specs=HBM,
        out_shape=pltpu.HBM((total_rows, columns), BF16),
        scratch_shapes=[
            pltpu.VMEM((rows, columns), BF16),
            pltpu.SemaphoreType.DMA((columns // TILE,)),
        ],
        input_output_aliases=aliases,
        compiler_params=params(24),
        cost_estimate=cost(2 * rows * depth * columns, depth * columns * 2),
    )(*operands)


def swap(x, axis, mask):
    size = lax.axis_size(axis)
    return lax.ppermute(x, axis, [(i, i ^ mask) for i in range(size)])


def body(queries, keys, values, span_bounds, mem_decay, mem_gate, out_weight):
    mem_decay, span_bounds = mem_decay.T, span_bounds.T
    seg_rows = queries.shape[0]
    heads = mem_gate.shape[0]
    width = queries.shape[1] // heads
    seq_size, head_size = lax.axis_size("seq"), lax.axis_size("head")
    assert head_size & (head_size - 1) == 0 and seg_rows == BAND * SPAN_DEV
    assert seq_size & (seq_size - 1) == 0 and seq_size > 1
    seq_index, head_index = lax.axis_index("seq"), lax.axis_index("head")
    me = seq_index.astype(jnp.int32).reshape(1)
    odd = me & 1
    depth = out_weight.shape[0]
    unit = depth // 4
    columns = out_weight.shape[1] // head_size

    masks = sorted(range(1, head_size), reverse=True)
    slices = [(mask, depth if mask == 1 else 3 * unit) for mask in masks] + [(0, depth)]
    at = jnp.concatenate([odd, head_index.astype(jnp.int32).reshape(1)])
    first = make_slices(out_weight, slices[:1], at, columns)
    state, send, *more = make_state(
        queries, keys, values, out_weight, slices[1:], at, heads, width,
        columns,
    )
    queries, keys, values = more[:3]
    tails, blocks = more[3:6], [*first, *more[6:]]
    weights = {}
    for mask, block in zip([*masks, 0], blocks):
        weights[mask] = (swap(block, "head", mask) if mask else block,)
        if mask > 1:
            most = weights[mask][0]
            part = make_part(most, odd, unit)
            weights[mask] = (most, swap(part, "seq", 1))

    halo = []
    for tail in tails:
        halo.append(lax.ppermute(tail, "seq", [(i, i + 1) for i in range(seq_size - 1)]))

    inner, group, distance = [], state, 1
    while True:
        got = swap(send, "seq", distance)
        if 2 * distance >= seq_size:
            break
        shape = pltpu.VMEM(state.shape, F32)
        operands = [me, mem_decay, *inner, got, group]
        memory, group, send = pl.pallas_call(
            functools.partial(fold_kernel, distance),
            in_specs=[SMEM, SMEM] + [VMEM] * (len(operands) - 2),
            out_specs=[VMEM] * 3,
            out_shape=[shape, shape, pltpu.VMEM(send.shape, BF16)],
            compiler_params=params(16),
            cost_estimate=cost(1e9, 5 * state.size * 4),
        )(*operands)
        inner, distance = [memory], 2 * distance
    memory = [*inner, got, group]

    local = make_local(queries, keys, values, span_bounds, me, width)
    own, total, norm = make_readout(distance, queries, local, memory, me, mem_decay, mem_gate)
    chunks = [(BAND, own)]
    for start in range(0, BAND, BLOCK):
        own = make_attend(
            start, queries, keys,
            values, halo, total, norm, span_bounds, me, mem_gate,
        )
        chunks.append((start, own))

    out = None
    for start, own in chunks:
        xs = {0: own}
        mask = head_size // 2
        while mask:
            for at, x in list(xs.items()):
                xs[at ^ mask] = swap(x, "head", mask)
            mask //= 2
        order = range(head_size)
        out = project(
            start, seg_rows,
            [xs[i] for i in order], [weights[i] for i in order], odd, out,
        )
    return out


def solution(mesh):
    return jax.shard_map(
        body,
        mesh=mesh,
        in_specs=(
            P("seq", "head"),
            P("seq", "head"),
            P("seq", "head"),
            P(),
            P(None, "head"),
            P("head"),
            P("head", None),
        ),
        out_specs=P("seq", "head"),
        check_vma=False,
    )
```

```python
import functools
import math

import jax
import jax.numpy as jnp
from jax import lax
from jax.experimental import pallas as pl
from jax.experimental.pallas import tpu as pltpu
from jax.sharding import PartitionSpec as P

BAND = 512
SPAN_DEV = 2
PAD = 8
SEND_PAD = 16
MASKED = -1e30
BLOCK = 256
TILE = 256
HALO = (128, 256)


SMEM = pl.BlockSpec(memory_space=pltpu.SMEM)
VMEM = pl.BlockSpec(memory_space=pltpu.VMEM)
HBM = pl.BlockSpec(memory_space=pltpu.HBM)
F32, BF16 = jnp.float32, jnp.bfloat16


def phi(x):
    return jnp.where(x > 0, x + 1.0, jnp.exp(jnp.minimum(x, 0.0)))


def split(x):
    high = x.astype(BF16)
    return high, (x - high.astype(F32)).astype(BF16)


def params(limit_mib):
    return pltpu.CompilerParams(vmem_limit_bytes=limit_mib << 20)


def in_hbm(x):
    return pltpu.with_memory_space_constraint(x, pltpu.HBM)


def in_vmem(x):
    return pltpu.with_memory_space_constraint(x, pltpu.VMEM)


def cost(flops, moved):
    return pl.CostEstimate(flops=int(flops), bytes_accessed=int(moved), transcendentals=0)


def pack(ref, head, memory, total):
    width = memory.shape[0]
    ref[head, :width, :] = memory.astype(BF16)
    high, low = split(total)
    row = lax.broadcasted_iota(jnp.int32, (SEND_PAD, total.shape[1]), 0)
    both = jnp.where(row == 0, high.astype(F32), jnp.where(row == 1, low.astype(F32), 0.0))
    ref[head, width:, :] = both.astype(BF16)


def unpack(ref, head):
    width = ref.shape[2]
    memory = ref[head, :width, :].astype(F32)
    total = jnp.sum(ref[head, width:, :].astype(F32), axis=0, keepdims=True)
    return memory, total


def store(ref, head, memory, total):
    width = memory.shape[0]
    ref[head, :width, :] = memory
    ref[head, width:, :] = jnp.broadcast_to(total, (PAD, total.shape[1]))


def load(ref, head):
    width = ref.shape[2]
    return ref[head, :width, :], ref[head, width : width + 1, :]


def slice_copies(slices, at_ref, w_hbm, blocks, sems):
    me, head_index = at_ref[0], at_ref[1]
    copies = []
    for number, (mask, partner) in enumerate(slices):
        rows, columns = blocks[number].shape
        row = jnp.where((me & partner) != 0, rows, 0) if partner else 0
        col = pl.multiple_of((head_index ^ mask) * columns, columns)
        source = w_hbm.at[pl.ds(pl.multiple_of(row, rows), rows), pl.ds(col, columns)]
        copies.append(pltpu.make_async_copy(source, blocks[number], sems.at[number]))
    return copies


def state_kernel(slices, at_ref, q_hbm, k_hbm, v_hbm, w_hbm, state_ref, send_ref, *refs):
    *outs, sems, w_sems = refs
    (q_buf, k_buf, v_buf), tails, blocks = outs[:3], outs[3:6], outs[6:]
    heads, width = state_ref.shape[0], state_ref.shape[2]
    rows = k_buf.shape[0]
    steps = rows // BLOCK
    copies = []
    for step in range(steps):
        at = pl.ds(step * BLOCK, BLOCK)
        pair = [
            pltpu.make_async_copy(src.at[at], buf.at[at], sems.at[which, step])
            for which, (src, buf) in enumerate(((k_hbm, k_buf), (v_hbm, v_buf)))
        ]
        for copy in pair:
            copy.start()
        copies.append(pair)
    moves = slice_copies(slices, at_ref, w_hbm, blocks, w_sems)
    moves.append(pltpu.make_async_copy(q_hbm, q_buf, w_sems.at[len(slices)]))
    for copy in moves:
        copy.start()
    for step in range(steps):
        for copy in copies[step]:
            copy.wait()
        at = slice(step * BLOCK, (step + 1) * BLOCK)
        for head in range(heads):
            cols = slice(head * width, (head + 1) * width)
            feats = phi(k_buf[at, cols].astype(F32))
            high, low = split(feats)
            vals = v_buf[at, cols]
            dims = (((0,), (0,)), ((), ()))
            memory = lax.dot_general(high, vals, dims, preferred_element_type=F32)
            memory += lax.dot_general(low, vals, dims, preferred_element_type=F32)
            total = jnp.sum(feats, axis=0, keepdims=True)
            if step:
                had, had_total = load(state_ref, head)
                memory, total = memory + had, total + had_total
            store(state_ref, head, memory, total)
            if step == steps - 1:
                pack(send_ref, head, memory, total)
    near, far = rows - BAND + HALO[0], rows - BAND + HALO[0] + HALO[1]
    tails[0][...] = k_buf[rows - BAND : near, :]
    tails[1][...] = k_buf[near:far, :]
    tails[2][: rows - far, :] = k_buf[far:, :]
    tails[2][rows - far :, :] = v_buf[rows - BAND :, :]
    for copy in moves:
        copy.wait()


def make_state(queries, keys, values, out_weight, slices, at, heads, width, columns):
    rows, cols = keys.shape
    depth = out_weight.shape[0]
    steps = rows // BLOCK
    tails = (*HALO, 2 * BAND - sum(HALO))
    return pl.pallas_call(
        functools.partial(state_kernel, slices),
        in_specs=[SMEM, HBM, HBM, HBM, HBM],
        out_specs=[VMEM] * (8 + len(slices)),
        out_shape=[
            pltpu.VMEM((heads, width + PAD, width), F32),
            pltpu.VMEM((heads, width + SEND_PAD, width), BF16),
            *[pltpu.VMEM((rows, cols), BF16)] * 3,
            *(pltpu.VMEM((tail, cols), BF16) for tail in tails),
            *(pltpu.VMEM((depth // (2 if by else 1), columns), BF16) for _, by in slices),
        ],
        scratch_shapes=[
            pltpu.SemaphoreType.DMA((2, steps)),
            pltpu.SemaphoreType.DMA((len(slices) + 1,)),
        ],
        compiler_params=params(24),
        cost_estimate=cost(1e10, 4 * keys.size * 2),
        name="state",
    )(at, in_hbm(queries), in_hbm(keys), in_hbm(values), in_hbm(out_weight))


def fold(distance, me, decay_ref, head, memory, group, got):
    upper = (me & distance) != 0
    base = me & ~(distance - 1)
    above = base | distance
    through, before = 1.0, 1.0
    for step in range(distance):
        through = through * decay_ref[head, above + step]
        if step < distance - 1:
            factor = decay_ref[head, base + step]
            before = before * jnp.where(base + step < me, factor, 1.0)
    before = jnp.where(upper, before, 0.0)
    low, high = jnp.where(upper, 1.0, through), jnp.where(upper, through, 1.0)
    both = [low * mine + high * theirs for mine, theirs in zip(group, got)]
    if memory is None:
        memory = [before * theirs for theirs in got]
    else:
        memory = [mine + before * theirs for mine, theirs in zip(memory, got)]
    return memory, both


def fold_kernel(distance, me_ref, decay_ref, *refs):
    *inner, got_ref, group_ref, memory_ref, total_ref, send_ref = refs
    me = me_ref[0]
    for head in range(group_ref.shape[0]):
        memory = load(inner[0], head) if inner else None
        memory, both = fold(
            distance, me, decay_ref, head, memory, load(group_ref, head), unpack(got_ref, head)
        )
        store(memory_ref, head, *memory)
        store(total_ref, head, *both)
        pack(send_ref, head, *both)


def local_block(half, start, me_ref, spans_ref, query, keys_before, values_before, keys, values):
    me = me_ref[0]
    rows, width = keys.shape
    factor = math.log2(math.e) / math.sqrt(width)
    origin = (me * SPAN_DEV + half) * rows
    first = spans_ref[0, me * SPAN_DEV + half] - origin
    end = spans_ref[1, me * SPAN_DEV + half] - origin
    shift = 0 if half else jnp.where(me > 0, 0, rows + 1)
    dims = (((1,), (1,)), ((), ()))
    prev = lax.dot_general(query, keys_before, dims, preferred_element_type=F32)
    own = lax.dot_general(query, keys, dims, preferred_element_type=F32)
    row = start + lax.broadcasted_iota(jnp.int32, (query.shape[0], 1), 0)
    limit = jnp.where((row >= first) & (row < end), end - 1, row)
    col = lax.broadcasted_iota(jnp.int32, prev.shape, 1) + start
    prev = jnp.where(col > row + shift, prev, MASKED)
    col = lax.broadcasted_iota(jnp.int32, own.shape, 1)
    own = jnp.where(col <= limit, own, MASKED)
    top = jnp.maximum(jnp.max(prev, axis=1, keepdims=True), jnp.max(own, axis=1, keepdims=True))
    prev = jnp.exp2((prev - top) * factor)
    own = jnp.exp2((own - top) * factor)
    total = jnp.sum(prev, axis=1, keepdims=True) + jnp.sum(own, axis=1, keepdims=True)
    mixed = jnp.dot(prev.astype(BF16), values_before, preferred_element_type=F32)
    mixed += jnp.dot(own.astype(BF16), values, preferred_element_type=F32)
    return mixed / total


def read_block(query, memory, norm, gate, local):
    width = query.shape[1]
    feats = phi(query.astype(F32))
    left = jnp.concatenate(split(feats), axis=1)
    both = jnp.dot(left, memory, preferred_element_type=F32)
    numer = both[:, :width] + both[:, width:]
    denom = jnp.sum(feats * norm, axis=1, keepdims=True) + 1.0
    gate = 1.0 / (1.0 + jnp.exp(jnp.full((1, width), -gate, F32)))
    return (gate * (numer / denom) + (1.0 - gate) * local).astype(BF16)


def local_kernel(width, me_ref, spans_ref, q_ref, k_ref, v_ref, out_ref):
    rows, cols = out_ref.shape
    for head in range(cols // width):
        at = slice(head * width, (head + 1) * width)
        for start in range(0, rows, BLOCK):
            out_ref[start : start + BLOCK, at] = local_block(
                1, start, me_ref, spans_ref, q_ref[rows + start : rows + start + BLOCK, at],
                k_ref[start:rows, at], v_ref[start:rows, at], k_ref[rows:, at], v_ref[rows:, at],
            )


def make_local(queries, keys, values, spans, me, width):
    rows, cols = queries.shape[0] // SPAN_DEV, queries.shape[1]
    return pl.pallas_call(
        functools.partial(local_kernel, width),
        in_specs=[SMEM, SMEM, VMEM, VMEM, VMEM],
        out_specs=VMEM,
        out_shape=pltpu.VMEM((rows, cols), F32),
        compiler_params=params(24),
        cost_estimate=cost(1.5e10, 6 * rows * cols * 2),
        name="local",
    )(me, spans, *map(in_vmem, (queries, keys, values)))


def readout_kernel(distance, me_ref, decay_ref, gate_ref, q_ref, local_ref, *refs):
    *inner, got_ref, group_ref, out_ref, memory_ref, norm_ref = refs
    me = me_ref[0]
    heads, width = group_ref.shape[0], group_ref.shape[2]
    rows = out_ref.shape[0]
    for head in range(heads):
        had = load(inner[0], head) if inner else None
        (memory, norm), unused = fold(
            distance, me, decay_ref, head, had, load(group_ref, head), unpack(got_ref, head)
        )
        high, low = split(memory)
        memory_ref[head, :width, :width] = high
        memory_ref[head, :width, width:] = low
        memory_ref[head, width:, :width] = high
        memory_ref[head, width:, width:] = jnp.zeros_like(low)
        norm_ref[head] = jnp.broadcast_to(norm, (PAD, width))
        at = slice(head * width, (head + 1) * width)
        out_ref[:, at] = read_block(
            q_ref[-rows:, at], memory_ref[head], norm, gate_ref[head], local_ref[:, at]
        )


def make_readout(distance, queries, local, memory, me, decay, gate):
    rows, cols = local.shape
    heads, _, width = memory[-1].shape
    return pl.pallas_call(
        functools.partial(readout_kernel, distance),
        in_specs=[SMEM, SMEM, SMEM] + [VMEM] * (2 + len(memory)),
        out_specs=[VMEM] * 3,
        out_shape=[
            pltpu.VMEM((rows, cols), BF16),
            pltpu.VMEM((heads, 2 * width, 2 * width), BF16),
            pltpu.VMEM((heads, PAD, width), F32),
        ],
        compiler_params=params(16),
        cost_estimate=cost(2e9, rows * cols * 8),
        name="readout",
    )(me, decay, gate, *map(in_vmem, (queries, local)), *memory)


def attend_kernel(start, me_ref, spans_ref, gate_ref, q_ref, k_ref, v_ref, *refs):
    *halo, memory_ref, norm_ref, out_ref, before_ref = refs
    heads, width = norm_ref.shape[0], norm_ref.shape[2]
    rows = before_ref.shape[0]
    near, far = HALO[0], sum(HALO)
    before_ref[:near, :] = halo[0][...]
    before_ref[near:far, :] = halo[1][...]
    before_ref[far:, :] = halo[2][: rows - far, :]
    for head in range(heads):
        at = slice(head * width, (head + 1) * width)
        query = q_ref[start : start + BLOCK, at]
        local = local_block(
            0, start, me_ref, spans_ref, query, before_ref[start:, at],
            halo[2][rows - far + start :, at], k_ref[:rows, at], v_ref[:rows, at],
        )
        out_ref[:, at] = read_block(
            query, memory_ref[head], norm_ref[head, :1, :], gate_ref[head], local
        )


def make_attend(start, queries, keys, values, halo, memory, norm, spans, me, gate):
    rows, cols = queries.shape[0] // SPAN_DEV, queries.shape[1]
    operands = [*map(in_vmem, (queries, keys, values, *halo)), memory, norm]
    return pl.pallas_call(
        functools.partial(attend_kernel, start),
        in_specs=[SMEM] * 3 + [VMEM] * len(operands),
        out_specs=VMEM,
        out_shape=pltpu.VMEM((BLOCK, cols), BF16),
        scratch_shapes=[pltpu.VMEM((rows, cols), BF16)],
        compiler_params=params(24),
        cost_estimate=cost(8e9, 6 * rows * cols * 2),
    )(me, spans, gate, *operands)


def project_kernel(partners, first_row, me_ref, *refs):
    *refs, out_hbm, out_ref, sems = refs
    xs, ws = refs[: len(partners)], list(refs[len(partners) :])
    rows, columns = out_ref.shape
    me = me_ref[0]
    lefts, rights = [], []
    for x_ref, partner in zip(xs, partners):
        if partner:
            half = x_ref.shape[1] // 2
            mine = jnp.where((me & partner) != 0, half, 0)
            parts = [x_ref[:, pl.ds(pl.multiple_of(at, half), half)] for at in (mine, half - mine)]
            lefts.append(jnp.concatenate(parts, axis=1))
            rights.append((ws.pop(0), ws.pop(0)))
        else:
            lefts.append(x_ref[...])
            rights.append((ws.pop(0),))
    copies = []
    for number, start in enumerate(range(0, columns, TILE)):
        at = slice(start, start + TILE)
        acc = None
        for left, right in zip(lefts, rights):
            block = [w_ref[:, at] for w_ref in right]
            block = jnp.concatenate(block, axis=0) if len(block) > 1 else block[0]
            term = jnp.dot(left, block, preferred_element_type=F32)
            acc = term if acc is None else acc + term
        out_ref[:, at] = acc.astype(out_ref.dtype)
        target = out_hbm.at[pl.ds(first_row, rows), pl.ds(start, TILE)]
        copy = pltpu.make_async_copy(out_ref.at[:, pl.ds(start, TILE)], target, sems.at[number])
        copy.start()
        copies.append(copy)
    for copy in copies:
        copy.wait()


def project(start, total_rows, xs, weights, partners, me, out):
    rows = xs[0].shape[0]
    flat = [w for ws in weights for w in ws]
    columns = flat[0].shape[1]
    operands = [me, *map(in_vmem, xs), *map(in_vmem, flat)]
    in_specs = [SMEM] + [VMEM] * (len(operands) - 1)
    aliases = {}
    if out is not None:
        in_specs.append(HBM)
        aliases = {len(operands): 0}
        operands.append(out)
    depth = sum(w.shape[0] for w in flat)
    return pl.pallas_call(
        functools.partial(project_kernel, partners, start),
        in_specs=in_specs,
        out_specs=HBM,
        out_shape=pltpu.HBM((total_rows, columns), BF16),
        scratch_shapes=[
            pltpu.VMEM((rows, columns), BF16),
            pltpu.SemaphoreType.DMA((columns // TILE,)),
        ],
        input_output_aliases=aliases,
        compiler_params=params(24),
        cost_estimate=cost(2 * rows * depth * columns, depth * columns * 2),
    )(*operands)


def swap(x, axis, mask):
    size = lax.axis_size(axis)
    return lax.ppermute(x, axis, [(i, i ^ mask) for i in range(size)])


def body(queries, keys, values, span_bounds, mem_decay, mem_gate, out_weight):
    mem_decay, span_bounds = mem_decay.T, span_bounds.T
    seg_rows = queries.shape[0]
    heads = mem_gate.shape[0]
    width = queries.shape[1] // heads
    seq_size, head_size = lax.axis_size("seq"), lax.axis_size("head")
    assert head_size & (head_size - 1) == 0 and seg_rows == BAND * SPAN_DEV
    assert seq_size & (seq_size - 1) == 0 and seq_size > 1
    seq_index, head_index = lax.axis_index("seq"), lax.axis_index("head")
    me = seq_index.astype(jnp.int32).reshape(1)
    columns = out_weight.shape[1] // head_size

    masks = sorted(range(1, head_size), reverse=True)
    partners = {mask: 1 << (mask % 2 == 0 and seq_size > 2) for mask in masks if mask > 1}
    slices = [(mask, partners.get(mask, 0)) for mask in (*masks, 0)]
    at = jnp.concatenate([me, head_index.astype(jnp.int32).reshape(1)])
    state, send, *more = make_state(
        queries, keys, values, out_weight, slices, at, heads, width, columns
    )
    queries, keys, values = more[:3]
    tails, blocks = more[3:6], more[6:]
    weights = {}
    for (mask, partner), block in zip(slices, blocks):
        block = swap(block, "head", mask) if mask else block
        weights[mask] = (block, swap(block, "seq", partner)) if partner else (block,)

    halo = []
    for tail in tails:
        halo.append(lax.ppermute(tail, "seq", [(i, i + 1) for i in range(seq_size - 1)]))

    inner, group, distance = [], state, 1
    while True:
        got = swap(send, "seq", distance)
        if 2 * distance >= seq_size:
            break
        shape = pltpu.VMEM(state.shape, F32)
        operands = [me, mem_decay, *inner, got, group]
        memory, group, send = pl.pallas_call(
            functools.partial(fold_kernel, distance),
            in_specs=[SMEM, SMEM] + [VMEM] * (len(operands) - 2),
            out_specs=[VMEM] * 3,
            out_shape=[shape, shape, pltpu.VMEM(send.shape, BF16)],
            compiler_params=params(16),
            cost_estimate=cost(1e9, 5 * state.size * 4),
        )(*operands)
        inner, distance = [memory], 2 * distance
    memory = [*inner, got, group]

    local = make_local(queries, keys, values, span_bounds, me, width)
    own, total, norm = make_readout(distance, queries, local, memory, me, mem_decay, mem_gate)
    chunks = [(BAND, own)]
    for start in range(0, BAND, BLOCK):
        own = make_attend(
            start, queries, keys,
            values, halo, total, norm, span_bounds, me, mem_gate,
        )
        chunks.append((start, own))

    out = None
    for start, own in chunks:
        xs = {0: own}
        mask = head_size // 2
        while mask:
            for at, x in list(xs.items()):
                xs[at ^ mask] = swap(x, "head", mask)
            mask //= 2
        order = range(head_size)
        out = project(
            start, seg_rows,
            [xs[i] for i in order], [weights[i] for i in order], [partners.get(i, 0) for i in order], me, out,
        )
    return out


def solution(mesh):
    return jax.shard_map(
        body,
        mesh=mesh,
        in_specs=(
            P("seq", "head"),
            P("seq", "head"),
            P("seq", "head"),
            P(),
            P(None, "head"),
            P("head"),
            P("head", None),
        ),
        out_specs=P("seq", "head"),
        check_vma=False,
    )
```

```python
import functools
import math

import jax
import jax.numpy as jnp
from jax import lax
from jax.experimental import pallas as pl
from jax.experimental.pallas import tpu as pltpu
from jax.sharding import PartitionSpec as P

BAND = 512
SPAN_DEV = 2
PAD = 8
SEND_PAD = 16
MASKED = -1e30
BLOCK = 256
TILE = 256
LATE = 384


SMEM = pl.BlockSpec(memory_space=pltpu.SMEM)
VMEM = pl.BlockSpec(memory_space=pltpu.VMEM)
HBM = pl.BlockSpec(memory_space=pltpu.HBM)
F32, BF16 = jnp.float32, jnp.bfloat16


def phi(x):
    return jnp.where(x > 0, x + 1.0, jnp.exp(jnp.minimum(x, 0.0)))


def split(x):
    high = x.astype(BF16)
    return high, (x - high.astype(F32)).astype(BF16)


def params(limit_mib):
    return pltpu.CompilerParams(vmem_limit_bytes=limit_mib << 20)


def in_hbm(x):
    return pltpu.with_memory_space_constraint(x, pltpu.HBM)


def in_vmem(x):
    return pltpu.with_memory_space_constraint(x, pltpu.VMEM)


def cost(flops, moved):
    return pl.CostEstimate(flops=int(flops), bytes_accessed=int(moved), transcendentals=0)


def pack(ref, head, memory, total):
    width = memory.shape[0]
    ref[head, :width, :] = memory.astype(BF16)
    high, low = split(total)
    row = lax.broadcasted_iota(jnp.int32, (SEND_PAD, total.shape[1]), 0)
    both = jnp.where(row == 0, high.astype(F32), jnp.where(row == 1, low.astype(F32), 0.0))
    ref[head, width:, :] = both.astype(BF16)


def unpack(ref, head):
    width = ref.shape[2]
    memory = ref[head, :width, :].astype(F32)
    total = jnp.sum(ref[head, width:, :].astype(F32), axis=0, keepdims=True)
    return memory, total


def store(ref, head, memory, total):
    width = memory.shape[0]
    ref[head, :width, :] = memory
    ref[head, width:, :] = jnp.broadcast_to(total, (PAD, total.shape[1]))


def load(ref, head):
    width = ref.shape[2]
    return ref[head, :width, :], ref[head, width : width + 1, :]


def slice_copies(slices, at_ref, w_hbm, blocks, sems):
    me, head_index = at_ref[0], at_ref[1]
    copies = []
    for number, (mask, partner) in enumerate(slices):
        rows, columns = blocks[number].shape
        row = jnp.where((me & partner) != 0, rows, 0) if partner else 0
        col = pl.multiple_of((head_index ^ mask) * columns, columns)
        source = w_hbm.at[pl.ds(pl.multiple_of(row, rows), rows), pl.ds(col, columns)]
        copies.append(pltpu.make_async_copy(source, blocks[number], sems.at[number]))
    return copies


def state_kernel(slices, at_ref, q_hbm, k_hbm, v_hbm, w_hbm, state_ref, send_ref, *refs):
    *outs, sems, w_sems = refs
    (q_buf, k_buf, v_buf), tails, blocks = outs[:3], outs[3:6], outs[6:]
    heads, width = state_ref.shape[0], state_ref.shape[2]
    rows = k_buf.shape[0]
    steps = rows // BLOCK
    copies = []
    for step in range(steps):
        at = pl.ds(step * BLOCK, BLOCK)
        pair = [
            pltpu.make_async_copy(src.at[at], buf.at[at], sems.at[which, step])
            for which, (src, buf) in enumerate(((k_hbm, k_buf), (v_hbm, v_buf)))
        ]
        for copy in pair:
            copy.start()
        copies.append(pair)
    moves = slice_copies(slices, at_ref, w_hbm, blocks, w_sems)
    moves.append(pltpu.make_async_copy(q_hbm, q_buf, w_sems.at[len(slices)]))
    for copy in moves:
        copy.start()
    for step in range(steps):
        for copy in copies[step]:
            copy.wait()
        at = slice(step * BLOCK, (step + 1) * BLOCK)
        for head in range(heads):
            cols = slice(head * width, (head + 1) * width)
            feats = phi(k_buf[at, cols].astype(F32))
            high, low = split(feats)
            vals = v_buf[at, cols]
            dims = (((0,), (0,)), ((), ()))
            memory = lax.dot_general(high, vals, dims, preferred_element_type=F32)
            memory += lax.dot_general(low, vals, dims, preferred_element_type=F32)
            total = jnp.sum(feats, axis=0, keepdims=True)
            if step:
                had, had_total = load(state_ref, head)
                memory, total = memory + had, total + had_total
            store(state_ref, head, memory, total)
            if step == steps - 1:
                pack(send_ref, head, memory, total)
    base = rows - BAND
    tails[0][...] = k_buf[base + LATE :, :]
    tails[1][: LATE - BLOCK, :] = k_buf[base + BLOCK : base + LATE, :]
    tails[1][LATE - BLOCK :, :] = v_buf[base + BLOCK :, :]
    tails[2][:BLOCK, :] = k_buf[base : base + BLOCK, :]
    tails[2][BLOCK:, :] = v_buf[base : base + BLOCK, :]
    for copy in moves:
        copy.wait()


def make_state(queries, keys, values, out_weight, slices, at, heads, width, columns):
    rows, cols = keys.shape
    depth = out_weight.shape[0]
    steps = rows // BLOCK
    tails = (BAND - LATE, LATE - BLOCK + BAND - BLOCK, 2 * BLOCK)
    return pl.pallas_call(
        functools.partial(state_kernel, slices),
        in_specs=[SMEM, HBM, HBM, HBM, HBM],
        out_specs=[VMEM] * (8 + len(slices)),
        out_shape=[
            pltpu.VMEM((heads, width + PAD, width), F32),
            pltpu.VMEM((heads, width + SEND_PAD, width), BF16),
            *[pltpu.VMEM((rows, cols), BF16)] * 3,
            *(pltpu.VMEM((tail, cols), BF16) for tail in tails),
            *(pltpu.VMEM((depth // (2 if by else 1), columns), BF16) for _, by in slices),
        ],
        scratch_shapes=[
            pltpu.SemaphoreType.DMA((2, steps)),
            pltpu.SemaphoreType.DMA((len(slices) + 1,)),
        ],
        compiler_params=params(24),
        cost_estimate=cost(1e10, 4 * keys.size * 2),
        name="state",
    )(at, in_hbm(queries), in_hbm(keys), in_hbm(values), in_hbm(out_weight))


def fold(distance, me, decay_ref, head, memory, group, got):
    upper = (me & distance) != 0
    base = me & ~(distance - 1)
    above = base | distance
    through, before = 1.0, 1.0
    for step in range(distance):
        through = through * decay_ref[head, above + step]
        if step < distance - 1:
            factor = decay_ref[head, base + step]
            before = before * jnp.where(base + step < me, factor, 1.0)
    before = jnp.where(upper, before, 0.0)
    low, high = jnp.where(upper, 1.0, through), jnp.where(upper, through, 1.0)
    both = [low * mine + high * theirs for mine, theirs in zip(group, got)]
    if memory is None:
        memory = [before * theirs for theirs in got]
    else:
        memory = [mine + before * theirs for mine, theirs in zip(memory, got)]
    return memory, both


def fold_kernel(distance, me_ref, decay_ref, *refs):
    *inner, got_ref, group_ref, memory_ref, total_ref, send_ref = refs
    me = me_ref[0]
    for head in range(group_ref.shape[0]):
        memory = load(inner[0], head) if inner else None
        memory, both = fold(
            distance, me, decay_ref, head, memory, load(group_ref, head), unpack(got_ref, head)
        )
        store(memory_ref, head, *memory)
        store(total_ref, head, *both)
        pack(send_ref, head, *both)


def local_block(half, start, me_ref, spans_ref, query, keys_before, values_before, keys, values):
    me = me_ref[0]
    rows, width = keys.shape
    factor = math.log2(math.e) / math.sqrt(width)
    origin = (me * SPAN_DEV + half) * rows
    first = spans_ref[0, me * SPAN_DEV + half] - origin
    end = spans_ref[1, me * SPAN_DEV + half] - origin
    shift = 0 if half else jnp.where(me > 0, 0, rows + 1)
    dims = (((1,), (1,)), ((), ()))
    prev = lax.dot_general(query, keys_before, dims, preferred_element_type=F32)
    own = lax.dot_general(query, keys, dims, preferred_element_type=F32)
    row = start + lax.broadcasted_iota(jnp.int32, (query.shape[0], 1), 0)
    limit = jnp.where((row >= first) & (row < end), end - 1, row)
    col = lax.broadcasted_iota(jnp.int32, prev.shape, 1) + start
    prev = jnp.where(col > row + shift, prev, MASKED)
    col = lax.broadcasted_iota(jnp.int32, own.shape, 1)
    own = jnp.where(col <= limit, own, MASKED)
    top = jnp.maximum(jnp.max(prev, axis=1, keepdims=True), jnp.max(own, axis=1, keepdims=True))
    prev = jnp.exp2((prev - top) * factor)
    own = jnp.exp2((own - top) * factor)
    total = jnp.sum(prev, axis=1, keepdims=True) + jnp.sum(own, axis=1, keepdims=True)
    mixed = jnp.dot(prev.astype(BF16), values_before, preferred_element_type=F32)
    mixed += jnp.dot(own.astype(BF16), values, preferred_element_type=F32)
    return mixed / total


def read_block(query, memory, norm, gate, local):
    width = query.shape[1]
    feats = phi(query.astype(F32))
    left = jnp.concatenate(split(feats), axis=1)
    both = jnp.dot(left, memory, preferred_element_type=F32)
    numer = both[:, :width] + both[:, width:]
    denom = jnp.sum(feats * norm, axis=1, keepdims=True) + 1.0
    gate = 1.0 / (1.0 + jnp.exp(jnp.full((1, width), -gate, F32)))
    return (gate * (numer / denom) + (1.0 - gate) * local).astype(BF16)


def local_kernel(width, me_ref, spans_ref, q_ref, k_ref, v_ref, out_ref):
    rows, cols = out_ref.shape
    for head in range(cols // width):
        at = slice(head * width, (head + 1) * width)
        for start in range(0, rows, BLOCK):
            out_ref[start : start + BLOCK, at] = local_block(
                1, start, me_ref, spans_ref, q_ref[rows + start : rows + start + BLOCK, at],
                k_ref[start:rows, at], v_ref[start:rows, at], k_ref[rows:, at], v_ref[rows:, at],
            )


def make_local(queries, keys, values, spans, me, width):
    rows, cols = queries.shape[0] // SPAN_DEV, queries.shape[1]
    return pl.pallas_call(
        functools.partial(local_kernel, width),
        in_specs=[SMEM, SMEM, VMEM, VMEM, VMEM],
        out_specs=VMEM,
        out_shape=pltpu.VMEM((rows, cols), F32),
        compiler_params=params(24),
        cost_estimate=cost(1.5e10, 6 * rows * cols * 2),
        name="local",
    )(me, spans, *map(in_vmem, (queries, keys, values)))


def readout_kernel(distance, me_ref, decay_ref, gate_ref, q_ref, local_ref, *refs):
    *inner, got_ref, group_ref, out_ref, memory_ref, norm_ref = refs
    me = me_ref[0]
    heads, width = group_ref.shape[0], group_ref.shape[2]
    rows = out_ref.shape[0]
    for head in range(heads):
        had = load(inner[0], head) if inner else None
        (memory, norm), unused = fold(
            distance, me, decay_ref, head, had, load(group_ref, head), unpack(got_ref, head)
        )
        high, low = split(memory)
        memory_ref[head, :width, :width] = high
        memory_ref[head, :width, width:] = low
        memory_ref[head, width:, :width] = high
        memory_ref[head, width:, width:] = jnp.zeros_like(low)
        norm_ref[head] = jnp.broadcast_to(norm, (PAD, width))
        at = slice(head * width, (head + 1) * width)
        out_ref[:, at] = read_block(
            q_ref[-rows:, at], memory_ref[head], norm, gate_ref[head], local_ref[:, at]
        )


def make_readout(distance, queries, local, memory, me, decay, gate):
    rows, cols = local.shape
    heads, _, width = memory[-1].shape
    return pl.pallas_call(
        functools.partial(readout_kernel, distance),
        in_specs=[SMEM, SMEM, SMEM] + [VMEM] * (2 + len(memory)),
        out_specs=[VMEM] * 3,
        out_shape=[
            pltpu.VMEM((rows, cols), BF16),
            pltpu.VMEM((heads, 2 * width, 2 * width), BF16),
            pltpu.VMEM((heads, PAD, width), F32),
        ],
        compiler_params=params(16),
        cost_estimate=cost(2e9, rows * cols * 8),
        name="readout",
    )(me, decay, gate, *map(in_vmem, (queries, local)), *memory)


def attend_kernel(start, me_ref, spans_ref, gate_ref, q_ref, k_ref, v_ref, *refs):
    *halo, memory_ref, norm_ref, out_ref, keys_ref, values_ref = refs
    heads, width = norm_ref.shape[0], norm_ref.shape[2]
    rows = q_ref.shape[0] // SPAN_DEV
    middle = LATE - BLOCK
    if start == 0:
        keys_ref[:BLOCK, :] = halo[2][:BLOCK, :]
        values_ref[:BLOCK, :] = halo[2][BLOCK:, :]
    keys_ref[BLOCK - start : LATE - start, :] = halo[1][:middle, :]
    keys_ref[LATE - start :, :] = halo[0][...]
    values_ref[BLOCK - start :, :] = halo[1][middle:, :]
    for head in range(heads):
        at = slice(head * width, (head + 1) * width)
        query = q_ref[start : start + BLOCK, at]
        local = local_block(
            0, start, me_ref, spans_ref, query, keys_ref[:, at], values_ref[:, at],
            k_ref[:rows, at], v_ref[:rows, at],
        )
        out_ref[:, at] = read_block(
            query, memory_ref[head], norm_ref[head, :1, :], gate_ref[head], local
        )


def make_attend(start, queries, keys, values, halo, memory, norm, spans, me, gate):
    rows, cols = queries.shape[0] // SPAN_DEV, queries.shape[1]
    halo = halo if start == 0 else halo[:2]
    before = pltpu.VMEM((BAND - start, cols), BF16)
    operands = [*map(in_vmem, (queries, keys, values, *halo)), memory, norm]
    return pl.pallas_call(
        functools.partial(attend_kernel, start),
        in_specs=[SMEM] * 3 + [VMEM] * len(operands),
        out_specs=VMEM,
        out_shape=pltpu.VMEM((BLOCK, cols), BF16),
        scratch_shapes=[before, before],
        compiler_params=params(24),
        cost_estimate=cost(8e9, 6 * rows * cols * 2),
    )(me, spans, gate, *operands)


def project_kernel(partners, first_row, me_ref, *refs):
    *refs, out_hbm, out_ref, sems = refs
    xs, ws = refs[: len(partners)], list(refs[len(partners) :])
    rows, columns = out_ref.shape
    me = me_ref[0]
    lefts, rights = [], []
    for x_ref, partner in zip(xs, partners):
        if partner:
            half = x_ref.shape[1] // 2
            mine = jnp.where((me & partner) != 0, half, 0)
            parts = [x_ref[:, pl.ds(pl.multiple_of(at, half), half)] for at in (mine, half - mine)]
            lefts.append(jnp.concatenate(parts, axis=1))
            rights.append((ws.pop(0), ws.pop(0)))
        else:
            lefts.append(x_ref[...])
            rights.append((ws.pop(0),))
    copies = []
    for number, start in enumerate(range(0, columns, TILE)):
        at = slice(start, start + TILE)
        acc = None
        for left, right in zip(lefts, rights):
            block = [w_ref[:, at] for w_ref in right]
            block = jnp.concatenate(block, axis=0) if len(block) > 1 else block[0]
            term = jnp.dot(left, block, preferred_element_type=F32)
            acc = term if acc is None else acc + term
        out_ref[:, at] = acc.astype(out_ref.dtype)
        target = out_hbm.at[pl.ds(first_row, rows), pl.ds(start, TILE)]
        copy = pltpu.make_async_copy(out_ref.at[:, pl.ds(start, TILE)], target, sems.at[number])
        copy.start()
        copies.append(copy)
    for copy in copies:
        copy.wait()


def project(start, total_rows, xs, weights, partners, me, out):
    rows = xs[0].shape[0]
    flat = [w for ws in weights for w in ws]
    columns = flat[0].shape[1]
    operands = [me, *map(in_vmem, xs), *map(in_vmem, flat)]
    in_specs = [SMEM] + [VMEM] * (len(operands) - 1)
    aliases = {}
    if out is not None:
        in_specs.append(HBM)
        aliases = {len(operands): 0}
        operands.append(out)
    depth = sum(w.shape[0] for w in flat)
    return pl.pallas_call(
        functools.partial(project_kernel, partners, start),
        in_specs=in_specs,
        out_specs=HBM,
        out_shape=pltpu.HBM((total_rows, columns), BF16),
        scratch_shapes=[
            pltpu.VMEM((rows, columns), BF16),
            pltpu.SemaphoreType.DMA((columns // TILE,)),
        ],
        input_output_aliases=aliases,
        compiler_params=params(24),
        cost_estimate=cost(2 * rows * depth * columns, depth * columns * 2),
    )(*operands)


def swap(x, axis, mask):
    size = lax.axis_size(axis)
    return lax.ppermute(x, axis, [(i, i ^ mask) for i in range(size)])


def body(queries, keys, values, span_bounds, mem_decay, mem_gate, out_weight):
    mem_decay, span_bounds = mem_decay.T, span_bounds.T
    seg_rows = queries.shape[0]
    heads = mem_gate.shape[0]
    width = queries.shape[1] // heads
    seq_size, head_size = lax.axis_size("seq"), lax.axis_size("head")
    assert head_size & (head_size - 1) == 0 and seg_rows == BAND * SPAN_DEV == 4 * BLOCK
    assert seq_size & (seq_size - 1) == 0 and seq_size > 1
    seq_index, head_index = lax.axis_index("seq"), lax.axis_index("head")
    me = seq_index.astype(jnp.int32).reshape(1)
    columns = out_weight.shape[1] // head_size

    masks = sorted(range(1, head_size), reverse=True)
    partners = {mask: 1 << (mask % 2 == 0 and seq_size > 2) for mask in masks if mask > 1}
    slices = [(mask, partners.get(mask, 0)) for mask in (*masks, 0)]
    at = jnp.concatenate([me, head_index.astype(jnp.int32).reshape(1)])
    state, send, *more = make_state(
        queries, keys, values, out_weight, slices, at, heads, width, columns
    )
    queries, keys, values = more[:3]
    tails, blocks = more[3:6], more[6:]
    weights = {}
    for (mask, partner), block in zip(slices, blocks):
        block = swap(block, "head", mask) if mask else block
        weights[mask] = (block, swap(block, "seq", partner)) if partner else (block,)

    halo = []
    for tail in tails:
        halo.append(lax.ppermute(tail, "seq", [(i, i + 1) for i in range(seq_size - 1)]))

    inner, group, distance = [], state, 1
    while True:
        got = swap(send, "seq", distance)
        if 2 * distance >= seq_size:
            break
        shape = pltpu.VMEM(state.shape, F32)
        operands = [me, mem_decay, *inner, got, group]
        memory, group, send = pl.pallas_call(
            functools.partial(fold_kernel, distance),
            in_specs=[SMEM, SMEM] + [VMEM] * (len(operands) - 2),
            out_specs=[VMEM] * 3,
            out_shape=[shape, shape, pltpu.VMEM(send.shape, BF16)],
            compiler_params=params(16),
            cost_estimate=cost(1e9, 5 * state.size * 4),
        )(*operands)
        inner, distance = [memory], 2 * distance
    memory = [*inner, got, group]

    local = make_local(queries, keys, values, span_bounds, me, width)
    own, total, norm = make_readout(distance, queries, local, memory, me, mem_decay, mem_gate)
    chunks = [(BAND, own)]
    for start in (BLOCK, 0):
        own = make_attend(
            start, queries, keys,
            values, halo, total, norm, span_bounds, me, mem_gate,
        )
        chunks.append((start, own))

    out = None
    for start, own in chunks:
        xs = {0: own}
        mask = head_size // 2
        while mask:
            for at, x in list(xs.items()):
                xs[at ^ mask] = swap(x, "head", mask)
            mask //= 2
        order = range(head_size)
        out = project(
            start, seg_rows,
            [xs[i] for i in order], [weights[i] for i in order],
            [partners.get(i, 0) for i in order], me, out,
        )
    return out


def solution(mesh):
    return jax.shard_map(
        body,
        mesh=mesh,
        in_specs=(
            P("seq", "head"),
            P("seq", "head"),
            P("seq", "head"),
            P(),
            P(None, "head"),
            P("head"),
            P("head", None),
        ),
        out_specs=P("seq", "head"),
        check_vma=False,
    )
```

```python
import functools
import math

import jax
import jax.numpy as jnp
from jax import lax
from jax.experimental import pallas as pl
from jax.experimental.pallas import tpu as pltpu
from jax.sharding import PartitionSpec as P

BAND = 512
SPAN_DEV = 2
PAD = 8
SEND_PAD = 16
MASKED = -1e30
BLOCK = 256
TILE = 256
LATE = 384


SMEM = pl.BlockSpec(memory_space=pltpu.SMEM)
VMEM = pl.BlockSpec(memory_space=pltpu.VMEM)
HBM = pl.BlockSpec(memory_space=pltpu.HBM)
F32, BF16 = jnp.float32, jnp.bfloat16


def phi(x):
    return jnp.where(x > 0, x + 1.0, jnp.exp(jnp.minimum(x, 0.0)))


def split(x):
    high = x.astype(BF16)
    return high, (x - high.astype(F32)).astype(BF16)


def params(limit_mib):
    return pltpu.CompilerParams(vmem_limit_bytes=limit_mib << 20)


def in_hbm(x):
    return pltpu.with_memory_space_constraint(x, pltpu.HBM)


def in_vmem(x):
    return pltpu.with_memory_space_constraint(x, pltpu.VMEM)


def cost(flops, moved):
    return pl.CostEstimate(flops=int(flops), bytes_accessed=int(moved), transcendentals=0)


def pack(ref, head, memory, total):
    width = memory.shape[0]
    ref[head, :width, :] = memory.astype(BF16)
    high, low = split(total)
    row = lax.broadcasted_iota(jnp.int32, (SEND_PAD, total.shape[1]), 0)
    both = jnp.where(row == 0, high.astype(F32), jnp.where(row == 1, low.astype(F32), 0.0))
    ref[head, width:, :] = both.astype(BF16)


def unpack(ref, head):
    width = ref.shape[2]
    memory = ref[head, :width, :].astype(F32)
    total = jnp.sum(ref[head, width:, :].astype(F32), axis=0, keepdims=True)
    return memory, total


def store(ref, head, memory, total):
    width = memory.shape[0]
    ref[head, :width, :] = memory
    ref[head, width:, :] = jnp.broadcast_to(total, (PAD, total.shape[1]))


def load(ref, head):
    width = ref.shape[2]
    return ref[head, :width, :], ref[head, width : width + 1, :]


def slice_copies(slices, at_ref, w_hbm, blocks, sems):
    me, head_index = at_ref[0], at_ref[1]
    copies = []
    for number, (mask, partner, part) in enumerate(slices):
        rows, columns = blocks[number].shape
        half = w_hbm.shape[0] // 2
        row = part * rows + (jnp.where((me & partner) != 0, half, 0) if partner else 0)
        col = pl.multiple_of((head_index ^ mask) * columns, columns)
        source = w_hbm.at[pl.ds(pl.multiple_of(row, rows), rows), pl.ds(col, columns)]
        copies.append(pltpu.make_async_copy(source, blocks[number], sems.at[number]))
    return copies


def state_kernel(slices, at_ref, q_hbm, k_hbm, v_hbm, w_hbm, state_ref, send_ref, *refs):
    *outs, sems, w_sems = refs
    (q_buf, k_buf, v_buf), tails, blocks = outs[:3], outs[3:6], outs[6:]
    heads, width = state_ref.shape[0], state_ref.shape[2]
    rows = k_buf.shape[0]
    steps = rows // BLOCK
    copies = []
    for step in range(steps):
        at = pl.ds(step * BLOCK, BLOCK)
        pair = [
            pltpu.make_async_copy(src.at[at], buf.at[at], sems.at[which, step])
            for which, (src, buf) in enumerate(((k_hbm, k_buf), (v_hbm, v_buf)))
        ]
        for copy in pair:
            copy.start()
        copies.append(pair)
    moves = slice_copies(slices, at_ref, w_hbm, blocks, w_sems)
    moves.append(pltpu.make_async_copy(q_hbm, q_buf, w_sems.at[len(slices)]))
    for copy in moves:
        copy.start()
    for step in range(steps):
        for copy in copies[step]:
            copy.wait()
        at = slice(step * BLOCK, (step + 1) * BLOCK)
        for head in range(heads):
            cols = slice(head * width, (head + 1) * width)
            feats = phi(k_buf[at, cols].astype(F32))
            high, low = split(feats)
            vals = v_buf[at, cols]
            dims = (((0,), (0,)), ((), ()))
            memory = lax.dot_general(high, vals, dims, preferred_element_type=F32)
            memory += lax.dot_general(low, vals, dims, preferred_element_type=F32)
            total = jnp.sum(feats, axis=0, keepdims=True)
            if step:
                had, had_total = load(state_ref, head)
                memory, total = memory + had, total + had_total
            store(state_ref, head, memory, total)
            if step == steps - 1:
                pack(send_ref, head, memory, total)
    base = rows - BAND
    middle = LATE - BLOCK
    tails[0][...] = k_buf[base + LATE :, :]
    tails[1][:middle, :] = k_buf[base + BLOCK : base + LATE, :]
    tails[1][middle:, :] = v_buf[base + BLOCK :, :]
    tails[2][:BLOCK, :] = k_buf[base : base + BLOCK, :]
    tails[2][BLOCK:, :] = v_buf[base : base + BLOCK, :]
    for copy in moves:
        copy.wait()


def make_state(queries, keys, values, out_weight, slices, at, heads, width, columns):
    rows, cols = keys.shape
    depth = out_weight.shape[0]
    split_in = [sum(other[0] == mask for other in slices) for mask, _, _ in slices]
    sizes = [depth // (2 * n if by else n) for n, (_, by, _) in zip(split_in, slices)]
    steps = rows // BLOCK
    tails = (BAND - LATE, LATE - BLOCK + BAND - BLOCK, 2 * BLOCK)
    return pl.pallas_call(
        functools.partial(state_kernel, slices),
        in_specs=[SMEM, HBM, HBM, HBM, HBM],
        out_specs=[VMEM] * (8 + len(slices)),
        out_shape=[
            pltpu.VMEM((heads, width + PAD, width), F32),
            pltpu.VMEM((heads, width + SEND_PAD, width), BF16),
            *[pltpu.VMEM((rows, cols), BF16)] * 3,
            *(pltpu.VMEM((tail, cols), BF16) for tail in tails),
            *(pltpu.VMEM((rows_, columns), BF16) for rows_ in sizes),
        ],
        scratch_shapes=[
            pltpu.SemaphoreType.DMA((2, steps)),
            pltpu.SemaphoreType.DMA((len(slices) + 1,)),
        ],
        compiler_params=params(24),
        cost_estimate=cost(1e10, 4 * keys.size * 2),
        name="state",
    )(at, in_hbm(queries), in_hbm(keys), in_hbm(values), in_hbm(out_weight))


def fold(distance, me, decay_ref, head, memory, group, got):
    upper = (me & distance) != 0
    base = me & ~(distance - 1)
    above = base | distance
    through, before = 1.0, 1.0
    for step in range(distance):
        through = through * decay_ref[head, above + step]
        if step < distance - 1:
            factor = decay_ref[head, base + step]
            before = before * jnp.where(base + step < me, factor, 1.0)
    before = jnp.where(upper, before, 0.0)
    low, high = jnp.where(upper, 1.0, through), jnp.where(upper, through, 1.0)
    both = [low * mine + high * theirs for mine, theirs in zip(group, got)]
    if memory is None:
        memory = [before * theirs for theirs in got]
    else:
        memory = [mine + before * theirs for mine, theirs in zip(memory, got)]
    return memory, both


def fold_kernel(distance, me_ref, decay_ref, *refs):
    *inner, got_ref, group_ref, memory_ref, total_ref, send_ref = refs
    me = me_ref[0]
    for head in range(group_ref.shape[0]):
        memory = load(inner[0], head) if inner else None
        memory, both = fold(
            distance, me, decay_ref, head, memory, load(group_ref, head), unpack(got_ref, head)
        )
        store(memory_ref, head, *memory)
        store(total_ref, head, *both)
        pack(send_ref, head, *both)


def local_block(half, start, me_ref, spans_ref, query, keys_before, values_before, keys, values):
    me = me_ref[0]
    rows, width = keys.shape
    factor = math.log2(math.e) / math.sqrt(width)
    origin = (me * SPAN_DEV + half) * rows
    first = spans_ref[0, me * SPAN_DEV + half] - origin
    end = spans_ref[1, me * SPAN_DEV + half] - origin
    shift = 0 if half else jnp.where(me > 0, 0, rows + 1)
    dims = (((1,), (1,)), ((), ()))
    prev = lax.dot_general(query, keys_before, dims, preferred_element_type=F32)
    own = lax.dot_general(query, keys, dims, preferred_element_type=F32)
    row = start + lax.broadcasted_iota(jnp.int32, (query.shape[0], 1), 0)
    limit = jnp.where((row >= first) & (row < end), end - 1, row)
    col = lax.broadcasted_iota(jnp.int32, prev.shape, 1) + start
    prev = jnp.where(col > row + shift, prev, MASKED)
    col = lax.broadcasted_iota(jnp.int32, own.shape, 1)
    own = jnp.where(col <= limit, own, MASKED)
    top = jnp.maximum(jnp.max(prev, axis=1, keepdims=True), jnp.max(own, axis=1, keepdims=True))
    prev = jnp.exp2((prev - top) * factor)
    own = jnp.exp2((own - top) * factor)
    total = jnp.sum(prev, axis=1, keepdims=True) + jnp.sum(own, axis=1, keepdims=True)
    mixed = jnp.dot(prev.astype(BF16), values_before, preferred_element_type=F32)
    mixed += jnp.dot(own.astype(BF16), values, preferred_element_type=F32)
    return mixed / total


def read_block(query, memory, norm, gate, local):
    width = query.shape[1]
    feats = phi(query.astype(F32))
    left = jnp.concatenate(split(feats), axis=1)
    both = jnp.dot(left, memory, preferred_element_type=F32)
    numer = both[:, :width] + both[:, width:]
    denom = jnp.sum(feats * norm, axis=1, keepdims=True) + 1.0
    gate = 1.0 / (1.0 + jnp.exp(jnp.full((1, width), -gate, F32)))
    return (gate * (numer / denom) + (1.0 - gate) * local).astype(BF16)


def local_kernel(width, me_ref, spans_ref, q_ref, k_ref, v_ref, out_ref):
    rows, cols = out_ref.shape
    for head in range(cols // width):
        at = slice(head * width, (head + 1) * width)
        for start in range(0, rows, BLOCK):
            out_ref[start : start + BLOCK, at] = local_block(
                1, start, me_ref, spans_ref, q_ref[rows + start : rows + start + BLOCK, at],
                k_ref[start:rows, at], v_ref[start:rows, at], k_ref[rows:, at], v_ref[rows:, at],
            )


def make_local(queries, keys, values, spans, me, width):
    rows, cols = queries.shape[0] // SPAN_DEV, queries.shape[1]
    return pl.pallas_call(
        functools.partial(local_kernel, width),
        in_specs=[SMEM, SMEM, VMEM, VMEM, VMEM],
        out_specs=VMEM,
        out_shape=pltpu.VMEM((rows, cols), F32),
        compiler_params=params(24),
        cost_estimate=cost(1.5e10, 6 * rows * cols * 2),
        name="local",
    )(me, spans, *map(in_vmem, (queries, keys, values)))


def readout_kernel(distance, me_ref, decay_ref, gate_ref, q_ref, local_ref, *refs):
    *inner, got_ref, group_ref, out_ref, memory_ref, norm_ref = refs
    me = me_ref[0]
    heads, width = group_ref.shape[0], group_ref.shape[2]
    rows = out_ref.shape[0]
    for head in range(heads):
        had = load(inner[0], head) if inner else None
        (memory, norm), unused = fold(
            distance, me, decay_ref, head, had, load(group_ref, head), unpack(got_ref, head)
        )
        high, low = split(memory)
        memory_ref[head, :width, :width] = high
        memory_ref[head, :width, width:] = low
        memory_ref[head, width:, :width] = high
        memory_ref[head, width:, width:] = jnp.zeros_like(low)
        norm_ref[head] = jnp.broadcast_to(norm, (PAD, width))
        at = slice(head * width, (head + 1) * width)
        out_ref[:, at] = read_block(
            q_ref[-rows:, at], memory_ref[head], norm, gate_ref[head], local_ref[:, at]
        )


def make_readout(distance, queries, local, memory, me, decay, gate):
    rows, cols = local.shape
    heads, _, width = memory[-1].shape
    return pl.pallas_call(
        functools.partial(readout_kernel, distance),
        in_specs=[SMEM, SMEM, SMEM] + [VMEM] * (2 + len(memory)),
        out_specs=[VMEM] * 3,
        out_shape=[
            pltpu.VMEM((rows, cols), BF16),
            pltpu.VMEM((heads, 2 * width, 2 * width), BF16),
            pltpu.VMEM((heads, PAD, width), F32),
        ],
        compiler_params=params(16),
        cost_estimate=cost(2e9, rows * cols * 8),
        name="readout",
    )(me, decay, gate, *map(in_vmem, (queries, local)), *memory)


def attend_kernel(start, me_ref, spans_ref, gate_ref, q_ref, k_ref, v_ref, *refs):
    *halo, memory_ref, norm_ref, out_ref, keys_ref, values_ref = refs
    heads, width = norm_ref.shape[0], norm_ref.shape[2]
    rows = q_ref.shape[0] // SPAN_DEV
    middle = LATE - BLOCK
    if start == 0:
        keys_ref[:BLOCK, :] = halo[2][:BLOCK, :]
        values_ref[:BLOCK, :] = halo[2][BLOCK:, :]
    keys_ref[BLOCK - start : LATE - start, :] = halo[1][:middle, :]
    keys_ref[LATE - start :, :] = halo[0][...]
    values_ref[BLOCK - start :, :] = halo[1][middle:, :]
    for head in range(heads):
        at = slice(head * width, (head + 1) * width)
        query = q_ref[start : start + BLOCK, at]
        local = local_block(
            0, start, me_ref, spans_ref, query, keys_ref[:, at], values_ref[:, at],
            k_ref[:rows, at], v_ref[:rows, at],
        )
        out_ref[:, at] = read_block(
            query, memory_ref[head], norm_ref[head, :1, :], gate_ref[head], local
        )


def make_attend(start, queries, keys, values, halo, memory, norm, spans, me, gate):
    rows, cols = queries.shape[0] // SPAN_DEV, queries.shape[1]
    before = pltpu.VMEM((BAND - start, cols), BF16)
    halo = halo if start == 0 else halo[:2]
    operands = [*map(in_vmem, (queries, keys, values, *halo)), memory, norm]
    return pl.pallas_call(
        functools.partial(attend_kernel, start),
        in_specs=[SMEM] * 3 + [VMEM] * len(operands),
        out_specs=VMEM,
        out_shape=pltpu.VMEM((BLOCK, cols), BF16),
        scratch_shapes=[before, before],
        compiler_params=params(24),
        cost_estimate=cost(8e9, 6 * rows * cols * 2),
    )(me, spans, gate, *operands)


def project_kernel(plan, first_row, adds, done, me_ref, *refs):
    if done:
        *refs, out_hbm, out_ref, sems = refs
    else:
        *refs, out_ref = refs
    refs = list(refs)
    copies = []
    for number, row in enumerate(done):
        ready = refs.pop()
        target = out_hbm.at[pl.ds(row, ready.shape[0])]
        copies.append(pltpu.make_async_copy(ready, target, sems.at[number]))
        copies[-1].start()
    me = me_ref[0]
    lefts, rights = [], []
    for pieces in plan:
        x_ref = refs.pop(0)
        parts = []
        for piece in pieces:
            if piece is None:
                parts.append(x_ref[...])
                continue
            partner, count, part, own = piece
            half = x_ref.shape[1] // 2
            size = half // count
            mine = jnp.where((me & partner) != 0, half, 0)
            at = (mine if own else half - mine) + part * size
            parts.append(x_ref[:, pl.ds(pl.multiple_of(at, size), size)])
        lefts.append(jnp.concatenate(parts, axis=1) if len(parts) > 1 else parts[0])
    for pieces in plan:
        rights.append([refs.pop(0) for _ in pieces])
    sums_ref = refs.pop(0) if adds else None
    rows, columns = out_ref.shape
    for number, start in enumerate(range(0, columns, TILE), len(done)):
        at = slice(start, start + TILE)
        acc = sums_ref[:, at] if adds else None
        for left, right in zip(lefts, rights):
            block = [w_ref[:, at] for w_ref in right]
            block = jnp.concatenate(block, axis=0) if len(block) > 1 else block[0]
            term = jnp.dot(left, block, preferred_element_type=F32)
            acc = term if acc is None else acc + term
        out_ref[:, at] = acc.astype(out_ref.dtype)
        if done:
            target = out_hbm.at[pl.ds(first_row, rows), pl.ds(start, TILE)]
            source = out_ref.at[:, pl.ds(start, TILE)]
            copies.append(pltpu.make_async_copy(source, target, sems.at[number]))
            copies[-1].start()
    for copy in copies:
        copy.wait()


def project(start, total_rows, dtype, terms, me, sums=None, done=()):
    xs = [x for x, _ in terms]
    flat = [w for _, pieces in terms for _, w in pieces]
    plan = [[kind for kind, _ in pieces] for _, pieces in terms]
    rows, columns = xs[0].shape[0], flat[0].shape[1]
    depth = sum(w.shape[0] for w in flat)
    operands = [*xs, *flat, *([] if sums is None else [sums]), *(x for _, x in reversed(done))]
    copies = pltpu.SemaphoreType.DMA((len(done) + columns // TILE,))
    return pl.pallas_call(
        functools.partial(project_kernel, plan, start, sums is not None, [row for row, _ in done]),
        in_specs=[SMEM] + [VMEM] * len(operands),
        out_specs=HBM if done else VMEM,
        out_shape=pltpu.HBM((total_rows, columns), BF16) if done else pltpu.VMEM((rows, columns), dtype),
        scratch_shapes=[pltpu.VMEM((rows, columns), BF16), copies] if done else [],
        compiler_params=params(24),
        cost_estimate=cost(2 * rows * depth * columns, depth * columns * 2),
    )(me, *map(in_vmem, operands))


def swap(x, axis, mask):
    size = lax.axis_size(axis)
    return lax.ppermute(x, axis, [(i, i ^ mask) for i in range(size)])


def body(queries, keys, values, span_bounds, mem_decay, mem_gate, out_weight):
    mem_decay, span_bounds = mem_decay.T, span_bounds.T
    seg_rows = queries.shape[0]
    heads = mem_gate.shape[0]
    width = queries.shape[1] // heads
    seq_size, head_size = lax.axis_size("seq"), lax.axis_size("head")
    assert head_size & (head_size - 1) == 0 and seg_rows == BAND * SPAN_DEV == 4 * BLOCK
    assert seq_size & (seq_size - 1) == 0 and seq_size > 1
    seq_index, head_index = lax.axis_index("seq"), lax.axis_index("head")
    me = seq_index.astype(jnp.int32).reshape(1)
    columns = out_weight.shape[1] // head_size

    masks = sorted(range(1, head_size), reverse=True)
    partners = {
        mask: (2, 1) if mask % 2 == 0 and seq_size > 2 else (1, 1) for mask in masks if mask > 1
    }
    slices = []
    for mask in (*masks, 0):
        partner, parts = partners.get(mask, (0, 1))
        slices += [(mask, partner, part) for part in range(parts)]
    at = jnp.concatenate([me, head_index.astype(jnp.int32).reshape(1)])
    state, send, *more = make_state(
        queries, keys, values, out_weight, slices, at, heads, width, columns
    )
    queries, keys, values = more[:3]
    tails, blocks = more[3:6], more[6:]
    weights = {mask: [] for mask in (*masks, 0)}
    for (mask, partner, part), block in zip(slices, blocks):
        block = swap(block, "head", mask) if mask else block
        if partner:
            count = partners[mask][1]
            other = swap(block, "seq", partner)
            weights[mask].append(((partner, count, part, True), block))
            weights[mask].append(((partner, count, part, False), other))
        else:
            weights[mask].append((None, block))

    halo = []
    for tail in tails:
        halo.append(lax.ppermute(tail, "seq", [(i, i + 1) for i in range(seq_size - 1)]))

    inner, group, distance = [], state, 1
    while True:
        got = swap(send, "seq", distance)
        if 2 * distance >= seq_size:
            break
        shape = pltpu.VMEM(state.shape, F32)
        operands = [me, mem_decay, *inner, got, group]
        memory, group, send = pl.pallas_call(
            functools.partial(fold_kernel, distance),
            in_specs=[SMEM, SMEM] + [VMEM] * (len(operands) - 2),
            out_specs=[VMEM] * 3,
            out_shape=[shape, shape, pltpu.VMEM(send.shape, BF16)],
            compiler_params=params(16),
            cost_estimate=cost(1e9, 5 * state.size * 4),
        )(*operands)
        inner, distance = [memory], 2 * distance
    memory = [*inner, got, group]

    local = make_local(queries, keys, values, span_bounds, me, width)
    own, total, norm = make_readout(distance, queries, local, memory, me, mem_decay, mem_gate)
    chunks = [(BAND, own)]
    for start in (BLOCK, 0):
        own = make_attend(
            start, queries, keys,
            values, halo, total, norm, span_bounds, me, mem_gate,
        )
        chunks.append((start, own))

    done = []
    for number, (start, own) in enumerate(chunks):
        xs = {0: own}
        mask = head_size // 2
        while mask:
            for at, x in list(xs.items()):
                xs[at ^ mask] = swap(x, "head", mask)
            mask //= 2
        terms = [(xs[i], weights[i]) for i in range(head_size)]
        sums = None
        if number == 0 and partners:
            late = lambda kind: kind is not None and not kind[3]
            early = [(x, [w for w in ws if not late(w[0])]) for x, ws in terms]
            sums = project(start, seg_rows, F32, early, me)
            terms = [(xs[i], [w for w in weights[i] if late(w[0])]) for i in partners]
        ready = done if number == len(chunks) - 1 else ()
        out = project(
            start, seg_rows, BF16, terms, me, sums,
            ready,
        )
        done.append((start, out))
    return out


def solution(mesh):
    return jax.shard_map(
        body,
        mesh=mesh,
        in_specs=(
            P("seq", "head"),
            P("seq", "head"),
            P("seq", "head"),
            P(),
            P(None, "head"),
            P("head"),
            P("head", None),
        ),
        out_specs=P("seq", "head"),
        check_vma=False,
    )
```

```python
import functools
import math

import jax
import jax.numpy as jnp
from jax import lax
from jax.experimental import pallas as pl
from jax.experimental.pallas import tpu as pltpu
from jax.sharding import PartitionSpec as P

BAND = 512
SPAN_DEV = 2
PAD = 8
SEND_PAD = 16
MASKED = -1e30
BLOCK = 256
TILE = 256
EARLY = 320
LATE = 384


SMEM = pl.BlockSpec(memory_space=pltpu.SMEM)
VMEM = pl.BlockSpec(memory_space=pltpu.VMEM)
HBM = pl.BlockSpec(memory_space=pltpu.HBM)
F32, BF16 = jnp.float32, jnp.bfloat16


def phi(x):
    return jnp.where(x > 0, x + 1.0, jnp.exp(jnp.minimum(x, 0.0)))


def split(x):
    high = x.astype(BF16)
    return high, (x - high.astype(F32)).astype(BF16)


def params(limit_mib):
    return pltpu.CompilerParams(vmem_limit_bytes=limit_mib << 20)


def in_hbm(x):
    return pltpu.with_memory_space_constraint(x, pltpu.HBM)


def in_vmem(x):
    return pltpu.with_memory_space_constraint(x, pltpu.VMEM)


def cost(flops, moved):
    return pl.CostEstimate(flops=int(flops), bytes_accessed=int(moved), transcendentals=0)


def pack(ref, head, memory, total):
    width = memory.shape[0]
    ref[head, :width, :] = memory.astype(BF16)
    high, low = split(total)
    row = lax.broadcasted_iota(jnp.int32, (SEND_PAD, total.shape[1]), 0)
    both = jnp.where(row == 0, high.astype(F32), jnp.where(row == 1, low.astype(F32), 0.0))
    ref[head, width:, :] = both.astype(BF16)


def unpack(ref, head):
    width = ref.shape[2]
    memory = ref[head, :width, :].astype(F32)
    total = jnp.sum(ref[head, width:, :].astype(F32), axis=0, keepdims=True)
    return memory, total


def store(ref, head, memory, total):
    width = memory.shape[0]
    ref[head, :width, :] = memory
    ref[head, width:, :] = jnp.broadcast_to(total, (PAD, total.shape[1]))


def load(ref, head):
    width = ref.shape[2]
    return ref[head, :width, :], ref[head, width : width + 1, :]


def slice_copies(slices, at_ref, w_hbm, blocks, sems):
    me, head_index = at_ref[0], at_ref[1]
    copies = []
    for number, (mask, partner, part) in enumerate(slices):
        rows, columns = blocks[number].shape
        half = w_hbm.shape[0] // 2
        row = part * rows + (jnp.where((me & partner) != 0, half, 0) if partner else 0)
        col = pl.multiple_of((head_index ^ mask) * columns, columns)
        source = w_hbm.at[pl.ds(pl.multiple_of(row, rows), rows), pl.ds(col, columns)]
        copies.append(pltpu.make_async_copy(source, blocks[number], sems.at[number]))
    return copies


def state_kernel(slices, at_ref, q_hbm, k_hbm, v_hbm, w_hbm, state_ref, send_ref, *refs):
    *outs, sems, w_sems = refs
    (q_buf, k_buf, v_buf), tails, blocks = outs[:3], outs[3:6], outs[6:]
    heads, width = state_ref.shape[0], state_ref.shape[2]
    rows = k_buf.shape[0]
    steps = rows // BLOCK
    copies = []
    for step in range(steps):
        at = pl.ds(step * BLOCK, BLOCK)
        pair = [
            pltpu.make_async_copy(src.at[at], buf.at[at], sems.at[which, step])
            for which, (src, buf) in enumerate(((k_hbm, k_buf), (v_hbm, v_buf)))
        ]
        for copy in pair:
            copy.start()
        copies.append(pair)
    moves = slice_copies(slices, at_ref, w_hbm, blocks, w_sems)
    moves.append(pltpu.make_async_copy(q_hbm, q_buf, w_sems.at[len(slices)]))
    for copy in moves:
        copy.start()
    for step in range(steps):
        for copy in copies[step]:
            copy.wait()
        at = slice(step * BLOCK, (step + 1) * BLOCK)
        for head in range(heads):
            cols = slice(head * width, (head + 1) * width)
            feats = phi(k_buf[at, cols].astype(F32))
            high, low = split(feats)
            vals = v_buf[at, cols]
            dims = (((0,), (0,)), ((), ()))
            memory = lax.dot_general(high, vals, dims, preferred_element_type=F32)
            memory += lax.dot_general(low, vals, dims, preferred_element_type=F32)
            total = jnp.sum(feats, axis=0, keepdims=True)
            if step:
                had, had_total = load(state_ref, head)
                memory, total = memory + had, total + had_total
            store(state_ref, head, memory, total)
            if step == steps - 1:
                pack(send_ref, head, memory, total)
    base = rows - BAND
    middle = LATE - EARLY
    tails[0][...] = k_buf[base + LATE :, :]
    tails[1][:middle, :] = k_buf[base + EARLY : base + LATE, :]
    tails[1][middle:, :] = v_buf[base + EARLY :, :]
    tails[2][:EARLY, :] = k_buf[base : base + EARLY, :]
    tails[2][EARLY:, :] = v_buf[base : base + EARLY, :]
    for copy in moves:
        copy.wait()


def make_state(queries, keys, values, out_weight, slices, at, heads, width, columns):
    rows, cols = keys.shape
    depth = out_weight.shape[0]
    split_in = [sum(other[0] == mask for other in slices) for mask, _, _ in slices]
    sizes = [depth // (2 * n if by else n) for n, (_, by, _) in zip(split_in, slices)]
    steps = rows // BLOCK
    tails = (BAND - LATE, LATE - EARLY + BAND - EARLY, 2 * EARLY)
    return pl.pallas_call(
        functools.partial(state_kernel, slices),
        in_specs=[SMEM, HBM, HBM, HBM, HBM],
        out_specs=[VMEM] * (8 + len(slices)),
        out_shape=[
            pltpu.VMEM((heads, width + PAD, width), F32),
            pltpu.VMEM((heads, width + SEND_PAD, width), BF16),
            *[pltpu.VMEM((rows, cols), BF16)] * 3,
            *(pltpu.VMEM((tail, cols), BF16) for tail in tails),
            *(pltpu.VMEM((rows_, columns), BF16) for rows_ in sizes),
        ],
        scratch_shapes=[
            pltpu.SemaphoreType.DMA((2, steps)),
            pltpu.SemaphoreType.DMA((len(slices) + 1,)),
        ],
        compiler_params=params(24),
        cost_estimate=cost(1e10, 4 * keys.size * 2),
        name="state",
    )(at, in_hbm(queries), in_hbm(keys), in_hbm(values), in_hbm(out_weight))


def fold(distance, me, decay_ref, head, memory, group, got):
    upper = (me & distance) != 0
    base = me & ~(distance - 1)
    above = base | distance
    through, before = 1.0, 1.0
    for step in range(distance):
        through = through * decay_ref[head, above + step]
        if step < distance - 1:
            factor = decay_ref[head, base + step]
            before = before * jnp.where(base + step < me, factor, 1.0)
    before = jnp.where(upper, before, 0.0)
    low, high = jnp.where(upper, 1.0, through), jnp.where(upper, through, 1.0)
    both = [low * mine + high * theirs for mine, theirs in zip(group, got)]
    if memory is None:
        memory = [before * theirs for theirs in got]
    else:
        memory = [mine + before * theirs for mine, theirs in zip(memory, got)]
    return memory, both


def fold_kernel(distance, me_ref, decay_ref, *refs):
    *inner, got_ref, group_ref, memory_ref, total_ref, send_ref = refs
    me = me_ref[0]
    for head in range(group_ref.shape[0]):
        memory = load(inner[0], head) if inner else None
        memory, both = fold(
            distance, me, decay_ref, head, memory, load(group_ref, head), unpack(got_ref, head)
        )
        store(memory_ref, head, *memory)
        store(total_ref, head, *both)
        pack(send_ref, head, *both)


def local_block(half, start, base, me_ref, spans_ref, query, keys_before, values_before, keys, values):
    me = me_ref[0]
    rows, width = keys.shape
    factor = math.log2(math.e) / math.sqrt(width)
    origin = (me * SPAN_DEV + half) * rows
    first = spans_ref[0, me * SPAN_DEV + half] - origin
    end = spans_ref[1, me * SPAN_DEV + half] - origin
    shift = 0 if half else jnp.where(me > 0, 0, rows + 1)
    dims = (((1,), (1,)), ((), ()))
    prev = lax.dot_general(query, keys_before, dims, preferred_element_type=F32)
    own = lax.dot_general(query, keys, dims, preferred_element_type=F32)
    row = start + lax.broadcasted_iota(jnp.int32, (query.shape[0], 1), 0)
    limit = jnp.where((row >= first) & (row < end), end - 1, row)
    col = lax.broadcasted_iota(jnp.int32, prev.shape, 1) + base
    prev = jnp.where(col > row + shift, prev, MASKED)
    col = lax.broadcasted_iota(jnp.int32, own.shape, 1)
    own = jnp.where(col <= limit, own, MASKED)
    top = jnp.maximum(jnp.max(prev, axis=1, keepdims=True), jnp.max(own, axis=1, keepdims=True))
    prev = jnp.exp2((prev - top) * factor)
    own = jnp.exp2((own - top) * factor)
    total = jnp.sum(prev, axis=1, keepdims=True) + jnp.sum(own, axis=1, keepdims=True)
    mixed = jnp.dot(prev.astype(BF16), values_before, preferred_element_type=F32)
    mixed += jnp.dot(own.astype(BF16), values, preferred_element_type=F32)
    return mixed / total


def read_block(query, memory, norm, gate, local):
    width = query.shape[1]
    feats = phi(query.astype(F32))
    left = jnp.concatenate(split(feats), axis=1)
    both = jnp.dot(left, memory, preferred_element_type=F32)
    numer = both[:, :width] + both[:, width:]
    denom = jnp.sum(feats * norm, axis=1, keepdims=True) + 1.0
    gate = 1.0 / (1.0 + jnp.exp(jnp.full((1, width), -gate, F32)))
    return (gate * (numer / denom) + (1.0 - gate) * local).astype(BF16)


def local_kernel(width, me_ref, spans_ref, q_ref, k_ref, v_ref, out_ref):
    rows, cols = out_ref.shape
    for head in range(cols // width):
        at = slice(head * width, (head + 1) * width)
        for start in range(0, rows, BLOCK):
            out_ref[start : start + BLOCK, at] = local_block(
                1, start, start, me_ref, spans_ref, q_ref[rows + start : rows + start + BLOCK, at],
                k_ref[start:rows, at], v_ref[start:rows, at], k_ref[rows:, at], v_ref[rows:, at],
            )


def make_local(queries, keys, values, spans, me, width):
    rows, cols = queries.shape[0] // SPAN_DEV, queries.shape[1]
    return pl.pallas_call(
        functools.partial(local_kernel, width),
        in_specs=[SMEM, SMEM, VMEM, VMEM, VMEM],
        out_specs=VMEM,
        out_shape=pltpu.VMEM((rows, cols), F32),
        compiler_params=params(24),
        cost_estimate=cost(1.5e10, 6 * rows * cols * 2),
        name="local",
    )(me, spans, *map(in_vmem, (queries, keys, values)))


def readout_kernel(distance, me_ref, decay_ref, gate_ref, q_ref, local_ref, *refs):
    *inner, got_ref, group_ref, out_ref, memory_ref, norm_ref = refs
    me = me_ref[0]
    heads, width = group_ref.shape[0], group_ref.shape[2]
    rows = out_ref.shape[0]
    for head in range(heads):
        had = load(inner[0], head) if inner else None
        (memory, norm), unused = fold(
            distance, me, decay_ref, head, had, load(group_ref, head), unpack(got_ref, head)
        )
        high, low = split(memory)
        memory_ref[head, :width, :width] = high
        memory_ref[head, :width, width:] = low
        memory_ref[head, width:, :width] = high
        memory_ref[head, width:, width:] = jnp.zeros_like(low)
        norm_ref[head] = jnp.broadcast_to(norm, (PAD, width))
        at = slice(head * width, (head + 1) * width)
        out_ref[:, at] = read_block(
            q_ref[-rows:, at], memory_ref[head], norm, gate_ref[head], local_ref[:, at]
        )


def make_readout(distance, queries, local, memory, me, decay, gate):
    rows, cols = local.shape
    heads, _, width = memory[-1].shape
    return pl.pallas_call(
        functools.partial(readout_kernel, distance),
        in_specs=[SMEM, SMEM, SMEM] + [VMEM] * (2 + len(memory)),
        out_specs=[VMEM] * 3,
        out_shape=[
            pltpu.VMEM((rows, cols), BF16),
            pltpu.VMEM((heads, 2 * width, 2 * width), BF16),
            pltpu.VMEM((heads, PAD, width), F32),
        ],
        compiler_params=params(16),
        cost_estimate=cost(2e9, rows * cols * 8),
        name="readout",
    )(me, decay, gate, *map(in_vmem, (queries, local)), *memory)


def attend_kernel(start, base, me_ref, spans_ref, gate_ref, q_ref, k_ref, v_ref, *refs):
    *halo, memory_ref, norm_ref, out_ref, keys_ref, values_ref = refs
    heads, width = norm_ref.shape[0], norm_ref.shape[2]
    rows = q_ref.shape[0] // SPAN_DEV
    middle = LATE - EARLY
    if start == 0:
        keys_ref[:EARLY, :] = halo[2][:EARLY, :]
        values_ref[:EARLY, :] = halo[2][EARLY:, :]
    elif base < EARLY:
        for ref in (keys_ref, values_ref):
            ref[: EARLY - base, :] = jnp.zeros((EARLY - base, ref.shape[1]), ref.dtype)
    keys_ref[EARLY - base : LATE - base, :] = halo[1][:middle, :]
    keys_ref[LATE - base :, :] = halo[0][...]
    values_ref[EARLY - base :, :] = halo[1][middle:, :]
    for head in range(heads):
        at = slice(head * width, (head + 1) * width)
        query = q_ref[start : start + out_ref.shape[0], at]
        local = local_block(
            0, start, base, me_ref, spans_ref, query, keys_ref[:, at], values_ref[:, at],
            k_ref[:rows, at], v_ref[:rows, at],
        )
        out_ref[:, at] = read_block(
            query, memory_ref[head], norm_ref[head, :1, :], gate_ref[head], local
        )


def make_attend(start, size, queries, keys, values, halo, memory, norm, spans, me, gate):
    rows, cols = queries.shape[0] // SPAN_DEV, queries.shape[1]
    base = start // BLOCK * BLOCK
    before = pltpu.VMEM((BAND - base, cols), BF16)
    halo = halo if start == 0 else halo[:2]
    operands = [*map(in_vmem, (queries, keys, values, *halo)), memory, norm]
    return pl.pallas_call(
        functools.partial(attend_kernel, start, base),
        in_specs=[SMEM] * 3 + [VMEM] * len(operands),
        out_specs=VMEM,
        out_shape=pltpu.VMEM((size, cols), BF16),
        scratch_shapes=[before, before],
        compiler_params=params(24),
        cost_estimate=cost(8e9, 6 * rows * cols * 2),
    )(me, spans, gate, *operands)


def project_kernel(plan, first_row, adds, done, me_ref, *refs):
    if done:
        *refs, out_hbm, out_ref, sems = refs
    else:
        *refs, out_ref = refs
    refs = list(refs)
    copies = []
    for number, row in enumerate(done):
        ready = refs.pop()
        target = out_hbm.at[pl.ds(row, ready.shape[0])]
        copies.append(pltpu.make_async_copy(ready, target, sems.at[number]))
        copies[-1].start()
    me = me_ref[0]
    lefts, rights = [], []
    for pieces in plan:
        x_ref = refs.pop(0)
        parts = []
        for piece in pieces:
            if piece is None:
                parts.append(x_ref[...])
                continue
            partner, count, part, own = piece
            half = x_ref.shape[1] // 2
            size = half // count
            mine = jnp.where((me & partner) != 0, half, 0)
            at = (mine if own else half - mine) + part * size
            parts.append(x_ref[:, pl.ds(pl.multiple_of(at, size), size)])
        lefts.append(jnp.concatenate(parts, axis=1) if len(parts) > 1 else parts[0])
    for pieces in plan:
        rights.append([refs.pop(0) for _ in pieces])
    sums_ref = refs.pop(0) if adds else None
    rows, columns = out_ref.shape
    for number, start in enumerate(range(0, columns, TILE), len(done)):
        at = slice(start, start + TILE)
        acc = sums_ref[:, at] if adds else None
        for left, right in zip(lefts, rights):
            block = [w_ref[:, at] for w_ref in right]
            block = jnp.concatenate(block, axis=0) if len(block) > 1 else block[0]
            term = jnp.dot(left, block, preferred_element_type=F32)
            acc = term if acc is None else acc + term
        out_ref[:, at] = acc.astype(out_ref.dtype)
        if done:
            target = out_hbm.at[pl.ds(first_row, rows), pl.ds(start, TILE)]
            source = out_ref.at[:, pl.ds(start, TILE)]
            copies.append(pltpu.make_async_copy(source, target, sems.at[number]))
            copies[-1].start()
    for copy in copies:
        copy.wait()


def project(start, total_rows, dtype, terms, me, sums=None, done=()):
    xs = [x for x, _ in terms]
    flat = [w for _, pieces in terms for _, w in pieces]
    plan = [[kind for kind, _ in pieces] for _, pieces in terms]
    rows, columns = xs[0].shape[0], flat[0].shape[1]
    depth = sum(w.shape[0] for w in flat)
    operands = [*xs, *flat, *([] if sums is None else [sums]), *(x for _, x in reversed(done))]
    copies = pltpu.SemaphoreType.DMA((len(done) + columns // TILE,))
    return pl.pallas_call(
        functools.partial(project_kernel, plan, start, sums is not None, [row for row, _ in done]),
        in_specs=[SMEM] + [VMEM] * len(operands),
        out_specs=HBM if done else VMEM,
        out_shape=pltpu.HBM((total_rows, columns), BF16) if done else pltpu.VMEM((rows, columns), dtype),
        scratch_shapes=[pltpu.VMEM((rows, columns), BF16), copies] if done else [],
        compiler_params=params(24),
        cost_estimate=cost(2 * rows * depth * columns, depth * columns * 2),
    )(me, *map(in_vmem, operands))


def swap(x, axis, mask):
    size = lax.axis_size(axis)
    return lax.ppermute(x, axis, [(i, i ^ mask) for i in range(size)])


def body(queries, keys, values, span_bounds, mem_decay, mem_gate, out_weight):
    mem_decay, span_bounds = mem_decay.T, span_bounds.T
    seg_rows = queries.shape[0]
    heads = mem_gate.shape[0]
    width = queries.shape[1] // heads
    seq_size, head_size = lax.axis_size("seq"), lax.axis_size("head")
    assert head_size & (head_size - 1) == 0 and seg_rows == BAND * SPAN_DEV == 4 * BLOCK
    assert seq_size & (seq_size - 1) == 0 and seq_size > 1
    seq_index, head_index = lax.axis_index("seq"), lax.axis_index("head")
    me = seq_index.astype(jnp.int32).reshape(1)
    columns = out_weight.shape[1] // head_size

    masks = sorted(range(1, head_size), reverse=True)
    partners = {
        mask: (2, 1) if mask % 2 == 0 and seq_size > 2 else (1, 1) for mask in masks if mask > 1
    }
    slices = []
    for mask in (*masks, 0):
        partner, parts = partners.get(mask, (0, 1))
        slices += [(mask, partner, part) for part in range(parts)]
    at = jnp.concatenate([me, head_index.astype(jnp.int32).reshape(1)])
    state, send, *more = make_state(
        queries, keys, values, out_weight, slices, at, heads, width, columns
    )
    queries, keys, values = more[:3]
    tails, blocks = more[3:6], more[6:]
    weights = {mask: [] for mask in (*masks, 0)}
    for (mask, partner, part), block in zip(slices, blocks):
        block = swap(block, "head", mask) if mask else block
        if partner:
            count = partners[mask][1]
            other = swap(block, "seq", partner)
            weights[mask].append(((partner, count, part, True), block))
            weights[mask].append(((partner, count, part, False), other))
        else:
            weights[mask].append((None, block))

    halo = []
    for tail in tails:
        halo.append(lax.ppermute(tail, "seq", [(i, i + 1) for i in range(seq_size - 1)]))

    inner, group, distance = [], state, 1
    while True:
        got = swap(send, "seq", distance)
        if 2 * distance >= seq_size:
            break
        shape = pltpu.VMEM(state.shape, F32)
        operands = [me, mem_decay, *inner, got, group]
        memory, group, send = pl.pallas_call(
            functools.partial(fold_kernel, distance),
            in_specs=[SMEM, SMEM] + [VMEM] * (len(operands) - 2),
            out_specs=[VMEM] * 3,
            out_shape=[shape, shape, pltpu.VMEM(send.shape, BF16)],
            compiler_params=params(16),
            cost_estimate=cost(1e9, 5 * state.size * 4),
        )(*operands)
        inner, distance = [memory], 2 * distance
    memory = [*inner, got, group]

    local = make_local(queries, keys, values, span_bounds, me, width)
    own, total, norm = make_readout(distance, queries, local, memory, me, mem_decay, mem_gate)
    chunks = [(BAND, own)]
    for start, size in ((EARLY, BAND - EARLY), (0, EARLY)):
        own = make_attend(
            start, size, queries, keys, values,
            halo, total, norm, span_bounds, me, mem_gate,
        )
        chunks.append((start, own))

    done = []
    for number, (start, own) in enumerate(chunks):
        xs = {0: own}
        mask = head_size // 2
        while mask:
            for at, x in list(xs.items()):
                xs[at ^ mask] = swap(x, "head", mask)
            mask //= 2
        terms = [(xs[i], weights[i]) for i in range(head_size)]
        sums = None
        if number == 0 and partners:
            late = lambda kind: kind is not None and not kind[3]
            early = [(x, [w for w in ws if not late(w[0])]) for x, ws in terms]
            sums = project(start, seg_rows, F32, early, me)
            terms = [(xs[i], [w for w in weights[i] if late(w[0])]) for i in partners]
        ready = done if number == len(chunks) - 1 else ()
        out = project(
            start, seg_rows, BF16, terms, me, sums,
            ready,
        )
        done.append((start, out))
    return out


def solution(mesh):
    return jax.shard_map(
        body,
        mesh=mesh,
        in_specs=(
            P("seq", "head"),
            P("seq", "head"),
            P("seq", "head"),
            P(),
            P(None, "head"),
            P("head"),
            P("head", None),
        ),
        out_specs=P("seq", "head"),
        check_vma=False,
    )
```

```python
import functools
import math

import jax
import jax.numpy as jnp
from jax import lax
from jax.experimental import pallas as pl
from jax.experimental.pallas import tpu as pltpu
from jax.sharding import PartitionSpec as P

BAND = 512
SPAN_DEV = 2
PAD = 8
SEND_PAD = 16
MASKED = -1e30
BLOCK = 256
TILE = 256
EARLY = 320
LATE = 384


SMEM = pl.BlockSpec(memory_space=pltpu.SMEM)
VMEM = pl.BlockSpec(memory_space=pltpu.VMEM)
HBM = pl.BlockSpec(memory_space=pltpu.HBM)
F32, BF16 = jnp.float32, jnp.bfloat16


def phi(x):
    return jnp.where(x > 0, x + 1.0, jnp.exp(jnp.minimum(x, 0.0)))


def split(x):
    high = x.astype(BF16)
    return high, (x - high.astype(F32)).astype(BF16)


def params(limit_mib):
    return pltpu.CompilerParams(vmem_limit_bytes=limit_mib << 20)


def in_hbm(x):
    return pltpu.with_memory_space_constraint(x, pltpu.HBM)


def in_vmem(x):
    return pltpu.with_memory_space_constraint(x, pltpu.VMEM)


def cost(flops, moved):
    return pl.CostEstimate(flops=int(flops), bytes_accessed=int(moved), transcendentals=0)


def pack(ref, head, memory, total):
    width = memory.shape[0]
    ref[head, :width, :] = memory.astype(BF16)
    high, low = split(total)
    row = lax.broadcasted_iota(jnp.int32, (SEND_PAD, total.shape[1]), 0)
    both = jnp.where(row == 0, high.astype(F32), jnp.where(row == 1, low.astype(F32), 0.0))
    ref[head, width:, :] = both.astype(BF16)


def unpack(ref, head):
    width = ref.shape[2]
    memory = ref[head, :width, :].astype(F32)
    total = jnp.sum(ref[head, width:, :].astype(F32), axis=0, keepdims=True)
    return memory, total


def store(ref, head, memory, total):
    width = memory.shape[0]
    ref[head, :width, :] = memory
    ref[head, width:, :] = jnp.broadcast_to(total, (PAD, total.shape[1]))


def load(ref, head):
    width = ref.shape[2]
    return ref[head, :width, :], ref[head, width : width + 1, :]


def slice_copies(slices, at_ref, w_hbm, blocks, sems):
    me, head_index = at_ref[0], at_ref[1]
    copies = []
    for number, (mask, partner, part) in enumerate(slices):
        rows, columns = blocks[number].shape
        half = w_hbm.shape[0] // 2
        row = part * rows + (jnp.where((me & partner) != 0, half, 0) if partner else 0)
        col = pl.multiple_of((head_index ^ mask) * columns, columns)
        source = w_hbm.at[pl.ds(pl.multiple_of(row, rows), rows), pl.ds(col, columns)]
        copies.append(pltpu.make_async_copy(source, blocks[number], sems.at[number]))
    return copies


def state_kernel(slices, at_ref, q_hbm, k_hbm, v_hbm, w_hbm, state_ref, send_ref, *refs):
    *outs, sems, w_sems = refs
    (q_buf, k_buf, v_buf), tails, blocks = outs[:3], outs[3:6], outs[6:]
    heads, width = state_ref.shape[0], state_ref.shape[2]
    rows = k_buf.shape[0]
    steps = rows // BLOCK
    copies = []
    for step in range(steps):
        at = pl.ds(step * BLOCK, BLOCK)
        pair = [
            pltpu.make_async_copy(src.at[at], buf.at[at], sems.at[which, step])
            for which, (src, buf) in enumerate(((k_hbm, k_buf), (v_hbm, v_buf)))
        ]
        for copy in pair:
            copy.start()
        copies.append(pair)
    moves = slice_copies(slices, at_ref, w_hbm, blocks, w_sems)
    base, middle = rows - BAND, LATE - EARLY
    pieces = [
        (q_hbm, q_buf),
        (k_hbm.at[base + LATE : rows], tails[0]),
        (k_hbm.at[base + EARLY : base + LATE], tails[1].at[:middle]),
        (v_hbm.at[base + EARLY : rows], tails[1].at[middle:]),
        (k_hbm.at[base : base + EARLY], tails[2].at[:EARLY]),
        (v_hbm.at[base : base + EARLY], tails[2].at[EARLY:]),
    ]
    for number, (source, target) in enumerate(pieces, len(slices)):
        moves.append(pltpu.make_async_copy(source, target, w_sems.at[number]))
    for copy in moves:
        copy.start()
    for step in range(steps):
        for copy in copies[step]:
            copy.wait()
        at = slice(step * BLOCK, (step + 1) * BLOCK)
        for head in range(heads):
            cols = slice(head * width, (head + 1) * width)
            feats = phi(k_buf[at, cols].astype(F32))
            high, low = split(feats)
            vals = v_buf[at, cols]
            dims = (((0,), (0,)), ((), ()))
            memory = lax.dot_general(high, vals, dims, preferred_element_type=F32)
            memory += lax.dot_general(low, vals, dims, preferred_element_type=F32)
            total = jnp.sum(feats, axis=0, keepdims=True)
            if step:
                had, had_total = load(state_ref, head)
                memory, total = memory + had, total + had_total
            store(state_ref, head, memory, total)
            if step == steps - 1:
                pack(send_ref, head, memory, total)
    for copy in moves:
        copy.wait()


def make_state(queries, keys, values, out_weight, slices, at, heads, width, columns):
    rows, cols = keys.shape
    depth = out_weight.shape[0]
    split_in = [sum(other[0] == mask for other in slices) for mask, _, _ in slices]
    sizes = [depth // (2 * n if by else n) for n, (_, by, _) in zip(split_in, slices)]
    steps = rows // BLOCK
    tails = (BAND - LATE, LATE - EARLY + BAND - EARLY, 2 * EARLY)
    return pl.pallas_call(
        functools.partial(state_kernel, slices),
        in_specs=[SMEM, HBM, HBM, HBM, HBM],
        out_specs=[VMEM] * (8 + len(slices)),
        out_shape=[
            pltpu.VMEM((heads, width + PAD, width), F32),
            pltpu.VMEM((heads, width + SEND_PAD, width), BF16),
            *[pltpu.VMEM((rows, cols), BF16)] * 3,
            *(pltpu.VMEM((tail, cols), BF16) for tail in tails),
            *(pltpu.VMEM((rows_, columns), BF16) for rows_ in sizes),
        ],
        scratch_shapes=[
            pltpu.SemaphoreType.DMA((2, steps)),
            pltpu.SemaphoreType.DMA((len(slices) + 6,)),
        ],
        compiler_params=params(24),
        cost_estimate=cost(1e10, 4 * keys.size * 2),
        name="state",
    )(at, in_hbm(queries), in_hbm(keys), in_hbm(values), in_hbm(out_weight))


def fold(distance, me, decay_ref, head, memory, group, got):
    upper = (me & distance) != 0
    base = me & ~(distance - 1)
    above = base | distance
    through, before = 1.0, 1.0
    for step in range(distance):
        through = through * decay_ref[head, above + step]
        if step < distance - 1:
            factor = decay_ref[head, base + step]
            before = before * jnp.where(base + step < me, factor, 1.0)
    before = jnp.where(upper, before, 0.0)
    low, high = jnp.where(upper, 1.0, through), jnp.where(upper, through, 1.0)
    both = [low * mine + high * theirs for mine, theirs in zip(group, got)]
    if memory is None:
        memory = [before * theirs for theirs in got]
    else:
        memory = [mine + before * theirs for mine, theirs in zip(memory, got)]
    return memory, both


def fold_kernel(distance, me_ref, decay_ref, *refs):
    *inner, got_ref, group_ref, memory_ref, total_ref, send_ref = refs
    me = me_ref[0]
    for head in range(group_ref.shape[0]):
        memory = load(inner[0], head) if inner else None
        memory, both = fold(
            distance, me, decay_ref, head, memory, load(group_ref, head), unpack(got_ref, head)
        )
        store(memory_ref, head, *memory)
        store(total_ref, head, *both)
        pack(send_ref, head, *both)


def local_block(half, start, base, me_ref, spans_ref, query, keys_before, values_before, keys, values):
    me = me_ref[0]
    rows, width = keys.shape
    factor = math.log2(math.e) / math.sqrt(width)
    origin = (me * SPAN_DEV + half) * rows
    first = spans_ref[0, me * SPAN_DEV + half] - origin
    end = spans_ref[1, me * SPAN_DEV + half] - origin
    shift = 0 if half else jnp.where(me > 0, 0, rows + 1)
    dims = (((1,), (1,)), ((), ()))
    prev = lax.dot_general(query, keys_before, dims, preferred_element_type=F32)
    own = lax.dot_general(query, keys, dims, preferred_element_type=F32)
    row = start + lax.broadcasted_iota(jnp.int32, (query.shape[0], 1), 0)
    limit = jnp.where((row >= first) & (row < end), end - 1, row)
    mixed_to = start + query.shape[0] - base if half else prev.shape[1]
    near = prev[:, :mixed_to]
    col = lax.broadcasted_iota(jnp.int32, near.shape, 1) + base
    near = jnp.where(col > row + shift, near, MASKED)
    if mixed_to < prev.shape[1]:
        prev = jnp.concatenate([near, prev[:, mixed_to:]], axis=1)
    else:
        prev = near
    seen = start // BLOCK * BLOCK
    ahead = own[:, seen:]
    col = lax.broadcasted_iota(jnp.int32, ahead.shape, 1) + seen
    ahead = jnp.where(col <= limit, ahead, MASKED)
    own = jnp.concatenate([own[:, :seen], ahead], axis=1) if seen else ahead
    top = jnp.maximum(jnp.max(prev, axis=1, keepdims=True), jnp.max(own, axis=1, keepdims=True))
    prev = jnp.exp2((prev - top) * factor)
    own = jnp.exp2((own - top) * factor)
    total = jnp.sum(prev, axis=1, keepdims=True) + jnp.sum(own, axis=1, keepdims=True)
    mixed = jnp.dot(prev.astype(BF16), values_before, preferred_element_type=F32)
    mixed += jnp.dot(own.astype(BF16), values, preferred_element_type=F32)
    return mixed / total


def read_block(query, memory, norm, gate, local):
    width = query.shape[1]
    feats = phi(query.astype(F32))
    left = jnp.concatenate(split(feats), axis=1)
    both = jnp.dot(left, memory, preferred_element_type=F32)
    numer = both[:, :width] + both[:, width:]
    denom = jnp.sum(feats * norm, axis=1, keepdims=True) + 1.0
    gate = 1.0 / (1.0 + jnp.exp(jnp.full((1, width), -gate, F32)))
    return (gate * (numer / denom) + (1.0 - gate) * local).astype(BF16)


def local_kernel(width, me_ref, spans_ref, q_ref, k_ref, v_ref, out_ref):
    rows, cols = out_ref.shape
    for head in range(cols // width):
        at = slice(head * width, (head + 1) * width)
        for start in range(0, rows, BLOCK):
            out_ref[start : start + BLOCK, at] = local_block(
                1, start, start, me_ref, spans_ref, q_ref[rows + start : rows + start + BLOCK, at],
                k_ref[start:rows, at], v_ref[start:rows, at], k_ref[rows:, at], v_ref[rows:, at],
            )


def make_local(queries, keys, values, spans, me, width):
    rows, cols = queries.shape[0] // SPAN_DEV, queries.shape[1]
    return pl.pallas_call(
        functools.partial(local_kernel, width),
        in_specs=[SMEM, SMEM, VMEM, VMEM, VMEM],
        out_specs=VMEM,
        out_shape=pltpu.VMEM((rows, cols), F32),
        compiler_params=params(24),
        cost_estimate=cost(1.5e10, 6 * rows * cols * 2),
        name="local",
    )(me, spans, *map(in_vmem, (queries, keys, values)))


def readout_kernel(distance, me_ref, decay_ref, gate_ref, q_ref, local_ref, *refs):
    *inner, got_ref, group_ref, out_ref, memory_ref, norm_ref = refs
    me = me_ref[0]
    heads, width = group_ref.shape[0], group_ref.shape[2]
    rows = out_ref.shape[0]
    for head in range(heads):
        had = load(inner[0], head) if inner else None
        (memory, norm), unused = fold(
            distance, me, decay_ref, head, had, load(group_ref, head), unpack(got_ref, head)
        )
        high, low = split(memory)
        memory_ref[head, :width, :width] = high
        memory_ref[head, :width, width:] = low
        memory_ref[head, width:, :width] = high
        memory_ref[head, width:, width:] = jnp.zeros_like(low)
        norm_ref[head] = jnp.broadcast_to(norm, (PAD, width))
        at = slice(head * width, (head + 1) * width)
        out_ref[:, at] = read_block(
            q_ref[-rows:, at], memory_ref[head], norm, gate_ref[head], local_ref[:, at]
        )


def make_readout(distance, queries, local, memory, me, decay, gate):
    rows, cols = local.shape
    heads, _, width = memory[-1].shape
    return pl.pallas_call(
        functools.partial(readout_kernel, distance),
        in_specs=[SMEM, SMEM, SMEM] + [VMEM] * (2 + len(memory)),
        out_specs=[VMEM] * 3,
        out_shape=[
            pltpu.VMEM((rows, cols), BF16),
            pltpu.VMEM((heads, 2 * width, 2 * width), BF16),
            pltpu.VMEM((heads, PAD, width), F32),
        ],
        compiler_params=params(16),
        cost_estimate=cost(2e9, rows * cols * 8),
        name="readout",
    )(me, decay, gate, *map(in_vmem, (queries, local)), *memory)


def attend_kernel(start, base, me_ref, spans_ref, gate_ref, q_ref, k_ref, v_ref, *refs):
    *halo, memory_ref, norm_ref, out_ref, keys_ref, values_ref = refs
    heads, width = norm_ref.shape[0], norm_ref.shape[2]
    rows = q_ref.shape[0] // SPAN_DEV
    middle = LATE - EARLY
    if start == 0:
        keys_ref[:EARLY, :] = halo[2][:EARLY, :]
        values_ref[:EARLY, :] = halo[2][EARLY:, :]
    elif base < EARLY:
        for ref in (keys_ref, values_ref):
            ref[: EARLY - base, :] = jnp.zeros((EARLY - base, ref.shape[1]), ref.dtype)
    keys_ref[EARLY - base : LATE - base, :] = halo[1][:middle, :]
    keys_ref[LATE - base :, :] = halo[0][...]
    values_ref[EARLY - base :, :] = halo[1][middle:, :]
    for head in range(heads):
        at = slice(head * width, (head + 1) * width)
        query = q_ref[start : start + out_ref.shape[0], at]
        local = local_block(
            0, start, base, me_ref, spans_ref, query, keys_ref[:, at], values_ref[:, at],
            k_ref[:rows, at], v_ref[:rows, at],
        )
        out_ref[:, at] = read_block(
            query, memory_ref[head], norm_ref[head, :1, :], gate_ref[head], local
        )


def make_attend(start, size, queries, keys, values, halo, memory, norm, spans, me, gate):
    rows, cols = queries.shape[0] // SPAN_DEV, queries.shape[1]
    base = start // BLOCK * BLOCK
    before = pltpu.VMEM((BAND - base, cols), BF16)
    halo = halo if start == 0 else halo[:2]
    operands = [*map(in_vmem, (queries, keys, values, *halo)), memory, norm]
    return pl.pallas_call(
        functools.partial(attend_kernel, start, base),
        in_specs=[SMEM] * 3 + [VMEM] * len(operands),
        out_specs=VMEM,
        out_shape=pltpu.VMEM((size, cols), BF16),
        scratch_shapes=[before, before],
        compiler_params=params(24),
        cost_estimate=cost(8e9, 6 * rows * cols * 2),
    )(me, spans, gate, *operands)


def project_kernel(plan, first_row, adds, done, me_ref, *refs):
    if done:
        *refs, out_hbm, out_ref, sems = refs
    else:
        *refs, out_ref = refs
    refs = list(refs)
    copies = []
    for number, row in enumerate(done):
        ready = refs.pop()
        target = out_hbm.at[pl.ds(row, ready.shape[0])]
        copies.append(pltpu.make_async_copy(ready, target, sems.at[number]))
        copies[-1].start()
    me = me_ref[0]
    lefts, rights = [], []
    for pieces in plan:
        x_ref = refs.pop(0)
        parts = []
        for piece in pieces:
            if piece is None:
                parts.append(x_ref[...])
                continue
            partner, count, part, own = piece
            half = x_ref.shape[1] // 2
            size = half // count
            mine = jnp.where((me & partner) != 0, half, 0)
            at = (mine if own else half - mine) + part * size
            parts.append(x_ref[:, pl.ds(pl.multiple_of(at, size), size)])
        lefts.append(jnp.concatenate(parts, axis=1) if len(parts) > 1 else parts[0])
    for pieces in plan:
        rights.append([refs.pop(0) for _ in pieces])
    sums_ref = refs.pop(0) if adds else None
    rows, columns = out_ref.shape
    for number, start in enumerate(range(0, columns, TILE), len(done)):
        at = slice(start, start + TILE)
        acc = sums_ref[:, at] if adds else None
        for left, right in zip(lefts, rights):
            block = [w_ref[:, at] for w_ref in right]
            block = jnp.concatenate(block, axis=0) if len(block) > 1 else block[0]
            term = jnp.dot(left, block, preferred_element_type=F32)
            acc = term if acc is None else acc + term
        out_ref[:, at] = acc.astype(out_ref.dtype)
        if done:
            target = out_hbm.at[pl.ds(first_row, rows), pl.ds(start, TILE)]
            source = out_ref.at[:, pl.ds(start, TILE)]
            copies.append(pltpu.make_async_copy(source, target, sems.at[number]))
            copies[-1].start()
    for copy in copies:
        copy.wait()


def project(start, total_rows, dtype, terms, me, sums=None, done=()):
    xs = [x for x, _ in terms]
    flat = [w for _, pieces in terms for _, w in pieces]
    plan = [[kind for kind, _ in pieces] for _, pieces in terms]
    rows, columns = xs[0].shape[0], flat[0].shape[1]
    depth = sum(w.shape[0] for w in flat)
    operands = [*xs, *flat, *([] if sums is None else [sums]), *(x for _, x in reversed(done))]
    copies = pltpu.SemaphoreType.DMA((len(done) + columns // TILE,))
    return pl.pallas_call(
        functools.partial(project_kernel, plan, start, sums is not None, [row for row, _ in done]),
        in_specs=[SMEM] + [VMEM] * len(operands),
        out_specs=HBM if done else VMEM,
        out_shape=pltpu.HBM((total_rows, columns), BF16) if done else pltpu.VMEM((rows, columns), dtype),
        scratch_shapes=[pltpu.VMEM((rows, columns), BF16), copies] if done else [],
        compiler_params=params(24),
        cost_estimate=cost(2 * rows * depth * columns, depth * columns * 2),
    )(me, *map(in_vmem, operands))


def swap(x, axis, mask):
    size = lax.axis_size(axis)
    return lax.ppermute(x, axis, [(i, i ^ mask) for i in range(size)])


def body(queries, keys, values, span_bounds, mem_decay, mem_gate, out_weight):
    mem_decay, span_bounds = mem_decay.T, span_bounds.T
    seg_rows = queries.shape[0]
    heads = mem_gate.shape[0]
    width = queries.shape[1] // heads
    seq_size, head_size = lax.axis_size("seq"), lax.axis_size("head")
    assert head_size & (head_size - 1) == 0 and seg_rows == BAND * SPAN_DEV == 4 * BLOCK
    assert seq_size & (seq_size - 1) == 0 and seq_size > 1
    seq_index, head_index = lax.axis_index("seq"), lax.axis_index("head")
    me = seq_index.astype(jnp.int32).reshape(1)
    columns = out_weight.shape[1] // head_size

    masks = sorted(range(1, head_size), reverse=True)
    partners = {
        mask: (2, 1) if mask % 2 == 0 and seq_size > 2 else (1, 1) for mask in masks if mask > 1
    }
    slices = []
    for mask in (*masks, 0):
        partner, parts = partners.get(mask, (0, 1))
        slices += [(mask, partner, part) for part in range(parts)]
    at = jnp.concatenate([me, head_index.astype(jnp.int32).reshape(1)])
    state, send, *more = make_state(
        queries, keys, values, out_weight, slices, at, heads, width, columns
    )
    queries, keys, values = more[:3]
    tails, blocks = more[3:6], more[6:]
    weights = {mask: [] for mask in (*masks, 0)}
    for (mask, partner, part), block in zip(slices, blocks):
        block = swap(block, "head", mask) if mask else block
        if partner:
            count = partners[mask][1]
            other = swap(block, "seq", partner)
            weights[mask].append(((partner, count, part, True), block))
            weights[mask].append(((partner, count, part, False), other))
        else:
            weights[mask].append((None, block))

    halo = []
    for tail in tails:
        halo.append(lax.ppermute(tail, "seq", [(i, i + 1) for i in range(seq_size - 1)]))

    inner, group, distance = [], state, 1
    while True:
        got = swap(send, "seq", distance)
        if 2 * distance >= seq_size:
            break
        shape = pltpu.VMEM(state.shape, F32)
        operands = [me, mem_decay, *inner, got, group]
        memory, group, send = pl.pallas_call(
            functools.partial(fold_kernel, distance),
            in_specs=[SMEM, SMEM] + [VMEM] * (len(operands) - 2),
            out_specs=[VMEM] * 3,
            out_shape=[shape, shape, pltpu.VMEM(send.shape, BF16)],
            compiler_params=params(16),
            cost_estimate=cost(1e9, 5 * state.size * 4),
        )(*operands)
        inner, distance = [memory], 2 * distance
    memory = [*inner, got, group]

    local = make_local(queries, keys, values, span_bounds, me, width)
    own, total, norm = make_readout(distance, queries, local, memory, me, mem_decay, mem_gate)
    chunks = [(BAND, own)]
    for start, size in ((EARLY, BAND - EARLY), (0, EARLY)):
        own = make_attend(
            start, size, queries, keys, values,
            halo, total, norm, span_bounds, me, mem_gate,
        )
        chunks.append((start, own))

    done = []
    for number, (start, own) in enumerate(chunks):
        xs = {0: own}
        mask = head_size // 2
        while mask:
            for at, x in list(xs.items()):
                xs[at ^ mask] = swap(x, "head", mask)
            mask //= 2
        terms = [(xs[i], weights[i]) for i in range(head_size)]
        sums = None
        if number == 0 and partners:
            late = lambda kind: kind is not None and not kind[3]
            early = [(x, [w for w in ws if not late(w[0])]) for x, ws in terms]
            sums = project(start, seg_rows, F32, early, me)
            terms = [(xs[i], [w for w in weights[i] if late(w[0])]) for i in partners]
        ready = done if number == len(chunks) - 1 else ()
        out = project(
            start, seg_rows, BF16, terms, me, sums,
            ready,
        )
        done.append((start, out))
    return out


def solution(mesh):
    return jax.shard_map(
        body,
        mesh=mesh,
        in_specs=(
            P("seq", "head"),
            P("seq", "head"),
            P("seq", "head"),
            P(),
            P(None, "head"),
            P("head"),
            P("head", None),
        ),
        out_specs=P("seq", "head"),
        check_vma=False,
    )
```

```python
import functools
import math

import jax
import jax.numpy as jnp
from jax import lax
from jax.experimental import pallas as pl
from jax.experimental.pallas import tpu as pltpu
from jax.sharding import PartitionSpec as P

BAND = 512
SPAN_DEV = 2
PAD = 8
SEND_PAD = 16
MASKED = -1e30
BLOCK = 256
TILE = 256
EARLY = 320
LATE = 384


SMEM = pl.BlockSpec(memory_space=pltpu.SMEM)
VMEM = pl.BlockSpec(memory_space=pltpu.VMEM)
HBM = pl.BlockSpec(memory_space=pltpu.HBM)
F32, BF16 = jnp.float32, jnp.bfloat16


def phi(x):
    return jnp.where(x > 0, x + 1.0, jnp.exp(jnp.minimum(x, 0.0)))


def split(x):
    high = x.astype(BF16)
    return high, (x - high.astype(F32)).astype(BF16)


def params(limit_mib):
    return pltpu.CompilerParams(vmem_limit_bytes=limit_mib << 20)


def in_hbm(x):
    return pltpu.with_memory_space_constraint(x, pltpu.HBM)


def in_vmem(x):
    return pltpu.with_memory_space_constraint(x, pltpu.VMEM)


def cost(flops, moved):
    return pl.CostEstimate(flops=int(flops), bytes_accessed=int(moved), transcendentals=0)


def pack(ref, head, memory, total):
    width = memory.shape[0]
    ref[head, :width, :] = memory.astype(BF16)
    high, low = split(total)
    row = lax.broadcasted_iota(jnp.int32, (SEND_PAD, total.shape[1]), 0)
    both = jnp.where(row == 0, high.astype(F32), jnp.where(row == 1, low.astype(F32), 0.0))
    ref[head, width:, :] = both.astype(BF16)


def unpack(ref, head):
    width = ref.shape[2]
    memory = ref[head, :width, :].astype(F32)
    total = jnp.sum(ref[head, width:, :].astype(F32), axis=0, keepdims=True)
    return memory, total


def store(ref, head, memory, total):
    width = memory.shape[0]
    ref[head, :width, :] = memory
    ref[head, width:, :] = jnp.broadcast_to(total, (PAD, total.shape[1]))


def load(ref, head):
    width = ref.shape[2]
    return ref[head, :width, :], ref[head, width : width + 1, :]


def slice_copies(slices, at_ref, w_hbm, blocks, sems):
    me, head_index = at_ref[0], at_ref[1]
    copies = []
    for number, (mask, partner, part) in enumerate(slices):
        rows, columns = blocks[number].shape
        half = w_hbm.shape[0] // 2
        row = part * rows + (jnp.where((me & partner) != 0, half, 0) if partner else 0)
        col = pl.multiple_of((head_index ^ mask) * columns, columns)
        source = w_hbm.at[pl.ds(pl.multiple_of(row, rows), rows), pl.ds(col, columns)]
        copies.append(pltpu.make_async_copy(source, blocks[number], sems.at[number]))
    return copies


def slice_kernel(slices, at_ref, w_hbm, *refs):
    *blocks, sems = refs
    copies = slice_copies(slices, at_ref, w_hbm, blocks, sems)
    for copy in copies:
        copy.start()
    for copy in copies:
        copy.wait()


def make_slices(out_weight, slices, at, columns):
    block = pltpu.VMEM((out_weight.shape[0], columns), BF16)
    return pl.pallas_call(
        functools.partial(slice_kernel, slices),
        in_specs=[SMEM, HBM],
        out_specs=[VMEM] * len(slices),
        out_shape=[block] * len(slices),
        scratch_shapes=[pltpu.SemaphoreType.DMA((len(slices),))],
        compiler_params=params(8),
        cost_estimate=cost(1e9, 4 * out_weight.shape[0] * columns * len(slices)),
        name="slices",
    )(at, in_hbm(out_weight))


def state_kernel(slices, at_ref, q_hbm, k_hbm, v_hbm, w_hbm, state_ref, send_ref, *refs):
    *outs, sems, w_sems = refs
    (q_buf, k_buf, v_buf), tails, blocks = outs[:3], outs[3:6], outs[6:]
    heads, width = state_ref.shape[0], state_ref.shape[2]
    rows = k_buf.shape[0]
    steps = rows // BLOCK
    copies = []
    for step in range(steps):
        at = pl.ds(step * BLOCK, BLOCK)
        pair = [
            pltpu.make_async_copy(src.at[at], buf.at[at], sems.at[which, step])
            for which, (src, buf) in enumerate(((k_hbm, k_buf), (v_hbm, v_buf)))
        ]
        for copy in pair:
            copy.start()
        copies.append(pair)
    moves = slice_copies(slices, at_ref, w_hbm, blocks, w_sems)
    moves.append(pltpu.make_async_copy(q_hbm, q_buf, w_sems.at[len(slices)]))
    for copy in moves:
        copy.start()
    for step in range(steps):
        for copy in copies[step]:
            copy.wait()
        at = slice(step * BLOCK, (step + 1) * BLOCK)
        for head in range(heads):
            cols = slice(head * width, (head + 1) * width)
            feats = phi(k_buf[at, cols].astype(F32))
            high, low = split(feats)
            vals = v_buf[at, cols]
            dims = (((0,), (0,)), ((), ()))
            memory = lax.dot_general(high, vals, dims, preferred_element_type=F32)
            memory += lax.dot_general(low, vals, dims, preferred_element_type=F32)
            total = jnp.sum(feats, axis=0, keepdims=True)
            if step:
                had, had_total = load(state_ref, head)
                memory, total = memory + had, total + had_total
            store(state_ref, head, memory, total)
            if step == steps - 1:
                pack(send_ref, head, memory, total)
    base = rows - BAND
    middle = LATE - EARLY
    tails[0][...] = k_buf[base + LATE :, :]
    tails[1][:middle, :] = k_buf[base + EARLY : base + LATE, :]
    tails[1][middle:, :] = v_buf[base + EARLY :, :]
    tails[2][:EARLY, :] = k_buf[base : base + EARLY, :]
    tails[2][EARLY:, :] = v_buf[base : base + EARLY, :]
    for copy in moves:
        copy.wait()


def make_state(queries, keys, values, out_weight, slices, at, heads, width, columns):
    rows, cols = keys.shape
    depth = out_weight.shape[0]
    split_in = [sum(other[0] == mask for other in slices) for mask, _, _ in slices]
    sizes = [depth // (2 * n if by else n) for n, (_, by, _) in zip(split_in, slices)]
    steps = rows // BLOCK
    tails = (BAND - LATE, LATE - EARLY + BAND - EARLY, 2 * EARLY)
    return pl.pallas_call(
        functools.partial(state_kernel, slices),
        in_specs=[SMEM, HBM, HBM, HBM, HBM],
        out_specs=[VMEM] * (8 + len(slices)),
        out_shape=[
            pltpu.VMEM((heads, width + PAD, width), F32),
            pltpu.VMEM((heads, width + SEND_PAD, width), BF16),
            *[pltpu.VMEM((rows, cols), BF16)] * 3,
            *(pltpu.VMEM((tail, cols), BF16) for tail in tails),
            *(pltpu.VMEM((rows_, columns), BF16) for rows_ in sizes),
        ],
        scratch_shapes=[
            pltpu.SemaphoreType.DMA((2, steps)),
            pltpu.SemaphoreType.DMA((len(slices) + 1,)),
        ],
        compiler_params=params(24),
        cost_estimate=cost(1e10, 4 * keys.size * 2),
        name="state",
    )(at, in_hbm(queries), in_hbm(keys), in_hbm(values), in_hbm(out_weight))


def fold(distance, me, decay_ref, head, memory, group, got):
    upper = (me & distance) != 0
    base = me & ~(distance - 1)
    above = base | distance
    through, before = 1.0, 1.0
    for step in range(distance):
        through = through * decay_ref[head, above + step]
        if step < distance - 1:
            factor = decay_ref[head, base + step]
            before = before * jnp.where(base + step < me, factor, 1.0)
    before = jnp.where(upper, before, 0.0)
    low, high = jnp.where(upper, 1.0, through), jnp.where(upper, through, 1.0)
    both = [low * mine + high * theirs for mine, theirs in zip(group, got)]
    if memory is None:
        memory = [before * theirs for theirs in got]
    else:
        memory = [mine + before * theirs for mine, theirs in zip(memory, got)]
    return memory, both


def fold_kernel(distance, me_ref, decay_ref, *refs):
    *inner, got_ref, group_ref, memory_ref, total_ref, send_ref = refs
    me = me_ref[0]
    for head in range(group_ref.shape[0]):
        memory = load(inner[0], head) if inner else None
        memory, both = fold(
            distance, me, decay_ref, head, memory, load(group_ref, head), unpack(got_ref, head)
        )
        store(memory_ref, head, *memory)
        store(total_ref, head, *both)
        pack(send_ref, head, *both)


def local_block(half, start, base, me_ref, spans_ref, query, keys_before, values_before, keys, values):
    me = me_ref[0]
    rows, width = keys.shape
    factor = math.log2(math.e) / math.sqrt(width)
    origin = (me * SPAN_DEV + half) * rows
    first = spans_ref[0, me * SPAN_DEV + half] - origin
    end = spans_ref[1, me * SPAN_DEV + half] - origin
    shift = 0 if half else jnp.where(me > 0, 0, rows + 1)
    dims = (((1,), (1,)), ((), ()))
    prev = lax.dot_general(query, keys_before, dims, preferred_element_type=F32)
    own = lax.dot_general(query, keys, dims, preferred_element_type=F32)
    row = start + lax.broadcasted_iota(jnp.int32, (query.shape[0], 1), 0)
    limit = jnp.where((row >= first) & (row < end), end - 1, row)
    col = lax.broadcasted_iota(jnp.int32, prev.shape, 1) + base
    prev = jnp.where(col > row + shift, prev, MASKED)
    col = lax.broadcasted_iota(jnp.int32, own.shape, 1)
    own = jnp.where(col <= limit, own, MASKED)
    top = jnp.maximum(jnp.max(prev, axis=1, keepdims=True), jnp.max(own, axis=1, keepdims=True))
    prev = jnp.exp2((prev - top) * factor)
    own = jnp.exp2((own - top) * factor)
    total = jnp.sum(prev, axis=1, keepdims=True) + jnp.sum(own, axis=1, keepdims=True)
    mixed = jnp.dot(prev.astype(BF16), values_before, preferred_element_type=F32)
    mixed += jnp.dot(own.astype(BF16), values, preferred_element_type=F32)
    return mixed / total


def read_block(query, memory, norm, gate, local):
    width = query.shape[1]
    feats = phi(query.astype(F32))
    left = jnp.concatenate(split(feats), axis=1)
    both = jnp.dot(left, memory, preferred_element_type=F32)
    numer = both[:, :width] + both[:, width:]
    denom = jnp.sum(feats * norm, axis=1, keepdims=True) + 1.0
    gate = 1.0 / (1.0 + jnp.exp(jnp.full((1, width), -gate, F32)))
    return (gate * (numer / denom) + (1.0 - gate) * local).astype(BF16)


def local_kernel(width, me_ref, spans_ref, q_ref, k_ref, v_ref, out_ref):
    rows, cols = out_ref.shape
    for head in range(cols // width):
        at = slice(head * width, (head + 1) * width)
        for start in range(0, rows, BLOCK):
            out_ref[start : start + BLOCK, at] = local_block(
                1, start, start, me_ref, spans_ref, q_ref[rows + start : rows + start + BLOCK, at],
                k_ref[start:rows, at], v_ref[start:rows, at], k_ref[rows:, at], v_ref[rows:, at],
            )


def make_local(queries, keys, values, spans, me, width):
    rows, cols = queries.shape[0] // SPAN_DEV, queries.shape[1]
    return pl.pallas_call(
        functools.partial(local_kernel, width),
        in_specs=[SMEM, SMEM, VMEM, VMEM, VMEM],
        out_specs=VMEM,
        out_shape=pltpu.VMEM((rows, cols), F32),
        compiler_params=params(24),
        cost_estimate=cost(1.5e10, 6 * rows * cols * 2),
        name="local",
    )(me, spans, *map(in_vmem, (queries, keys, values)))


def readout_kernel(distance, me_ref, decay_ref, gate_ref, q_ref, local_ref, *refs):
    *inner, got_ref, group_ref, out_ref, memory_ref, norm_ref = refs
    me = me_ref[0]
    heads, width = group_ref.shape[0], group_ref.shape[2]
    rows = out_ref.shape[0]
    for head in range(heads):
        had = load(inner[0], head) if inner else None
        (memory, norm), unused = fold(
            distance, me, decay_ref, head, had, load(group_ref, head), unpack(got_ref, head)
        )
        high, low = split(memory)
        memory_ref[head, :width, :width] = high
        memory_ref[head, :width, width:] = low
        memory_ref[head, width:, :width] = high
        memory_ref[head, width:, width:] = jnp.zeros_like(low)
        norm_ref[head] = jnp.broadcast_to(norm, (PAD, width))
        at = slice(head * width, (head + 1) * width)
        out_ref[:, at] = read_block(
            q_ref[-rows:, at], memory_ref[head], norm, gate_ref[head], local_ref[:, at]
        )


def make_readout(distance, queries, local, memory, me, decay, gate):
    rows, cols = local.shape
    heads, _, width = memory[-1].shape
    return pl.pallas_call(
        functools.partial(readout_kernel, distance),
        in_specs=[SMEM, SMEM, SMEM] + [VMEM] * (2 + len(memory)),
        out_specs=[VMEM] * 3,
        out_shape=[
            pltpu.VMEM((rows, cols), BF16),
            pltpu.VMEM((heads, 2 * width, 2 * width), BF16),
            pltpu.VMEM((heads, PAD, width), F32),
        ],
        compiler_params=params(16),
        cost_estimate=cost(2e9, rows * cols * 8),
        name="readout",
    )(me, decay, gate, *map(in_vmem, (queries, local)), *memory)


def attend_kernel(start, base, me_ref, spans_ref, gate_ref, q_ref, k_ref, v_ref, *refs):
    *halo, memory_ref, norm_ref, out_ref, keys_ref, values_ref = refs
    heads, width = norm_ref.shape[0], norm_ref.shape[2]
    rows = q_ref.shape[0] // SPAN_DEV
    middle = LATE - EARLY
    if start == 0:
        keys_ref[:EARLY, :] = halo[2][:EARLY, :]
        values_ref[:EARLY, :] = halo[2][EARLY:, :]
    elif base < EARLY:
        for ref in (keys_ref, values_ref):
            ref[: EARLY - base, :] = jnp.zeros((EARLY - base, ref.shape[1]), ref.dtype)
    keys_ref[EARLY - base : LATE - base, :] = halo[1][:middle, :]
    keys_ref[LATE - base :, :] = halo[0][...]
    values_ref[EARLY - base :, :] = halo[1][middle:, :]
    for head in range(heads):
        at = slice(head * width, (head + 1) * width)
        query = q_ref[start : start + out_ref.shape[0], at]
        local = local_block(
            0, start, base, me_ref, spans_ref, query, keys_ref[:, at], values_ref[:, at],
            k_ref[:rows, at], v_ref[:rows, at],
        )
        out_ref[:, at] = read_block(
            query, memory_ref[head], norm_ref[head, :1, :], gate_ref[head], local
        )


def make_attend(start, size, queries, keys, values, halo, memory, norm, spans, me, gate):
    rows, cols = queries.shape[0] // SPAN_DEV, queries.shape[1]
    base = start // BLOCK * BLOCK
    before = pltpu.VMEM((BAND - base, cols), BF16)
    halo = halo if start == 0 else halo[:2]
    operands = [*map(in_vmem, (queries, keys, values, *halo)), memory, norm]
    return pl.pallas_call(
        functools.partial(attend_kernel, start, base),
        in_specs=[SMEM] * 3 + [VMEM] * len(operands),
        out_specs=VMEM,
        out_shape=pltpu.VMEM((size, cols), BF16),
        scratch_shapes=[before, before],
        compiler_params=params(24),
        cost_estimate=cost(8e9, 6 * rows * cols * 2),
    )(me, spans, gate, *operands)


def project_kernel(plan, first_row, adds, done, me_ref, *refs):
    if done:
        *refs, out_hbm, out_ref, sems = refs
    else:
        *refs, out_ref = refs
    refs = list(refs)
    copies = []
    for number, row in enumerate(done):
        ready = refs.pop()
        target = out_hbm.at[pl.ds(row, ready.shape[0])]
        copies.append(pltpu.make_async_copy(ready, target, sems.at[number]))
        copies[-1].start()
    me = me_ref[0]
    lefts, rights = [], []
    for pieces in plan:
        x_ref = refs.pop(0)
        parts = []
        for piece in pieces:
            if piece is None:
                parts.append(x_ref[...])
                continue
            partner, count, part, own = piece
            half = x_ref.shape[1] // 2
            size = half // count
            mine = jnp.where((me & partner) != 0, half, 0)
            at = (mine if own else half - mine) + part * size
            parts.append(x_ref[:, pl.ds(pl.multiple_of(at, size), size)])
        lefts.append(jnp.concatenate(parts, axis=1) if len(parts) > 1 else parts[0])
    for pieces in plan:
        rights.append([refs.pop(0) for _ in pieces])
    sums_ref = refs.pop(0) if adds else None
    rows, columns = out_ref.shape
    for number, start in enumerate(range(0, columns, TILE), len(done)):
        at = slice(start, start + TILE)
        acc = sums_ref[:, at] if adds else None
        for left, right in zip(lefts, rights):
            block = [w_ref[:, at] for w_ref in right]
            block = jnp.concatenate(block, axis=0) if len(block) > 1 else block[0]
            term = jnp.dot(left, block, preferred_element_type=F32)
            acc = term if acc is None else acc + term
        out_ref[:, at] = acc.astype(out_ref.dtype)
        if done:
            target = out_hbm.at[pl.ds(first_row, rows), pl.ds(start, TILE)]
            source = out_ref.at[:, pl.ds(start, TILE)]
            copies.append(pltpu.make_async_copy(source, target, sems.at[number]))
            copies[-1].start()
    for copy in copies:
        copy.wait()


def project(start, total_rows, dtype, terms, me, sums=None, done=()):
    xs = [x for x, _ in terms]
    flat = [w for _, pieces in terms for _, w in pieces]
    plan = [[kind for kind, _ in pieces] for _, pieces in terms]
    rows, columns = xs[0].shape[0], flat[0].shape[1]
    depth = sum(w.shape[0] for w in flat)
    operands = [*xs, *flat, *([] if sums is None else [sums]), *(x for _, x in reversed(done))]
    copies = pltpu.SemaphoreType.DMA((len(done) + columns // TILE,))
    return pl.pallas_call(
        functools.partial(project_kernel, plan, start, sums is not None, [row for row, _ in done]),
        in_specs=[SMEM] + [VMEM] * len(operands),
        out_specs=HBM if done else VMEM,
        out_shape=pltpu.HBM((total_rows, columns), BF16) if done else pltpu.VMEM((rows, columns), dtype),
        scratch_shapes=[pltpu.VMEM((rows, columns), BF16), copies] if done else [],
        compiler_params=params(24),
        cost_estimate=cost(2 * rows * depth * columns, depth * columns * 2),
    )(me, *map(in_vmem, operands))


def swap(x, axis, mask):
    size = lax.axis_size(axis)
    return lax.ppermute(x, axis, [(i, i ^ mask) for i in range(size)])


def body(queries, keys, values, span_bounds, mem_decay, mem_gate, out_weight):
    mem_decay, span_bounds = mem_decay.T, span_bounds.T
    seg_rows = queries.shape[0]
    heads = mem_gate.shape[0]
    width = queries.shape[1] // heads
    seq_size, head_size = lax.axis_size("seq"), lax.axis_size("head")
    assert head_size & (head_size - 1) == 0 and seg_rows == BAND * SPAN_DEV == 4 * BLOCK
    assert seq_size & (seq_size - 1) == 0 and seq_size > 1
    seq_index, head_index = lax.axis_index("seq"), lax.axis_index("head")
    me = seq_index.astype(jnp.int32).reshape(1)
    columns = out_weight.shape[1] // head_size

    masks = sorted(range(1, head_size), reverse=True)
    partners = {
        mask: (2, 1) if mask % 2 == 0 and seq_size > 2 else (1, 1) for mask in masks if mask > 1
    }
    slices = []
    for mask in (*masks, 0):
        partner, parts = partners.get(mask, (0, 1))
        slices += [(mask, partner, part) for part in range(parts)]
    early = len(slices) - 2
    at = jnp.concatenate([me, head_index.astype(jnp.int32).reshape(1)])
    state, send, *more = make_state(
        queries, keys, values, out_weight, slices[:early], at, heads, width,
        columns,
    )
    queries, keys, values = more[:3]
    tails, blocks = more[3:6], more[6:]
    blocks += make_slices(out_weight, slices[early:], at, columns)
    weights = {mask: [] for mask in (*masks, 0)}
    for (mask, partner, part), block in zip(slices, blocks):
        block = swap(block, "head", mask) if mask else block
        if partner:
            count = partners[mask][1]
            other = swap(block, "seq", partner)
            weights[mask].append(((partner, count, part, True), block))
            weights[mask].append(((partner, count, part, False), other))
        else:
            weights[mask].append((None, block))

    halo = []
    for tail in tails:
        halo.append(lax.ppermute(tail, "seq", [(i, i + 1) for i in range(seq_size - 1)]))

    inner, group, distance = [], state, 1
    while True:
        got = swap(send, "seq", distance)
        if 2 * distance >= seq_size:
            break
        shape = pltpu.VMEM(state.shape, F32)
        operands = [me, mem_decay, *inner, got, group]
        memory, group, send = pl.pallas_call(
            functools.partial(fold_kernel, distance),
            in_specs=[SMEM, SMEM] + [VMEM] * (len(operands) - 2),
            out_specs=[VMEM] * 3,
            out_shape=[shape, shape, pltpu.VMEM(send.shape, BF16)],
            compiler_params=params(16),
            cost_estimate=cost(1e9, 5 * state.size * 4),
        )(*operands)
        inner, distance = [memory], 2 * distance
    memory = [*inner, got, group]

    local = make_local(queries, keys, values, span_bounds, me, width)
    own, total, norm = make_readout(distance, queries, local, memory, me, mem_decay, mem_gate)
    chunks = [(BAND, own)]
    for start, size in ((EARLY, BAND - EARLY), (0, EARLY)):
        own = make_attend(
            start, size, queries, keys, values,
            halo, total, norm, span_bounds, me, mem_gate,
        )
        chunks.append((start, own))

    done = []
    for number, (start, own) in enumerate(chunks):
        xs = {0: own}
        mask = head_size // 2
        while mask:
            for at, x in list(xs.items()):
                xs[at ^ mask] = swap(x, "head", mask)
            mask //= 2
        terms = [(xs[i], weights[i]) for i in range(head_size)]
        sums = None
        if number == 0 and partners:
            late = lambda kind: kind is not None and not kind[3]
            early = [(x, [w for w in ws if not late(w[0])]) for x, ws in terms]
            sums = project(start, seg_rows, F32, early, me)
            terms = [(xs[i], [w for w in weights[i] if late(w[0])]) for i in partners]
        ready = done if number == len(chunks) - 1 else ()
        out = project(
            start, seg_rows, BF16, terms, me, sums,
            ready,
        )
        done.append((start, out))
    return out


def solution(mesh):
    return jax.shard_map(
        body,
        mesh=mesh,
        in_specs=(
            P("seq", "head"),
            P("seq", "head"),
            P("seq", "head"),
            P(),
            P(None, "head"),
            P("head"),
            P("head", None),
        ),
        out_specs=P("seq", "head"),
        check_vma=False,
    )
```
